32 devices in a mesh: col: 4 (over z), row: 8 (over y, x, core).
Axes of the slice: x: 2, y: 2, z: 4, core: 2. Of those that a mesh axis runs over, the one named last changes fastest.
Arguments:
- mask: int32 [4096, 65536], P('row', 'col')
- user_emb: bfloat16 [4096, 64], P(('row', 'col'))
- item_emb: bfloat16 [65536, 64], P(('col', 'row'))
- queries: int32 [256], replicated
Outputs:
- output 1: bfloat16 [4096, 64], P(('row', 'col'))
- output 2: bfloat16 [65536, 64], P(('col', 'row'))
- output 3: float32 [256, 65536], P(None, ('col', 'row'))
All inputs are finite; a program needn't handle non-finite values.
Results may differ from the reference program's by a relative error of at most 0.00673458.
Values are sent between devices in bfloat16 or wider.
A program may use at most 1 GiB of HBM per device.

```python
import jax
import jax.numpy as jnp
from jax import lax

USERS = 4096
ITEMS = 65536
EMB = 64
LAYERS = 3
QUERIES = 256


def draw_mask(key):
    k_noise, k_rows, k_cols = jax.random.split(key, 3)
    row_level = jax.random.randint(k_rows, (USERS,), 4, 33)
    col_level = jax.random.randint(k_cols, (ITEMS,), 4, 33)
    noise = jax.random.randint(k_noise, (USERS, ITEMS), 0, 1024)
    return (noise < row_level[:, None] * col_level[None, :]).astype(jnp.int32)


def setup_inputs(seed: int = 0) -> dict:
    key = jax.random.key(seed)
    k_mask, k_user, k_item, k_umean, k_imean, k_query = jax.random.split(key, 6)
    scale = EMB ** -0.25
    user_mean = jax.random.normal(k_umean, (EMB,), jnp.float32)
    item_mean = jax.random.normal(k_imean, (EMB,), jnp.float32)
    user_emb = ((jax.random.normal(k_user, (USERS, EMB), jnp.float32) + user_mean[None, :]) * scale).astype(jnp.bfloat16)
    item_emb = ((jax.random.normal(k_item, (ITEMS, EMB), jnp.float32) + item_mean[None, :]) * scale).astype(jnp.bfloat16)
    queries = jax.random.randint(k_query, (QUERIES,), 0, USERS).astype(jnp.int32)
    return {'mask': draw_mask(k_mask), 'user_emb': user_emb, 'item_emb': item_emb, 'queries': queries}


def norm_adjacency(mask):
    deg_user = jnp.maximum(jnp.sum(mask, axis=1), 1)
    deg_item = jnp.maximum(jnp.sum(mask, axis=0), 1)
    inv_user = lax.rsqrt(deg_user.astype(jnp.float32))
    inv_item = lax.rsqrt(deg_item.astype(jnp.float32))
    return (inv_user[:, None] * mask.astype(jnp.float32) * inv_item[None, :]).astype(jnp.bfloat16)


def reference(mask, user_emb, item_emb, queries):
    norm_adj = norm_adjacency(mask)

    def one_layer(carried, unused):
        user_cur, item_cur, user_sum, item_sum = carried
        user_next = jnp.dot(norm_adj, item_cur, preferred_element_type=jnp.float32).astype(jnp.bfloat16)
        item_next = lax.dot_general(norm_adj, user_cur, (((0,), (0,)), ((), ())), preferred_element_type=jnp.float32).astype(jnp.bfloat16)
        return (user_next, item_next, user_sum + user_next.astype(jnp.float32), item_sum + item_next.astype(jnp.float32)), None

    start_state = (user_emb, item_emb, user_emb.astype(jnp.float32), item_emb.astype(jnp.float32))
    end_state, unused_out = lax.scan(one_layer, start_state, None, length=LAYERS)
    final_user = (end_state[2] / (LAYERS + 1)).astype(jnp.bfloat16)
    final_item = (end_state[3] / (LAYERS + 1)).astype(jnp.bfloat16)
    picked = jnp.take(final_user, queries, axis=0)
    scores = lax.dot_general(picked, final_item, (((1,), (1,)), ((), ())), preferred_element_type=jnp.float32)
    return final_user, final_item, scores
```

```python
import jax
import jax.numpy as jnp
from jax import lax
from jax.experimental import pallas as pl
from jax.experimental.pallas import tpu as pltpu
from jax.sharding import PartitionSpec as P

LAYERS = 3
EMB = 64
HALF = EMB // 2
NT = (((1,), (1,)), ((), ()))
NN = (((1,), (0,)), ((), ()))
TN = (((0,), (0,)), ((), ()))
F32 = jnp.float32
BF16 = jnp.bfloat16
STAGES = 4
N_COPIES = 112


def dot(lhs, rhs, dims):
    return lax.dot_general(lhs, rhs, dims, preferred_element_type=F32)


def kernel(mask_ref, item_ref, user_ref, query_ref, fu_ref, fi_ref, pick_ref,
           adj, stage, panel, upan, psend, drecv, sacc, hop1, rown, isum, usum,
           colacc, rowacc, deg_send, deg_recv, deg_own, deg_in, deg_fin, deg_oth,
           udeg, udeg_in, invu, upart, uin, pk, stage_sem, send_sem, recv_sem):
    c = lax.axis_index('col')
    r = lax.axis_index('row')
    users = rowacc.shape[0]
    width = adj.shape[2]
    rows = stage.shape[1]
    per_slot = users // rows
    core, cx, cy = r % 2, (r // 2) % 2, r // 4

    def plane(d, k):
        return ((cy + d // 2) % 2) * 4 + ((cx + d % 2) % 2) * 2 + (core + k) % 2

    def zpeer(k):
        return ((c // 2 + k // 2) % 2) * 2 + (c % 2 + k % 2) % 2

    slots = {d * 2 + k: (c, plane(d, k)) for d in range(4) for k in range(2)}
    partner, xn, yn, dg = slots[1], slots[2], slots[4], slots[6]
    zn = [None] + [(zpeer(k), r) for k in (1, 2, 3)]

    started = []

    def send(src, dst, device):
        n = len(started)
        copy = pltpu.make_async_remote_copy(
            src_ref=src, dst_ref=dst, send_sem=send_sem.at[n], recv_sem=recv_sem.at[n],
            device_id=device, device_id_type=pl.DeviceIdType.MESH)
        copy.start()
        started.append(copy)
        return copy

    def mask_copy(step):
        slot = step // per_slot
        part = step % per_slot
        col = plane(slot // 2, slot % 2) * width
        return pltpu.make_async_copy(
            mask_ref.at[pl.ds(pl.multiple_of(part * rows, rows), rows),
                        pl.ds(pl.multiple_of(col, width), width)],
            stage.at[step % STAGES], stage_sem.at[step % STAGES])

    steps = 8 * per_slot
    for s in range(STAGES):
        mask_copy(jnp.int32(s)).start()

    barrier = pltpu.get_barrier_semaphore()
    peers = (partner, xn, yn, dg, zn[1], zn[2], zn[3])
    for device in peers:
        pl.semaphore_signal(barrier, inc=1, device_id=device, device_id_type=pl.DeviceIdType.MESH)

    eye = (lax.broadcasted_iota(jnp.int32, (EMB, EMB), 0)
           == lax.broadcasted_iota(jnp.int32, (EMB, EMB), 1)).astype(BF16)
    items_t = dot(eye, item_ref[...], NT)
    users_t = dot(eye, user_ref[...], NT)
    isum[...] = items_t
    usum[...] = users_t
    panel[0, 0] = items_t.astype(BF16)
    upan[0, c] = users_t.astype(BF16)
    rowacc[...] = jnp.zeros_like(rowacc)
    colacc[...] = jnp.zeros_like(colacc)
    pl.semaphore_wait(barrier, len(peers))

    def gather_start(n):
        own = panel.at[n, 0]
        lo, hi = pl.ds(0, HALF), pl.ds(HALF, HALF)
        g = {}
        g['xa'] = send(own.at[lo], panel.at[n, 2, lo], xn)
        g['yb'] = send(own.at[hi], panel.at[n, 4, hi], yn)
        g['xb'] = send(own.at[hi], panel.at[n, 2, hi], xn)
        g['ya'] = send(own.at[lo], panel.at[n, 4, lo], yn)
        g['p0'] = send(own, panel.at[n, 1], partner)
        return g

    def gather_forward(n, g):
        lo, hi = pl.ds(0, HALF), pl.ds(HALF, HALF)
        g['xa'].wait_recv()
        g['da'] = send(panel.at[n, 2, lo], panel.at[n, 6, lo], yn)
        g['yb'].wait_recv()
        g['db'] = send(panel.at[n, 4, hi], panel.at[n, 6, hi], xn)
        g['xb'].wait_recv()
        g['p1'] = send(panel.at[n, 2], panel.at[n, 3], partner)
        g['ya'].wait_recv()
        g['p2'] = send(panel.at[n, 4], panel.at[n, 5], partner)

    def gather_last(n, g):
        g['da'].wait_recv()
        g['db'].wait_recv()
        g['p3'] = send(panel.at[n, 6], panel.at[n, 7], partner)

    def zgather_start(n):
        return [send(upan.at[n, c], upan.at[n, c], zn[k]) for k in (1, 2, 3)]

    def zgather_wait(n, g):
        for copy in g:
            copy.wait_recv()
        return jnp.concatenate([upan[n, k] for k in range(4)], axis=1)

    def zsum_start(n, acc):
        acc_t = acc.T
        for k in range(4):
            upart[n, k] = acc_t[:, k * 128:(k + 1) * 128]
        return [send(upart.at[n, zpeer(k)], uin.at[n, k - 1], zn[k]) for k in (1, 2, 3)]

    def zsum_wait(n, g):
        for copy in g:
            copy.wait_recv()
        total = (upart[n, c] + uin[n, 0]) + (uin[n, 1] + uin[n, 2])
        nxt = total.astype(BF16)
        usum[...] = usum[...] + nxt.astype(F32)
        return nxt

    gather0 = gather_start(0)
    zgather0 = zgather_start(0)

    def mask_step(step, carry):
        mask_copy(step).wait()
        slot = step // per_slot
        part = step % per_slot
        buf = step % STAGES

        def group(i, col):
            at = pl.multiple_of(i * 16, 16)
            x = stage[buf, pl.ds(at, 16), :].astype(F32)
            row = pl.multiple_of(part * rows + i * 16, 16)
            adj[slot, pl.ds(row, 16), :] = x.astype(BF16)
            lanes = x[:, :128]
            for t in range(1, width // 128):
                lanes = lanes + x[:, t * 128:(t + 1) * 128]
            rowacc[pl.ds(row, 16), :] += lanes
            return col + (x[:8] + x[8:])

        colacc[slot] += lax.fori_loop(0, rows // 16, group, jnp.zeros((8, width), F32), unroll=2)

        @pl.when(step + STAGES < steps)
        def _():
            mask_copy(step + STAGES).start()

        return carry

    lax.fori_loop(0, steps * 5 // 8, mask_step, 0)
    gather_forward(0, gather0)
    lax.fori_loop(steps * 5 // 8, steps, mask_step, 0)

    for d in range(4):
        deg_send[d:d + 1, :] = jnp.sum(colacc[2 * d + 1], axis=0, keepdims=True)
    dp = send(deg_send, deg_recv, partner)
    udeg[...] = dot(jnp.ones((8, 128), BF16), rowacc[...].astype(BF16), NT)
    zd = [send(udeg, udeg_in.at[k - 1], zn[k]) for k in (1, 2, 3)]
    mine = jnp.concatenate(
        [jnp.sum(colacc[2 * d], axis=0, keepdims=True) for d in range(4)], axis=0)
    dp.wait_recv()
    deg_own[...] = mine + deg_recv[...]
    ds = [send(deg_own, deg_in.at[0], xn), send(deg_own, deg_in.at[1], yn),
          send(deg_own, deg_in.at[2], dg)]
    gather_last(0, gather0)
    for copy in zd:
        copy.wait_recv()
    du = (udeg[...] + udeg_in[0]) + (udeg_in[1] + udeg_in[2])
    inv = lax.rsqrt(jnp.maximum(du, 1.0))
    invu[...] = jnp.broadcast_to(inv[0:1, :], (128, users)).T
    for copy in ds:
        copy.wait_recv()
    for d in range(4):
        total = ((deg_own[d:d + 1, :] + deg_in[0, (d ^ 1):(d ^ 1) + 1, :])
                 + (deg_in[1, (d ^ 2):(d ^ 2) + 1, :] + deg_in[2, (d ^ 3):(d ^ 3) + 1, :]))
        deg_fin[d:d + 1, :] = lax.rsqrt(jnp.maximum(total, 1.0))
    df = send(deg_fin, deg_oth, partner)

    def normalize(slot):
        d = slot // 2
        inv_item = (deg_oth if slot % 2 else deg_fin)[d:d + 1, :]

        def group(i, carry):
            at = pl.multiple_of(i * 16, 16)
            scale = (invu[pl.ds(at, 16), 0:1] * inv_item).astype(BF16)
            adj[slot, pl.ds(at, 16), :] = adj[slot, pl.ds(at, 16), :] * scale
            return carry

        lax.fori_loop(0, users // 16, group, 0, unroll=2)

    def items_start(n, u, first=False, between=None):
        p = {}
        for d in (3, 1, 2, 0):
            if first:
                normalize(2 * d + 1)
            psend[n, d] = dot(u, adj[2 * d + 1], NN)
            p[d] = send(psend.at[n, d], drecv.at[n, d], partner)
        s = {}
        for d in (3, 1, 2, 0):
            if first:
                normalize(2 * d)
            part = dot(u, adj[2 * d], NN)
            p[d].wait_recv()
            sacc[n, d] = part + drecv[n, d]
            lo, hi = pl.ds(0, HALF), pl.ds(HALF, HALF)
            if d == 3:
                s['x1'] = send(sacc.at[n, 3, lo], hop1.at[n, 0], xn)
                s['y1'] = send(sacc.at[n, 3, hi], hop1.at[n, 1], yn)
                if between is not None:
                    between()
            elif d == 1:
                s['xa'] = send(sacc.at[n, 1, lo], rown.at[n, 0], xn)
            elif d == 2:
                s['yb'] = send(sacc.at[n, 2, hi], rown.at[n, 3], yn)
        return s

    def items_mid(n, s):
        lo, hi = pl.ds(0, HALF), pl.ds(HALF, HALF)
        s['x1'].wait_recv()
        sacc[n, 2, lo] = sacc[n, 2, lo] + hop1[n, 0]
        s['ya'] = send(sacc.at[n, 2, lo], rown.at[n, 2], yn)
        s['y1'].wait_recv()
        sacc[n, 1, hi] = sacc[n, 1, hi] + hop1[n, 1]
        s['xb'] = send(sacc.at[n, 1, hi], rown.at[n, 1], xn)

    def items_finish(n, s):
        for key in ('xa', 'yb', 'ya', 'xb'):
            s[key].wait_recv()
        for h, at in ((0, pl.ds(0, HALF)), (1, pl.ds(HALF, HALF))):
            total = (sacc[n, 0, at] + rown[n, h]) + rown[n, 2 + h]
            nxt = total.astype(BF16)
            isum[at] = isum[at] + nxt.astype(F32)
            if n + 1 < LAYERS:
                panel[n + 1, 0, at] = nxt

    def user_partial(n, g):
        g['p0'].wait_recv()
        g['p1'].wait_recv()
        g['p2'].wait_recv()

        def one(j, acc):
            return acc + dot(adj[j], panel[n, j], NT)

        acc = lax.fori_loop(0, 7, one, jnp.zeros((users, EMB), F32))
        g['p3'].wait_recv()
        return acc + dot(adj[7], panel[n, 7], NT)

    u0 = zgather_wait(0, zgather0)
    df.wait_recv()
    s0 = items_start(0, u0, first=True)
    z0 = zsum_start(0, user_partial(0, gather0))
    items_mid(0, s0)
    upan[1, c] = zsum_wait(0, z0)
    zg1 = zgather_start(1)
    u1 = zgather_wait(1, zg1)
    items_finish(0, s0)
    g1 = gather_start(1)
    s1 = items_start(1, u1, between=lambda: gather_forward(1, g1))
    gather_last(1, g1)
    z1 = zsum_start(1, user_partial(1, g1))
    items_mid(1, s1)
    upan[2, c] = zsum_wait(1, z1)
    zg2 = zgather_start(2)
    u2 = zgather_wait(2, zg2)
    items_finish(1, s1)
    g2 = gather_start(2)
    s2 = items_start(2, u2, between=lambda: gather_forward(2, g2))
    gather_last(2, g2)
    z2 = zsum_start(2, user_partial(2, g2))
    items_mid(2, s2)
    zsum_wait(2, z2)
    final_user = (usum[...] / (LAYERS + 1)).astype(BF16)
    fu_ref[...] = final_user
    upan[3, c] = final_user
    zg3 = zgather_start(3)
    ufin = zgather_wait(3, zg3)
    local = query_ref[...] - r * users
    chosen = (lax.broadcasted_iota(jnp.int32, (users, local.shape[1]), 0)
              == jnp.broadcast_to(local, (users, local.shape[1]))).astype(F32).astype(BF16)
    pk[0] = dot(ufin, chosen, NN).astype(BF16)
    q = send(pk.at[0], pk.at[1], partner)
    q.wait_recv()
    pk[2] = pk[0] + pk[1]
    qs = [send(pk.at[2], pk.at[3], xn), send(pk.at[2], pk.at[4], yn), send(pk.at[2], pk.at[5], dg)]
    items_finish(2, s2)
    fi_ref[...] = (isum[...] / (LAYERS + 1)).astype(BF16)
    for copy in qs:
        copy.wait_recv()
    pick_ref[...] = (pk[2] + pk[3]) + (pk[4] + pk[5])
    for copy in started:
        copy.wait_send()


def propagate(mask_blk, user_shard, item_shard, queries):
    users, items = mask_blk.shape
    width = items // 8
    per = user_shard.shape[0]
    n_query = queries.shape[0]
    vmem = pl.BlockSpec(memory_space=pltpu.VMEM)
    scratch = [
        pltpu.VMEM((8, users, width), BF16),
        pltpu.VMEM((STAGES, users // 2, width), jnp.int32),
        pltpu.VMEM((LAYERS, 8, EMB, width), BF16),
        pltpu.VMEM((LAYERS + 1, 4, EMB, per), BF16),
        pltpu.VMEM((LAYERS, 4, EMB, width), F32),
        pltpu.VMEM((LAYERS, 4, EMB, width), F32),
        pltpu.VMEM((LAYERS, 4, EMB, width), F32),
        pltpu.VMEM((LAYERS, 2, HALF, width), F32),
        pltpu.VMEM((LAYERS, 4, HALF, width), F32),
        pltpu.VMEM((EMB, width), F32),
        pltpu.VMEM((EMB, per), F32),
        pltpu.VMEM((8, 8, width), F32),
        pltpu.VMEM((users, 128), F32),
        pltpu.VMEM((4, width), F32),
        pltpu.VMEM((4, width), F32),
        pltpu.VMEM((4, width), F32),
        pltpu.VMEM((3, 4, width), F32),
        pltpu.VMEM((4, width), F32),
        pltpu.VMEM((4, width), F32),
        pltpu.VMEM((8, users), F32),
        pltpu.VMEM((3, 8, users), F32),
        pltpu.VMEM((users, 128), F32),
        pltpu.VMEM((LAYERS, 4, EMB, per), F32),
        pltpu.VMEM((LAYERS, 3, EMB, per), F32),
        pltpu.VMEM((6, EMB, n_query), BF16),
        pltpu.SemaphoreType.DMA((STAGES,)),
        pltpu.SemaphoreType.DMA((N_COPIES,)),
        pltpu.SemaphoreType.DMA((N_COPIES,)),
    ]
    return pl.pallas_call(
        kernel,
        out_shape=(jax.ShapeDtypeStruct((EMB, per), BF16),
                   jax.ShapeDtypeStruct((EMB, width), BF16),
                   jax.ShapeDtypeStruct((EMB, n_query), BF16)),
        in_specs=[pl.BlockSpec(memory_space=pl.ANY), vmem, vmem, vmem],
        out_specs=(vmem, vmem, vmem),
        scratch_shapes=scratch,
        compiler_params=pltpu.CompilerParams(
            collective_id=0, has_side_effects=True, vmem_limit_bytes=67_000_000),
        name='propagate',
    )(mask_blk, item_shard, user_shard, queries.reshape(1, n_query))


def solution(mesh):
    def device_step(mask_blk, user_shard, item_shard, queries):
        fu_t, fi_t, picked_t = propagate(mask_blk, user_shard, item_shard, queries)
        scores = dot(picked_t, fi_t, TN)
        return fu_t.T, fi_t.T, scores

    return jax.shard_map(
        device_step, mesh=mesh,
        in_specs=(P('row', 'col'), P(('row', 'col'), None), P(('col', 'row'), None), P()),
        out_specs=(P(('row', 'col'), None), P(('col', 'row'), None), P(None, ('col', 'row'))),
        check_vma=False)
```

```python
import jax
import jax.numpy as jnp
from jax import lax
from jax.experimental import pallas as pl
from jax.experimental.pallas import tpu as pltpu
from jax.sharding import PartitionSpec as P

LAYERS = 3
EMB = 64
HALF = EMB // 2
NT = (((1,), (1,)), ((), ()))
NN = (((1,), (0,)), ((), ()))
TN = (((0,), (0,)), ((), ()))
F32 = jnp.float32
BF16 = jnp.bfloat16
STAGES = 4
N_COPIES = 112


def dot(lhs, rhs, dims):
    return lax.dot_general(lhs, rhs, dims, preferred_element_type=F32)


def kernel(mask_ref, item_ref, user_ref, query_ref, fu_ref, fi_ref, pick_ref,
           adj, stage, panel, upan, psend, drecv, sacc, hop1, rown, isum, usum,
           colacc, rowacc, deg_send, deg_recv, deg_own, deg_in, deg_fin, deg_oth,
           udeg, udeg_in, invu, uacc, upart, uin, pk, qbuf, stage_sem, in_sem, send_sem, recv_sem):
    c = lax.axis_index('col')
    r = lax.axis_index('row')
    users = rowacc.shape[0]
    width = adj.shape[2]
    rows = stage.shape[1]
    per_slot = users // rows
    core, cx, cy = r % 2, (r // 2) % 2, r // 4

    def plane(d, k):
        return ((cy + d // 2) % 2) * 4 + ((cx + d % 2) % 2) * 2 + (core + k) % 2

    def zpeer(k):
        return ((c // 2 + k // 2) % 2) * 2 + (c % 2 + k % 2) % 2

    slots = {d * 2 + k: (c, plane(d, k)) for d in range(4) for k in range(2)}
    partner, xn, yn, dg = slots[1], slots[2], slots[4], slots[6]
    zn = [None] + [(zpeer(k), r) for k in (1, 2, 3)]

    started = []

    def send(src, dst, device):
        n = len(started)
        copy = pltpu.make_async_remote_copy(
            src_ref=src, dst_ref=dst, send_sem=send_sem.at[n], recv_sem=recv_sem.at[n],
            device_id=device, device_id_type=pl.DeviceIdType.MESH)
        copy.start()
        started.append(copy)
        return copy

    def mask_copy(step):
        slot = step // per_slot
        part = step % per_slot
        col = plane(slot // 2, slot % 2) * width
        return pltpu.make_async_copy(
            mask_ref.at[pl.ds(pl.multiple_of(part * rows, rows), rows),
                        pl.ds(pl.multiple_of(col, width), width)],
            stage.at[step % STAGES], stage_sem.at[step % STAGES])

    steps = 8 * per_slot
    for s in range(STAGES):
        mask_copy(jnp.int32(s)).start()

    inputs = [pltpu.make_async_copy(item_ref, panel.at[0, 0], in_sem.at[0]),
              pltpu.make_async_copy(user_ref, upan.at[0, c], in_sem.at[1]),
              pltpu.make_async_copy(query_ref, qbuf, in_sem.at[2])]
    for copy in inputs:
        copy.start()

    barrier = pltpu.get_barrier_semaphore()
    peers = (partner, xn, yn, dg, zn[1], zn[2], zn[3])
    for device in peers:
        pl.semaphore_signal(barrier, inc=1, device_id=device, device_id_type=pl.DeviceIdType.MESH)

    rowacc[...] = jnp.zeros_like(rowacc)
    colacc[...] = jnp.zeros_like(colacc)

    def gather_start(n):
        own = panel.at[n, 0]
        lo, hi = pl.ds(0, HALF), pl.ds(HALF, HALF)
        g = {}
        g['xa'] = send(own.at[lo], panel.at[n, 2, lo], xn)
        g['yb'] = send(own.at[hi], panel.at[n, 4, hi], yn)
        g['xb'] = send(own.at[hi], panel.at[n, 2, hi], xn)
        g['ya'] = send(own.at[lo], panel.at[n, 4, lo], yn)
        g['p0'] = send(own, panel.at[n, 1], partner)
        return g

    def gather_forward(n, g):
        lo, hi = pl.ds(0, HALF), pl.ds(HALF, HALF)
        g['xa'].wait_recv()
        g['da'] = send(panel.at[n, 2, lo], panel.at[n, 6, lo], yn)
        g['yb'].wait_recv()
        g['db'] = send(panel.at[n, 4, hi], panel.at[n, 6, hi], xn)

    def gather_near(n, g):
        g['xb'].wait_recv()
        g['p1'] = send(panel.at[n, 2], panel.at[n, 3], partner)
        g['ya'].wait_recv()
        g['p2'] = send(panel.at[n, 4], panel.at[n, 5], partner)

    def gather_last(n, g):
        g['da'].wait_recv()
        g['db'].wait_recv()
        g['p3'] = send(panel.at[n, 6], panel.at[n, 7], partner)

    def zgather_start(n):
        return [send(upan.at[n, c], upan.at[n, c], zn[k]) for k in (1, 2, 3)]

    def zgather_wait(n, g):
        for copy in g:
            copy.wait_recv()
        return jnp.concatenate([upan[n, k] for k in range(4)], axis=1)

    def zsum_start(n, acc):
        acc_t = acc.T
        for k in range(4):
            upart[n, k] = acc_t[:, k * 128:(k + 1) * 128]
        return [send(upart.at[n, zpeer(k)], uin.at[n, k - 1], zn[k]) for k in (1, 2, 3)]

    def zsum_wait(n, g):
        for copy in g:
            copy.wait_recv()
        total = (upart[n, c] + uin[n, 0]) + (uin[n, 1] + uin[n, 2])
        nxt = total.astype(BF16)
        usum[...] = usum[...] + nxt.astype(F32)
        return nxt

    def mask_step(step, carry):
        mask_copy(step).wait()
        slot = step // per_slot
        part = step % per_slot
        buf = step % STAGES

        def group(i, col):
            at = pl.multiple_of(i * 16, 16)
            x = stage[buf, pl.ds(at, 16), :].astype(F32)
            row = pl.multiple_of(part * rows + i * 16, 16)
            adj[slot, pl.ds(row, 16), :] = x.astype(BF16)
            lanes = x[:, :128]
            for t in range(1, width // 128):
                lanes = lanes + x[:, t * 128:(t + 1) * 128]
            rowacc[pl.ds(row, 16), :] += lanes
            return col + (x[:8] + x[8:])

        colacc[slot] += lax.fori_loop(0, rows // 16, group, jnp.zeros((8, width), F32), unroll=2)

        @pl.when(step + STAGES < steps)
        def _():
            mask_copy(step + STAGES).start()

        return carry

    with jax.named_scope('mask_a'):
        lax.fori_loop(0, steps * 3 // 8, mask_step, 0)
    with jax.named_scope('barrier'):
        pl.semaphore_wait(barrier, len(peers))
    with jax.named_scope('inputs'):
        for copy in inputs:
            copy.wait()
        gather0 = gather_start(0)
        zgather0 = zgather_start(0)
        isum[...] = panel[0, 0].astype(F32)
        usum[...] = upan[0, c].astype(F32)
    with jax.named_scope('mask_b'):
        lax.fori_loop(steps * 3 // 8, steps, mask_step, 0)

    with jax.named_scope('degrees'):
        for d in range(4):
            deg_send[d:d + 1, :] = jnp.sum(colacc[2 * d + 1], axis=0, keepdims=True)
        dp = send(deg_send, deg_recv, partner)
        udeg[...] = dot(jnp.ones((8, 128), BF16), rowacc[...].astype(BF16), NT)
        zd = [send(udeg, udeg_in.at[k - 1], zn[k]) for k in (1, 2, 3)]
        mine = jnp.concatenate(
            [jnp.sum(colacc[2 * d], axis=0, keepdims=True) for d in range(4)], axis=0)
        gather_forward(0, gather0)
        dp.wait_recv()
        deg_own[...] = mine + deg_recv[...]
        ds = [send(deg_own, deg_in.at[0], xn), send(deg_own, deg_in.at[1], yn),
              send(deg_own, deg_in.at[2], dg)]
        gather_near(0, gather0)
        for copy in zd:
            copy.wait_recv()
        du = (udeg[...] + udeg_in[0]) + (udeg_in[1] + udeg_in[2])
        inv = lax.rsqrt(jnp.maximum(du, 1.0))
        invu[...] = jnp.broadcast_to(inv[0:1, :], (128, users)).T
        for copy in ds:
            copy.wait_recv()
        for d in range(4):
            total = ((deg_own[d:d + 1, :] + deg_in[0, (d ^ 1):(d ^ 1) + 1, :])
                     + (deg_in[1, (d ^ 2):(d ^ 2) + 1, :] + deg_in[2, (d ^ 3):(d ^ 3) + 1, :]))
            deg_fin[d:d + 1, :] = lax.rsqrt(jnp.maximum(total, 1.0))
        df = send(deg_fin, deg_oth, partner)

    def normalize(slot):
        d = slot // 2
        inv_item = (deg_oth if slot % 2 else deg_fin)[d:d + 1, :]

        def group(i, carry):
            at = pl.multiple_of(i * 16, 16)
            inv_user = jnp.concatenate([invu[pl.ds(at, 16), :]] * (width // 128), axis=1)
            adj[slot, pl.ds(at, 16), :] = adj[slot, pl.ds(at, 16), :] * (inv_user * inv_item).astype(BF16)
            return carry

        lax.fori_loop(0, users // 16, group, 0, unroll=2)

    def items_out(n, d, s):
        lo, hi = pl.ds(0, HALF), pl.ds(HALF, HALF)
        if d == 3:
            s['x1'] = send(sacc.at[n, 3, lo], hop1.at[n, 0], xn)
            s['y1'] = send(sacc.at[n, 3, hi], hop1.at[n, 1], yn)
        elif d == 1:
            s['xa'] = send(sacc.at[n, 1, lo], rown.at[n, 0], xn)
        else:
            s['yb'] = send(sacc.at[n, 2, hi], rown.at[n, 3], yn)

    def items_start(n, u, first=False):
        p, s = {}, {}

        def away(d):
            if first:
                normalize(2 * d + 1)
            psend[n, d] = dot(u, adj[2 * d + 1], NN)
            p[d] = send(psend.at[n, d], drecv.at[n, d], partner)

        def near(d):
            if first:
                normalize(2 * d)
            part = dot(u, adj[2 * d], NN)
            if d:
                p[d].wait_recv()
                part = part + drecv[n, d]
            sacc[n, d] = part

        away(3)
        away(1)
        near(3)
        if first:
            items_out(n, 3, s)
        away(2)
        near(1)
        if first:
            items_out(n, 1, s)
        away(0)
        near(2)
        if first:
            items_out(n, 2, s)
        near(0)
        s['p'] = p[0]
        return s

    def items_send(n, s):
        for d in (3, 1, 2):
            items_out(n, d, s)

    def items_mid(n, s):
        lo, hi = pl.ds(0, HALF), pl.ds(HALF, HALF)
        s['x1'].wait_recv()
        sacc[n, 2, lo] = sacc[n, 2, lo] + hop1[n, 0]
        s['ya'] = send(sacc.at[n, 2, lo], rown.at[n, 2], yn)
        s['y1'].wait_recv()
        sacc[n, 1, hi] = sacc[n, 1, hi] + hop1[n, 1]
        s['xb'] = send(sacc.at[n, 1, hi], rown.at[n, 1], xn)

    def items_finish(n, s):
        for key in ('p', 'xa', 'yb', 'ya', 'xb'):
            s[key].wait_recv()
        for h, at in ((0, pl.ds(0, HALF)), (1, pl.ds(HALF, HALF))):
            total = ((sacc[n, 0, at] + drecv[n, 0, at]) + rown[n, h]) + rown[n, 2 + h]
            nxt = total.astype(BF16)
            isum[at] = isum[at] + nxt.astype(F32)
            if n + 1 < LAYERS:
                panel[n + 1, 0, at] = nxt

    def user_partial(n, g, near=True, hook=None):
        def slots(first, stride, count):
            def one(j, carry):
                at = first + stride * j
                uacc[...] += dot(adj[at], panel[n, at], NT)
                return carry

            lax.fori_loop(0, count, one, 0)

        g['p0'].wait_recv()
        uacc[...] = dot(adj[0], panel[n, 0], NT)
        slots(1, 1, 1)
        if hook is not None:
            hook()
        if near:
            gather_near(n, g)
        slots(2, 2, 2)
        g['p1'].wait_recv()
        g['p2'].wait_recv()
        slots(3, 2, 2)
        gather_last(n, g)
        slots(6, 1, 1)
        g['p3'].wait_recv()
        slots(7, 1, 1)
        return uacc[...]

    scope = jax.named_scope
    with scope('u0'):
        u0 = zgather_wait(0, zgather0)
        df.wait_recv()
    with scope('items0'):
        s0 = items_start(0, u0, first=True)
    with scope('user0'):
        z0 = zsum_start(0, user_partial(0, gather0, near=False))
    with scope('mid0'):
        items_mid(0, s0)
    with scope('zsum0'):
        upan[1, c] = zsum_wait(0, z0)
        zg1 = zgather_start(1)
    with scope('finish0'):
        items_finish(0, s0)
        g1 = gather_start(1)
    with scope('zgather1'):
        u1 = zgather_wait(1, zg1)
    with scope('items1'):
        s1 = items_start(1, u1)
        gather_forward(1, g1)
        items_send(1, s1)
    with scope('user1'):
        z1 = zsum_start(1, user_partial(1, g1))
    with scope('zsum1'):
        upan[2, c] = zsum_wait(1, z1)
        zg2 = zgather_start(2)
    with scope('mid1'):
        items_mid(1, s1)
    with scope('zgather2'):
        u2 = zgather_wait(2, zg2)
    with scope('items2'):
        s2 = items_start(2, u2)
    with scope('finish1'):
        items_finish(1, s1)
        g2 = gather_start(2)
    with scope('user2'):
        def hook():
            gather_forward(2, g2)
            items_send(2, s2)

        z2 = zsum_start(2, user_partial(2, g2, hook=hook))
    with scope('mid2'):
        items_mid(2, s2)
    with scope('zsum2'):
        zsum_wait(2, z2)
        final_user = (usum[...] / (LAYERS + 1)).astype(BF16)
        fu_ref[...] = final_user
        upan[3, c] = final_user
        zg3 = zgather_start(3)
    with scope('zgather3'):
        ufin = zgather_wait(3, zg3)
    with scope('pick'):
        local = qbuf[...] - r * users
        chosen = (lax.broadcasted_iota(jnp.int32, (users, local.shape[1]), 0)
                  == jnp.broadcast_to(local, (users, local.shape[1]))).astype(F32).astype(BF16)
        pk[0] = dot(ufin, chosen, NN).astype(BF16)
        q = send(pk.at[0], pk.at[1], partner)
        q.wait_recv()
        pk[2] = pk[0] + pk[1]
        qs = [send(pk.at[2], pk.at[3 + i], dev) for i, dev in enumerate((xn, yn, dg))]
    with scope('finish2'):
        items_finish(2, s2)
        fi_ref[...] = (isum[...] / (LAYERS + 1)).astype(BF16)
    with scope('picked'):
        for copy in qs:
            copy.wait_recv()
        pick_ref[...] = (pk[2] + pk[3]) + (pk[4] + pk[5])
    with scope('drain'):
        for copy in started:
            copy.wait_send()


def propagate(mask_blk, user_shard, item_shard, queries):
    users, items = mask_blk.shape
    width = items // 8
    per = user_shard.shape[1]
    n_query = queries.shape[0]
    vmem = pl.BlockSpec(memory_space=pltpu.VMEM)
    hbm = pl.BlockSpec(memory_space=pl.ANY)
    scratch = [
        pltpu.VMEM((8, users, width), BF16),
        pltpu.VMEM((STAGES, users // 2, width), jnp.int32),
        pltpu.VMEM((LAYERS, 8, EMB, width), BF16),
        pltpu.VMEM((LAYERS + 1, 4, EMB, per), BF16),
        pltpu.VMEM((LAYERS, 4, EMB, width), F32),
        pltpu.VMEM((LAYERS, 4, EMB, width), F32),
        pltpu.VMEM((LAYERS, 4, EMB, width), F32),
        pltpu.VMEM((LAYERS, 2, HALF, width), F32),
        pltpu.VMEM((LAYERS, 4, HALF, width), F32),
        pltpu.VMEM((EMB, width), F32),
        pltpu.VMEM((EMB, per), F32),
        pltpu.VMEM((8, 8, width), F32),
        pltpu.VMEM((users, 128), F32),
        pltpu.VMEM((4, width), F32),
        pltpu.VMEM((4, width), F32),
        pltpu.VMEM((4, width), F32),
        pltpu.VMEM((3, 4, width), F32),
        pltpu.VMEM((4, width), F32),
        pltpu.VMEM((4, width), F32),
        pltpu.VMEM((8, users), F32),
        pltpu.VMEM((3, 8, users), F32),
        pltpu.VMEM((users, 128), F32),
        pltpu.VMEM((users, EMB), F32),
        pltpu.VMEM((LAYERS, 4, EMB, per), F32),
        pltpu.VMEM((LAYERS, 3, EMB, per), F32),
        pltpu.VMEM((6, EMB, n_query), BF16),
        pltpu.VMEM((1, n_query), jnp.int32),
        pltpu.SemaphoreType.DMA((STAGES,)),
        pltpu.SemaphoreType.DMA((3,)),
        pltpu.SemaphoreType.DMA((N_COPIES,)),
        pltpu.SemaphoreType.DMA((N_COPIES,)),
    ]
    return pl.pallas_call(
        kernel,
        out_shape=(jax.ShapeDtypeStruct((EMB, per), BF16),
                   jax.ShapeDtypeStruct((EMB, width), BF16),
                   jax.ShapeDtypeStruct((EMB, n_query), BF16)),
        in_specs=[hbm, hbm, hbm, hbm],
        out_specs=(vmem, vmem, vmem),
        scratch_shapes=scratch,
        compiler_params=pltpu.CompilerParams(
            collective_id=0, has_side_effects=True, vmem_limit_bytes=67_000_000),
        name='propagate',
    )(mask_blk, item_shard, user_shard, queries.reshape(1, n_query))


def solution(mesh):
    def device_step(mask_blk, user_shard, item_shard, queries):
        fu_t, fi_t, picked_t = propagate(mask_blk, user_shard.T, item_shard.T, queries)
        scores = dot(picked_t, fi_t, TN)
        return fu_t.T, fi_t.T, scores

    return jax.shard_map(
        device_step, mesh=mesh,
        in_specs=(P('row', 'col'), P(('row', 'col'), None), P(('col', 'row'), None), P()),
        out_specs=(P(('row', 'col'), None), P(('col', 'row'), None), P(None, ('col', 'row'))),
        check_vma=False)
```

```python
import jax
import jax.numpy as jnp
from jax import lax
from jax.experimental import pallas as pl
from jax.experimental.pallas import tpu as pltpu
from jax.sharding import PartitionSpec as P

LAYERS = 3
EMB = 64
HALF = EMB // 2
QUARTER = EMB // 4
NT = (((1,), (1,)), ((), ()))
NN = (((1,), (0,)), ((), ()))
TN = (((0,), (0,)), ((), ()))
F32 = jnp.float32
BF16 = jnp.bfloat16
STAGES = 8
N_COPIES = 160


def dot(lhs, rhs, dims):
    return lax.dot_general(lhs, rhs, dims, preferred_element_type=F32)


def kernel(mask_ref, item_ref, user_ref, query_ref, fu_ref, fi_ref, pick_ref,
           adj, stage, panel, upan, psend, drecv, sacc, hop1, rown, isum, usum,
           colacc, rowacc, deg_send, deg_recv, deg_own, deg_in, deg_fin, deg_oth, far_send, far_in,
           udeg, udeg_in, invu, uacc, upart, uin, pk, qbuf, stage_sem, in_sem, send_sem, recv_sem):
    c = lax.axis_index('col')
    r = lax.axis_index('row')
    users = rowacc.shape[0]
    width = adj.shape[2]
    rows = stage.shape[1]
    per_slot = users // rows
    core, cx, cy = r % 2, (r // 2) % 2, r // 4

    def plane(d, k):
        return ((cy + d // 2) % 2) * 4 + ((cx + d % 2) % 2) * 2 + (core + k) % 2

    def zpeer(k):
        return ((c // 2 + k // 2) % 2) * 2 + (c % 2 + k % 2) % 2

    slots = {d * 2 + k: (c, plane(d, k)) for d in range(4) for k in range(2)}
    partner, xn, yn, dg = slots[1], slots[2], slots[4], slots[6]
    zn = [None] + [(zpeer(k), r) for k in (1, 2, 3)]

    started = []

    def send(src, dst, device):
        n = len(started)
        copy = pltpu.make_async_remote_copy(
            src_ref=src, dst_ref=dst, send_sem=send_sem.at[n], recv_sem=recv_sem.at[n],
            device_id=device, device_id_type=pl.DeviceIdType.MESH)
        copy.start()
        started.append(copy)
        return copy

    def mask_slot(step):
        return (step // per_slot % 4) * 2 + 1 - step // (4 * per_slot)

    def mask_copy(step):
        slot = mask_slot(step)
        part = step % per_slot
        col = plane(slot // 2, slot % 2) * width
        return pltpu.make_async_copy(
            mask_ref.at[pl.ds(pl.multiple_of(part * rows, rows), rows),
                        pl.ds(pl.multiple_of(col, width), width)],
            stage.at[step % STAGES], stage_sem.at[step % STAGES])

    steps = 8 * per_slot
    for s in range(STAGES):
        mask_copy(jnp.int32(s)).start()

    inputs = [pltpu.make_async_copy(item_ref, panel.at[0, 0], in_sem.at[0]),
              pltpu.make_async_copy(user_ref, upan.at[0, c], in_sem.at[1]),
              pltpu.make_async_copy(query_ref, qbuf, in_sem.at[2])]
    for copy in inputs:
        copy.start()

    barrier = pltpu.get_barrier_semaphore()
    peers = tuple(slots[k] for k in range(1, 8)) + (zn[1], zn[2], zn[3])
    for device in peers:
        pl.semaphore_signal(barrier, inc=1, device_id=device, device_id_type=pl.DeviceIdType.MESH)

    rowacc[...] = jnp.zeros_like(rowacc)
    colacc[...] = jnp.zeros_like(colacc)

    def piece(h, i):
        return pl.ds(h * HALF + i * QUARTER, QUARTER)

    def gather_start(n, i, g):
        own = panel.at[n, 0]
        for h in (0, 1):
            g['x', h, i] = send(own.at[piece(h, i)], panel.at[n, 2, piece(h, i)], xn)
            g['y', 1 - h, i] = send(own.at[piece(1 - h, i)], panel.at[n, 4, piece(1 - h, i)], yn)
        if i:
            g['p0'] = send(own, panel.at[n, 1], partner)

    def gather_forward(n, i, g):
        g['x', 0, i].wait_recv()
        g['d', 0, i] = send(panel.at[n, 2, piece(0, i)], panel.at[n, 6, piece(0, i)], yn)
        g['y', 1, i].wait_recv()
        g['d', 1, i] = send(panel.at[n, 4, piece(1, i)], panel.at[n, 6, piece(1, i)], xn)

    def gather_near(n, g):
        g['x', 1, 0].wait_recv()
        g['x', 1, 1].wait_recv()
        g['p1'] = send(panel.at[n, 2], panel.at[n, 3], partner)
        g['y', 0, 0].wait_recv()
        g['y', 0, 1].wait_recv()
        g['p2'] = send(panel.at[n, 4], panel.at[n, 5], partner)

    def gather_last(n, g):
        for h in (0, 1):
            for i in (0, 1):
                g['d', h, i].wait_recv()
        g['p3'] = send(panel.at[n, 6], panel.at[n, 7], partner)

    def zgather_start(n):
        return [send(upan.at[n, c], upan.at[n, c], zn[k]) for k in (3, 2, 1)]

    def zgather_wait(n, g):
        for copy in g:
            copy.wait_recv()
        return jnp.concatenate([upan[n, k] for k in range(4)], axis=1)

    def zsum_start(n, acc):
        acc_t = acc.T
        for k in range(4):
            upart[n, k] = acc_t[:, k * 128:(k + 1) * 128]
        return [send(upart.at[n, zpeer(k)], uin.at[n, k - 1], zn[k]) for k in (3, 2, 1)]

    def zsum_wait(n, g):
        for copy in g:
            copy.wait_recv()
        total = (upart[n, c] + uin[n, 0]) + (uin[n, 1] + uin[n, 2])
        nxt = total.astype(BF16)
        usum[...] = usum[...] + nxt.astype(F32)
        return nxt

    def mask_step(step, carry):
        mask_copy(step).wait()
        slot = mask_slot(step)
        part = step % per_slot
        buf = step % STAGES

        def group(i, col):
            at = pl.multiple_of(i * 16, 16)
            x = stage[buf, pl.ds(at, 16), :].astype(F32)
            row = pl.multiple_of(part * rows + i * 16, 16)
            adj[slot, pl.ds(row, 16), :] = x.astype(BF16)
            lanes = x[:, :128]
            for t in range(1, width // 128):
                lanes = lanes + x[:, t * 128:(t + 1) * 128]
            rowacc[pl.ds(row, 16), :] += lanes
            return col + (x[:8] + x[8:])

        colacc[slot] += lax.fori_loop(0, rows // 16, group, jnp.zeros((8, width), F32), unroll=2)

        @pl.when(step + STAGES < steps)
        def _():
            mask_copy(step + STAGES).start()

        return carry

    with jax.named_scope('mask_a'):
        lax.fori_loop(0, steps // 4, mask_step, 0)
    with jax.named_scope('barrier'):
        pl.semaphore_wait(barrier, len(peers))
    with jax.named_scope('inputs'):
        for copy in inputs:
            copy.wait()
        g0 = {}
        gather_start(0, 0, g0)
        gather_start(0, 1, g0)
        zgather0 = zgather_start(0)
        isum[...] = panel[0, 0].astype(F32)
        usum[...] = upan[0, c].astype(F32)
    with jax.named_scope('mask_b'):
        lax.fori_loop(steps // 4, steps * 5 // 8, mask_step, 0)
        for d in range(4):
            deg_send[d:d + 1, :] = jnp.sum(colacc[2 * d + 1], axis=0, keepdims=True)
        dp = send(deg_send, deg_recv, partner)
    with jax.named_scope('mask_c'):
        lax.fori_loop(steps * 5 // 8, steps, mask_step, 0)

    with jax.named_scope('deg_sum'):
        udeg[...] = dot(jnp.ones((8, 128), BF16), rowacc[...].astype(BF16), NT)
        zd = [send(udeg, udeg_in.at[k - 1], zn[k]) for k in (3, 2, 1)]
        mine = jnp.concatenate(
            [jnp.sum(colacc[2 * d], axis=0, keepdims=True) for d in range(4)], axis=0)
    with jax.named_scope('deg_partner'):
        dp.wait_recv()
        deg_own[...] = mine + deg_recv[...]
        ds = [send(deg_own, deg_in.at[0], xn), send(deg_own, deg_in.at[1], yn),
              send(deg_own, deg_in.at[2], dg)]
        far = []
        for d in range(4):
            far_send[d] = deg_own[d:d + 1, :]
            far.append(send(far_send.at[d], far_in.at[d], slots[2 * (3 - d) + 1]))
    with jax.named_scope('deg_users'):
        for copy in zd:
            copy.wait_recv()
        du = (udeg[...] + udeg_in[0]) + (udeg_in[1] + udeg_in[2])
        inv = lax.rsqrt(jnp.maximum(du, 1.0))
        invu[...] = jnp.broadcast_to(inv[0:1, :], (128, users)).T
    with jax.named_scope('deg_items'):
        for copy in ds:
            copy.wait_recv()
    with jax.named_scope('deg_inv'):
        for d in range(4):
            total = ((deg_own[d:d + 1, :] + deg_in[0, (d ^ 1):(d ^ 1) + 1, :])
                     + (deg_in[1, (d ^ 2):(d ^ 2) + 1, :] + deg_in[2, (d ^ 3):(d ^ 3) + 1, :]))
            deg_fin[d:d + 1, :] = lax.rsqrt(jnp.maximum(total, 1.0))
        df = send(deg_fin, deg_oth, partner)
        for copy in far:
            copy.wait_recv()
        for i in (0, 1):
            gather_forward(0, i, g0)
        gather_near(0, g0)

    def normalize(slot, at=0, size=width):
        d = slot // 2
        cols = pl.ds(at, size)
        if slot == 7:
            total = (far_in[3, :, cols] + far_in[2, :, cols]) + (far_in[1, :, cols] + far_in[0, :, cols])
            inv_item = lax.rsqrt(jnp.maximum(total, 1.0))
        else:
            inv_item = (deg_oth if slot % 2 else deg_fin)[d:d + 1, cols]

        def group(i, carry):
            row = pl.ds(pl.multiple_of(i * 16, 16), 16)
            inv_user = jnp.concatenate([invu[row, :]] * (size // 128), axis=1)
            adj[slot, row, cols] = adj[slot, row, cols] * (inv_user * inv_item).astype(BF16)
            return carry

        lax.fori_loop(0, users // 16, group, 0, unroll=2)

    halves = (pl.ds(0, width // 2), pl.ds(width // 2, width // 2))

    def items_diagonal(n, i, s):
        cols = halves[i]
        lo, hi = pl.ds(0, HALF), pl.ds(HALF, HALF)
        s['x1', i] = send(sacc.at[n, 3, lo, cols], hop1.at[n, 0, :, cols], xn)
        s['y1', i] = send(sacc.at[n, 3, hi, cols], hop1.at[n, 1, :, cols], yn)

    def items_direct(n, s):
        s['xa'] = send(sacc.at[n, 1, pl.ds(0, HALF)], rown.at[n, 0], xn)
        s['yb'] = send(sacc.at[n, 2, pl.ds(HALF, HALF)], rown.at[n, 3], yn)

    def items_start(n, u, s, first=False, hooks=()):
        p = {}

        def away(d):
            if first:
                normalize(2 * d + 1)
            psend[n, d] = dot(u, adj[2 * d + 1], NN)
            p[d] = send(psend.at[n, d], drecv.at[n, d], partner)

        def near(d):
            if first:
                normalize(2 * d)
            part = dot(u, adj[2 * d], NN)
            if d:
                p[d].wait_recv()
                part = part + drecv[n, d]
            sacc[n, d] = part

        if first:
            for i, cols in enumerate(halves):
                normalize(7, i * (width // 2), width // 2)
                psend[n, 3, :, cols] = dot(u, adj[7, :, cols], NN)
                p[3, i] = send(psend.at[n, 3, :, cols], drecv.at[n, 3, :, cols], partner)
            for i, cols in enumerate(halves):
                normalize(6, i * (width // 2), width // 2)
                own = dot(u, adj[6, :, cols], NN)
                p[3, i].wait_recv()
                sacc[n, 3, :, cols] = own + drecv[n, 3, :, cols]
                items_diagonal(n, i, s)
            df.wait_recv()
            away(1)
            away(2)
            near(1)
            s['xa'] = send(sacc.at[n, 1, pl.ds(0, HALF)], rown.at[n, 0], xn)
            away(0)
            near(2)
            s['yb'] = send(sacc.at[n, 2, pl.ds(HALF, HALF)], rown.at[n, 3], yn)
            near(0)
        else:
            away(3)
            away(1)
            hooks[0]()
            near(3)
            hooks[1]()
            away(2)
            away(0)
            near(1)
            hooks[2]()
            near(2)
            near(0)
            hooks[3]()
        s['p'] = p[0]

    def items_mid(n, s):
        for i in (0, 1):
            s['x1', i].wait_recv()
            s['y1', i].wait_recv()
        for i in (0, 1):
            at = pl.ds(i * QUARTER, QUARTER)
            sacc[n, 2, piece(0, i)] = sacc[n, 2, piece(0, i)] + hop1[n, 0, at]
            s['ya', i] = send(sacc.at[n, 2, piece(0, i)], rown.at[n, 2, at], yn)
            sacc[n, 1, piece(1, i)] = sacc[n, 1, piece(1, i)] + hop1[n, 1, at]
            s['xb', i] = send(sacc.at[n, 1, piece(1, i)], rown.at[n, 1, at], xn)

    def items_finish(n, i, s):
        if i == 0:
            for key in ('p', 'xa', 'yb'):
                s[key].wait_recv()
        s['ya', i].wait_recv()
        s['xb', i].wait_recv()
        at = pl.ds(i * QUARTER, QUARTER)
        for h in (0, 1):
            rows_h = piece(h, i)
            total = ((sacc[n, 0, rows_h] + drecv[n, 0, rows_h]) + rown[n, h, at]) + rown[n, 2 + h, at]
            nxt = total.astype(BF16)
            isum[rows_h] = isum[rows_h] + nxt.astype(F32)
            if n + 1 < LAYERS:
                panel[n + 1, 0, rows_h] = nxt

    def user_partial(n, g, near=True, hook=None):
        def slots(first, stride, count):
            def one(j, carry):
                at = first + stride * j
                uacc[...] += dot(adj[at], panel[n, at], NT)
                return carry

            lax.fori_loop(0, count, one, 0)

        g['p0'].wait_recv()
        uacc[...] = dot(adj[0], panel[n, 0], NT)
        slots(1, 1, 1)
        if near:
            gather_near(n, g)
        slots(2, 2, 2)
        g['p1'].wait_recv()
        g['p2'].wait_recv()
        slots(3, 2, 2)
        if hook is not None:
            hook()
        gather_last(n, g)
        slots(6, 1, 1)
        g['p3'].wait_recv()
        slots(7, 1, 1)
        return uacc[...]

    scope = jax.named_scope

    def finish(n, i, s, g):
        with scope(f'finish{n}{i}'):
            items_finish(n, i, s)
            gather_start(n + 1, i, g)

    def forward(n, i, g):
        with scope(f'forward{n}{i}'):
            gather_forward(n, i, g)

    def nothing():
        pass

    with scope('u0'):
        u0 = zgather_wait(0, zgather0)
    with scope('items0'):
        s0 = {}
        items_start(0, u0, s0, first=True)
    with scope('user0'):
        z0 = zsum_start(0, user_partial(0, g0, near=False, hook=lambda: items_mid(0, s0)))
    g1, g2 = {}, {}
    finish(0, 0, s0, g1)
    with scope('zsum0'):
        upan[1, c] = zsum_wait(0, z0)
        zg1 = zgather_start(1)
    finish(0, 1, s0, g1)
    with scope('zgather1'):
        u1 = zgather_wait(1, zg1)
    with scope('items1'):
        def launch1():
            forward(1, 1, g1)
            items_diagonal(1, 0, s1)
            items_diagonal(1, 1, s1)

        forward(1, 0, g1)
        s1 = {}
        items_start(1, u1, s1, hooks=(nothing, launch1, nothing, nothing))
        items_direct(1, s1)
    with scope('user1'):
        z1 = zsum_start(1, user_partial(1, g1))
    with scope('mid1'):
        items_mid(1, s1)
    with scope('zsum1'):
        upan[2, c] = zsum_wait(1, z1)
        zg2 = zgather_start(2)
    with scope('zgather2'):
        u2 = zgather_wait(2, zg2)
    with scope('items2'):
        s2 = {}
        items_start(2, u2, s2, hooks=(lambda: finish(1, 0, s1, g2), lambda: finish(1, 1, s1, g2),
                                      lambda: forward(2, 0, g2), nothing))
        forward(2, 1, g2)
        items_diagonal(2, 0, s2)
        items_diagonal(2, 1, s2)
        items_direct(2, s2)
    with scope('user2'):
        z2 = zsum_start(2, user_partial(2, g2))
    with scope('mid2'):
        items_mid(2, s2)
    with scope('zsum2'):
        zsum_wait(2, z2)
        final_user = (usum[...] / (LAYERS + 1)).astype(BF16)
        fu_ref[...] = final_user
        upan[3, c] = final_user
        zg3 = zgather_start(3)
    with scope('zgather3'):
        ufin = zgather_wait(3, zg3)
    with scope('pick'):
        local = qbuf[...] - r * users
        chosen = (lax.broadcasted_iota(jnp.int32, (users, local.shape[1]), 0)
                  == jnp.broadcast_to(local, (users, local.shape[1]))).astype(F32).astype(BF16)
        pk[0] = dot(ufin, chosen, NN).astype(BF16)
        q = send(pk.at[0], pk.at[1], partner)
        q.wait_recv()
        pk[2] = pk[0] + pk[1]
        qs = [send(pk.at[2], pk.at[3 + i], dev) for i, dev in enumerate((xn, yn, dg))]
    with scope('finish2'):
        items_finish(2, 0, s2)
        items_finish(2, 1, s2)
        fi_ref[...] = (isum[...] / (LAYERS + 1)).astype(BF16)
    with scope('picked'):
        for copy in qs:
            copy.wait_recv()
        pick_ref[...] = (pk[2] + pk[3]) + (pk[4] + pk[5])
    with scope('drain'):
        for copy in started:
            copy.wait_send()


def propagate(mask_blk, user_shard, item_shard, queries):
    users, items = mask_blk.shape
    width = items // 8
    per = user_shard.shape[1]
    n_query = queries.shape[0]
    vmem = pl.BlockSpec(memory_space=pltpu.VMEM)
    hbm = pl.BlockSpec(memory_space=pl.ANY)
    scratch = [
        pltpu.VMEM((8, users, width), BF16),
        pltpu.VMEM((STAGES, users // 4, width), jnp.int32),
        pltpu.VMEM((LAYERS, 8, EMB, width), BF16),
        pltpu.VMEM((LAYERS + 1, 4, EMB, per), BF16),
        pltpu.VMEM((LAYERS, 4, EMB, width), F32),
        pltpu.VMEM((LAYERS, 4, EMB, width), F32),
        pltpu.VMEM((LAYERS, 4, EMB, width), F32),
        pltpu.VMEM((LAYERS, 2, HALF, width), F32),
        pltpu.VMEM((LAYERS, 4, HALF, width), F32),
        pltpu.VMEM((EMB, width), F32),
        pltpu.VMEM((EMB, per), F32),
        pltpu.VMEM((8, 8, width), F32),
        pltpu.VMEM((users, 128), F32),
        pltpu.VMEM((4, width), F32),
        pltpu.VMEM((4, width), F32),
        pltpu.VMEM((4, width), F32),
        pltpu.VMEM((3, 4, width), F32),
        pltpu.VMEM((4, width), F32),
        pltpu.VMEM((4, width), F32),
        pltpu.VMEM((4, 1, width), F32),
        pltpu.VMEM((4, 1, width), F32),
        pltpu.VMEM((8, users), F32),
        pltpu.VMEM((3, 8, users), F32),
        pltpu.VMEM((users, 128), F32),
        pltpu.VMEM((users, EMB), F32),
        pltpu.VMEM((LAYERS, 4, EMB, per), F32),
        pltpu.VMEM((LAYERS, 3, EMB, per), F32),
        pltpu.VMEM((6, EMB, n_query), BF16),
        pltpu.VMEM((1, n_query), jnp.int32),
        pltpu.SemaphoreType.DMA((STAGES,)),
        pltpu.SemaphoreType.DMA((3,)),
        pltpu.SemaphoreType.DMA((N_COPIES,)),
        pltpu.SemaphoreType.DMA((N_COPIES,)),
    ]
    return pl.pallas_call(
        kernel,
        out_shape=(pltpu.VMEM((EMB, per), BF16),
                   pltpu.VMEM((EMB, width), BF16),
                   pltpu.VMEM((EMB, n_query), BF16)),
        in_specs=[hbm, hbm, hbm, hbm],
        out_specs=(vmem, vmem, vmem),
        scratch_shapes=scratch,
        compiler_params=pltpu.CompilerParams(
            collective_id=0, has_side_effects=True, vmem_limit_bytes=61_600_000),
        name='propagate',
    )(mask_blk, item_shard, user_shard, queries.reshape(1, n_query))


def output_kernel(pick_ref, item_ref, user_ref, scores_ref, fi_ref, fu_ref, scores, sem):
    copies = [pltpu.make_async_copy(item_ref, fi_ref, sem.at[0]),
              pltpu.make_async_copy(user_ref, fu_ref, sem.at[1])]
    for copy in copies:
        copy.start()
    picked = pick_ref[...].astype(F32).T.astype(BF16)
    cols = scores.shape[1] // 4
    for i in range(4):
        at = pl.ds(i * cols, cols)
        scores[:, at] = dot(picked, item_ref[:, at], NN)
        copy = pltpu.make_async_copy(scores.at[:, at], scores_ref.at[:, at], sem.at[2 + i])
        copy.start()
        copies.append(copy)
    for copy in copies:
        copy.wait()


def outputs(fu_t, fi_t, picked_t):
    n_query = picked_t.shape[1]
    width, per = fi_t.shape[1], fu_t.shape[1]
    hbm = pl.BlockSpec(memory_space=pl.ANY)
    vmem = pl.BlockSpec(memory_space=pltpu.VMEM)
    args = [pltpu.with_memory_space_constraint(x, pltpu.VMEM) for x in (picked_t, fi_t, fu_t)]
    return pl.pallas_call(
        output_kernel,
        out_shape=(jax.ShapeDtypeStruct((n_query, width), F32),
                   jax.ShapeDtypeStruct((EMB, width), BF16),
                   jax.ShapeDtypeStruct((EMB, per), BF16)),
        in_specs=[vmem, vmem, vmem],
        out_specs=(hbm, hbm, hbm),
        scratch_shapes=[pltpu.VMEM((n_query, width), F32), pltpu.SemaphoreType.DMA((6,))],
        name='outputs',
    )(*args)


def solution(mesh):
    def device_step(mask_blk, user_shard, item_shard, queries):
        fu_t, fi_t, picked_t = propagate(mask_blk, user_shard.T, item_shard.T, queries)
        scores, fi_t, fu_t = outputs(fu_t, fi_t, picked_t)
        return fu_t.T, fi_t.T, scores

    return jax.shard_map(
        device_step, mesh=mesh,
        in_specs=(P('row', 'col'), P(('row', 'col'), None), P(('col', 'row'), None), P()),
        out_specs=(P(('row', 'col'), None), P(('col', 'row'), None), P(None, ('col', 'row'))),
        check_vma=False)
```

```python
import jax
import jax.numpy as jnp
from jax import lax
from jax.experimental import pallas as pl
from jax.experimental.pallas import tpu as pltpu
from jax.sharding import PartitionSpec as P

LAYERS = 3
EMB = 64
HALF = EMB // 2
QUARTER = EMB // 4
NT = (((1,), (1,)), ((), ()))
NN = (((1,), (0,)), ((), ()))
TN = (((0,), (0,)), ((), ()))
F32 = jnp.float32
BF16 = jnp.bfloat16
STAGES = 8
N_SENT = 24
N_GOT = 61


def dot(lhs, rhs, dims):
    return lax.dot_general(lhs, rhs, dims, preferred_element_type=F32)


def kernel(mask_ref, item_ref, user_ref, query_ref, fu_ref, fi_ref, pick_ref,
           adj, stage, panel, upan, psend, drecv, sacc, hop1, rown, isum, usum,
           colacc, rowacc, deg_send, deg_recv, deg_own, deg_in, deg_fin, deg_oth, far_send, far_in,
           udeg, udeg_in, invu, uacc, upart, uin, pk, qbuf, stage_sem, in_sem, send_sem, recv_sem):
    c = lax.axis_index('col')
    r = lax.axis_index('row')
    users = rowacc.shape[0]
    width = adj.shape[2]
    rows = stage.shape[1]
    per_slot = users // rows
    core, cx, cy = r % 2, (r // 2) % 2, r // 4

    def plane(d, k):
        return ((cy + d // 2) % 2) * 4 + ((cx + d % 2) % 2) * 2 + (core + k) % 2

    def zpeer(k):
        return ((c // 2 + k // 2) % 2) * 2 + (c % 2 + k % 2) % 2

    slots = {d * 2 + k: (c, plane(d, k)) for d in range(4) for k in range(2)}
    partner, xn, yn, dg = slots[1], slots[2], slots[4], slots[6]
    zn = [None] + [(zpeer(k), r) for k in (1, 2, 3)]

    got_index, out_index = {}, {}

    def send(src, dst, device, got, out):
        copy = pltpu.make_async_remote_copy(
            src_ref=src, dst_ref=dst,
            send_sem=send_sem.at[out_index.setdefault(out, len(out_index))],
            recv_sem=recv_sem.at[got_index.setdefault(got, len(got_index))],
            device_id=device, device_id_type=pl.DeviceIdType.MESH)
        copy.start()

    def group(whole, got, out):
        return pltpu.make_async_remote_copy(
            src_ref=whole, dst_ref=whole, send_sem=send_sem.at[out], recv_sem=recv_sem.at[got],
            device_id=partner, device_id_type=pl.DeviceIdType.MESH)

    def arrived(got, whole):
        group(whole, got_index[got], 0).wait_recv()

    def sent(out, whole):
        group(whole, 0, out_index[out]).wait_send()

    def mask_slot(step):
        return (step // per_slot % 4) * 2 + 1 - step // (4 * per_slot)

    def mask_copy(step):
        slot = mask_slot(step)
        part = step % per_slot
        col = plane(slot // 2, slot % 2) * width
        return pltpu.make_async_copy(
            mask_ref.at[pl.ds(pl.multiple_of(part * rows, rows), rows),
                        pl.ds(pl.multiple_of(col, width), width)],
            stage.at[step % STAGES], stage_sem.at[step % STAGES])

    steps = 8 * per_slot
    for s in range(STAGES):
        mask_copy(jnp.int32(s)).start()

    inputs = [pltpu.make_async_copy(item_ref, panel.at[0, 0], in_sem.at[0]),
              pltpu.make_async_copy(user_ref, upan.at[0, c], in_sem.at[1]),
              pltpu.make_async_copy(query_ref, qbuf, in_sem.at[2])]
    for copy in inputs:
        copy.start()

    barrier = pltpu.get_barrier_semaphore()
    peers = tuple(slots[k] for k in range(1, 8)) + (zn[1], zn[2], zn[3])
    for device in peers:
        pl.semaphore_signal(barrier, inc=1, device_id=device, device_id_type=pl.DeviceIdType.MESH)

    rowacc[...] = jnp.zeros_like(rowacc)
    colacc[...] = jnp.zeros_like(colacc)

    def piece(h, i):
        return pl.ds(h * HALF + i * QUARTER, QUARTER)

    def gather_start(n, i):
        own = panel.at[n, 0]
        for h in (0, 1):
            got = ('forward', n, i) if h == 0 else ('near', n)
            at, to = piece(h, i), piece(1 - h, i)
            send(own.at[at], panel.at[n, 2, at], xn, got, ('gather', n))
            send(own.at[to], panel.at[n, 4, to], yn, got, ('gather', n))
        if i:
            send(own, panel.at[n, 1], partner, ('p0', n), ('gather', n))

    def gather_forward(n, i):
        arrived(('forward', n, i), panel.at[n, 2, pl.ds(0, HALF)])
        at, to = piece(0, i), piece(1, i)
        send(panel.at[n, 2, at], panel.at[n, 6, at], yn, ('last', n), ('gather', n))
        send(panel.at[n, 4, to], panel.at[n, 6, to], xn, ('last', n), ('gather', n))

    def gather_near(n):
        arrived(('near', n), panel.at[n, 2])
        send(panel.at[n, 2], panel.at[n, 3], partner, ('p12', n), ('gather', n))
        send(panel.at[n, 4], panel.at[n, 5], partner, ('p12', n), ('gather', n))

    def gather_last(n):
        arrived(('last', n), panel.at[n, 6])
        send(panel.at[n, 6], panel.at[n, 7], partner, ('p3', n), ('gather', n))

    def zgather_start(n):
        for k in (3, 2, 1):
            send(upan.at[n, c], upan.at[n, c], zn[k], ('zgather', n), ('zgather', n))

    def zgather_wait(n):
        arrived(('zgather', n), upan.at[n, pl.ds(0, 3)])
        return jnp.concatenate([upan[n, k] for k in range(4)], axis=1)

    def zsum_start(n, acc):
        acc_t = acc.T
        for k in range(4):
            upart[n, k] = acc_t[:, k * 128:(k + 1) * 128]
        for k in (3, 2, 1):
            send(upart.at[n, zpeer(k)], uin.at[n, k - 1], zn[k], ('zsum', n), ('zsum', n))

    def zsum_wait(n):
        arrived(('zsum', n), uin.at[n])
        total = (upart[n, c] + uin[n, 0]) + (uin[n, 1] + uin[n, 2])
        nxt = total.astype(BF16)
        usum[...] = usum[...] + nxt.astype(F32)
        return nxt

    def mask_step(step, carry):
        mask_copy(step).wait()
        slot = mask_slot(step)
        part = step % per_slot
        buf = step % STAGES

        def convert(i, col):
            at = pl.multiple_of(i * 16, 16)
            x = stage[buf, pl.ds(at, 16), :].astype(F32)
            row = pl.multiple_of(part * rows + i * 16, 16)
            adj[slot, pl.ds(row, 16), :] = x.astype(BF16)
            lanes = x[:, :128]
            for t in range(1, width // 128):
                lanes = lanes + x[:, t * 128:(t + 1) * 128]
            rowacc[pl.ds(row, 16), :] += lanes
            return col + (x[:8] + x[8:])

        colacc[slot] += lax.fori_loop(0, rows // 16, convert, jnp.zeros((8, width), F32), unroll=2)

        @pl.when(step + STAGES < steps)
        def _():
            mask_copy(step + STAGES).start()

        return carry

    with jax.named_scope('mask_a'):
        lax.fori_loop(0, steps // 4, mask_step, 0)
    with jax.named_scope('barrier'):
        pl.semaphore_wait(barrier, len(peers))
    with jax.named_scope('inputs'):
        for copy in inputs:
            copy.wait()
        gather_start(0, 0)
        gather_start(0, 1)
        zgather_start(0)
        isum[...] = panel[0, 0].astype(F32)
        usum[...] = upan[0, c].astype(F32)
    with jax.named_scope('mask_b'):
        lax.fori_loop(steps // 4, steps * 5 // 8, mask_step, 0)
        for d in range(4):
            deg_send[d:d + 1, :] = jnp.sum(colacc[2 * d + 1], axis=0, keepdims=True)
        send(deg_send, deg_recv, partner, 'dp', 'dp')
    with jax.named_scope('mask_c'):
        lax.fori_loop(steps * 5 // 8, steps, mask_step, 0)

    with jax.named_scope('deg_sum'):
        udeg[...] = dot(jnp.ones((8, 128), BF16), rowacc[...].astype(BF16), NT)
        for k in (3, 2, 1):
            send(udeg, udeg_in.at[k - 1], zn[k], 'zd', 'zd')
        mine = jnp.concatenate(
            [jnp.sum(colacc[2 * d], axis=0, keepdims=True) for d in range(4)], axis=0)
    with jax.named_scope('deg_partner'):
        arrived('dp', deg_recv)
        deg_own[...] = mine + deg_recv[...]
        for k, device in enumerate((xn, yn, dg)):
            send(deg_own, deg_in.at[k], device, 'ds', 'ds')
        for d in range(4):
            far_send[d] = deg_own[d:d + 1, :]
            send(far_send.at[d], far_in.at[d], slots[2 * (3 - d) + 1], 'far', 'far')
    with jax.named_scope('deg_users'):
        arrived('zd', udeg_in)
        du = (udeg[...] + udeg_in[0]) + (udeg_in[1] + udeg_in[2])
        inv = lax.rsqrt(jnp.maximum(du, 1.0))
        invu[...] = jnp.broadcast_to(inv[0:1, :], (128, users)).T
    with jax.named_scope('deg_items'):
        arrived('ds', deg_in)
    with jax.named_scope('deg_inv'):
        for d in range(4):
            total = ((deg_own[d:d + 1, :] + deg_in[0, (d ^ 1):(d ^ 1) + 1, :])
                     + (deg_in[1, (d ^ 2):(d ^ 2) + 1, :] + deg_in[2, (d ^ 3):(d ^ 3) + 1, :]))
            deg_fin[d:d + 1, :] = lax.rsqrt(jnp.maximum(total, 1.0))
        send(deg_fin, deg_oth, partner, 'df', 'df')
        arrived('far', far_in)
        for i in (0, 1):
            gather_forward(0, i)
        gather_near(0)

    def normalize(slot, at=0, size=width):
        d = slot // 2
        cols = pl.ds(at, size)
        if slot == 7:
            total = (far_in[3, :, cols] + far_in[2, :, cols]) + (far_in[1, :, cols] + far_in[0, :, cols])
            inv_item = lax.rsqrt(jnp.maximum(total, 1.0))
        else:
            inv_item = (deg_oth if slot % 2 else deg_fin)[d:d + 1, cols]

        def scale(i, carry):
            row = pl.ds(pl.multiple_of(i * 16, 16), 16)
            inv_user = jnp.concatenate([invu[row, :]] * (size // 128), axis=1)
            adj[slot, row, cols] = adj[slot, row, cols] * (inv_user * inv_item).astype(BF16)
            return carry

        lax.fori_loop(0, users // 16, scale, 0, unroll=2)

    starts = (0, width // 4)
    sizes = (width // 4, width - width // 4)
    splits = [pl.ds(at, size) for at, size in zip(starts, sizes)]
    lo, hi = pl.ds(0, HALF), pl.ds(HALF, HALF)

    def items_diagonal(n, i):
        cols = splits[i]
        send(sacc.at[n, 3, lo, cols], hop1.at[n, 0, :, cols], xn, ('hop1', n), ('sum', n))
        send(sacc.at[n, 3, hi, cols], hop1.at[n, 1, :, cols], yn, ('hop1', n), ('sum', n))

    def items_x(n):
        send(sacc.at[n, 1, lo], rown.at[n, 0], xn, ('direct', n), ('sum', n))

    def items_y(n):
        send(sacc.at[n, 2, hi], rown.at[n, 3], yn, ('direct', n), ('sum', n))

    def away(n, u, d):
        psend[n, d] = dot(u, adj[2 * d + 1], NN)
        send(psend.at[n, d], drecv.at[n, d], partner, ('partner', n, d), ('items', n))

    def near(n, u, d):
        part = dot(u, adj[2 * d], NN)
        if d:
            arrived(('partner', n, d), drecv.at[n, d])
            part = part + drecv[n, d]
        sacc[n, d] = part

    def items_first(u):
        for i, cols in enumerate(splits):
            normalize(7, starts[i], sizes[i])
            psend[0, 3, :, cols] = dot(u, adj[7, :, cols], NN)
            send(psend.at[0, 3, :, cols], drecv.at[0, 3, :, cols], partner, ('partner', 0, 3, i), ('items', 0))
        for i, cols in enumerate(splits):
            normalize(6, starts[i], sizes[i])
            own = dot(u, adj[6, :, cols], NN)
            arrived(('partner', 0, 3, i), drecv.at[0, 3, :, cols])
            sacc[0, 3, :, cols] = own + drecv[0, 3, :, cols]
            items_diagonal(0, i)
        arrived('df', deg_oth)

        def both(slot, step, d):
            normalize(slot)
            step(0, u, d)

        both(3, away, 1)
        both(5, away, 2)
        both(2, near, 1)
        items_x(0)
        both(1, away, 0)
        both(4, near, 2)
        items_y(0)
        both(0, near, 0)

    def items_later(n, u, hooks):
        away(n, u, 3)
        away(n, u, 1)
        hooks[0]()
        near(n, u, 3)
        hooks[1]()
        away(n, u, 2)
        away(n, u, 0)
        near(n, u, 1)
        hooks[2]()
        near(n, u, 2)
        near(n, u, 0)

    def items_mid(n, i):
        if i == 0:
            arrived(('hop1', n), hop1.at[n])
        at = pl.ds(i * QUARTER, QUARTER)
        sacc[n, 2, piece(0, i)] = sacc[n, 2, piece(0, i)] + hop1[n, 0, at]
        send(sacc.at[n, 2, piece(0, i)], rown.at[n, 2, at], yn, ('hop2', n, i), ('sum', n))
        sacc[n, 1, piece(1, i)] = sacc[n, 1, piece(1, i)] + hop1[n, 1, at]
        send(sacc.at[n, 1, piece(1, i)], rown.at[n, 1, at], xn, ('hop2', n, i), ('sum', n))

    def items_finish(n, i):
        if i == 0:
            arrived(('partner', n, 0), drecv.at[n, 0])
            arrived(('direct', n), rown.at[n, pl.ds(0, 2)])
        arrived(('hop2', n, i), rown.at[n, 0])
        at = pl.ds(i * QUARTER, QUARTER)
        for h in (0, 1):
            rows_h = piece(h, i)
            total = ((sacc[n, 0, rows_h] + drecv[n, 0, rows_h]) + rown[n, h, at]) + rown[n, 2 + h, at]
            nxt = total.astype(BF16)
            isum[rows_h] = isum[rows_h] + nxt.astype(F32)
            if n + 1 < LAYERS:
                panel[n + 1, 0, rows_h] = nxt

    def user_partial(n, near_done=False, hook=None):
        def some(first, stride, count):
            def one(j, carry):
                at = first + stride * j
                uacc[...] += dot(adj[at], panel[n, at], NT)
                return carry

            lax.fori_loop(0, count, one, 0)

        arrived(('p0', n), panel.at[n, 1])
        uacc[...] = dot(adj[0], panel[n, 0], NT)
        some(1, 1, 1)
        if not near_done:
            gather_near(n)
        some(2, 2, 2)
        arrived(('p12', n), panel.at[n, pl.ds(2, 2)])
        some(3, 2, 2)
        if hook is not None:
            hook()
        gather_last(n)
        some(6, 1, 1)
        arrived(('p3', n), panel.at[n, 7])
        some(7, 1, 1)
        return uacc[...]

    scope = jax.named_scope

    def mid(n):
        items_mid(n, 0)
        items_mid(n, 1)

    def finish(n, i):
        with scope(f'finish{n}{i}'):
            items_finish(n, i)
            gather_start(n + 1, i)

    def forward(n, i):
        with scope(f'forward{n}{i}'):
            gather_forward(n, i)

    def launch1():
        forward(1, 1)
        items_diagonal(1, 0)
        items_diagonal(1, 1)

    def nothing():
        pass

    pick_all = pk.at[pl.ds(3, 3), lo]
    with scope('u0'):
        u0 = zgather_wait(0)
    with scope('items0'):
        items_first(u0)
    with scope('user0'):
        zsum_start(0, user_partial(0, near_done=True, hook=lambda: mid(0)))
    finish(0, 0)
    with scope('zsum0'):
        upan[1, c] = zsum_wait(0)
        zgather_start(1)
    finish(0, 1)
    with scope('zgather1'):
        u1 = zgather_wait(1)
    with scope('items1'):
        forward(1, 0)
        items_later(1, u1, (nothing, launch1, nothing))
        items_x(1)
        items_y(1)
    with scope('user1'):
        zsum_start(1, user_partial(1))
    with scope('mid1'):
        mid(1)
    with scope('zsum1'):
        upan[2, c] = zsum_wait(1)
        zgather_start(2)
    with scope('zgather2'):
        u2 = zgather_wait(2)
    with scope('items2'):
        items_later(2, u2, (lambda: finish(1, 0), lambda: finish(1, 1), lambda: forward(2, 0)))
        forward(2, 1)
        items_diagonal(2, 0)
        items_diagonal(2, 1)
        items_x(2)
        items_y(2)
    with scope('user2'):
        zsum_start(2, user_partial(2))
    with scope('mid2'):
        items_mid(2, 0)
    with scope('zsum2'):
        zsum_wait(2)
        final_user = (usum[...] / (LAYERS + 1)).astype(BF16)
        fu_ref[...] = final_user
        upan[3, c] = final_user
        zgather_start(3)
    with scope('zgather3'):
        ufin = zgather_wait(3)
    with scope('pick'):
        local = qbuf[...] - r * users
        chosen = (lax.broadcasted_iota(jnp.int32, (users, local.shape[1]), 0)
                  == jnp.broadcast_to(local, (users, local.shape[1]))).astype(F32).astype(BF16)
        pk[0] = dot(ufin, chosen, NN).astype(BF16)
        send(pk.at[0], pk.at[1], partner, 'pick', 'pick')
        arrived('pick', pk.at[1])
        pk[2] = pk[0] + pk[1]
        mine = pl.ds(pl.multiple_of(core * HALF, HALF), HALF)
        for k, device in enumerate((xn, yn, dg)):
            send(pk.at[2, mine], pk.at[3 + k, mine], device, 'picks', 'picks')
        items_mid(2, 1)
    with scope('finish20'):
        items_finish(2, 0)
    with scope('picked'):
        arrived('picks', pick_all)
        pk[6, mine] = (pk[2, mine] + pk[3, mine]) + (pk[4, mine] + pk[5, mine])
        send(pk.at[6, mine], pk.at[6, mine], partner, 'picked', 'picked')
    with scope('finish21'):
        items_finish(2, 1)
        fi_ref[...] = (isum[...] / (LAYERS + 1)).astype(BF16)
    with scope('pick_half'):
        arrived('picked', pk.at[6, lo])
        pick_ref[...] = pk[6]
    with scope('drain'):
        for n in range(LAYERS):
            sent(('gather', n), panel.at[n, pl.ds(0, 7)])
            sent(('items', n), psend.at[n])
            sent(('sum', n), sacc.at[n, pl.ds(1, 3)])
            sent(('zsum', n), uin.at[n])
        for n in range(LAYERS + 1):
            sent(('zgather', n), upan.at[n, pl.ds(0, 3)])
        for out, whole in (('dp', deg_send), ('zd', udeg_in), ('ds', deg_in), ('far', far_in),
                           ('df', deg_fin), ('pick', pk.at[0]), ('picks', pick_all), ('picked', pk.at[6, lo])):
            sent(out, whole)


def propagate(mask_blk, user_shard, item_shard, queries):
    users, items = mask_blk.shape
    width = items // 8
    per = user_shard.shape[1]
    n_query = queries.shape[0]
    vmem = pl.BlockSpec(memory_space=pltpu.VMEM)
    hbm = pl.BlockSpec(memory_space=pl.ANY)
    scratch = [
        pltpu.VMEM((8, users, width), BF16),
        pltpu.VMEM((STAGES, users // 4, width), jnp.int32),
        pltpu.VMEM((LAYERS, 8, EMB, width), BF16),
        pltpu.VMEM((LAYERS + 1, 4, EMB, per), BF16),
        pltpu.VMEM((LAYERS, 4, EMB, width), F32),
        pltpu.VMEM((LAYERS, 4, EMB, width), F32),
        pltpu.VMEM((LAYERS, 4, EMB, width), F32),
        pltpu.VMEM((LAYERS, 2, HALF, width), F32),
        pltpu.VMEM((LAYERS, 4, HALF, width), F32),
        pltpu.VMEM((EMB, width), F32),
        pltpu.VMEM((EMB, per), F32),
        pltpu.VMEM((8, 8, width), F32),
        pltpu.VMEM((users, 128), F32),
        pltpu.VMEM((4, width), F32),
        pltpu.VMEM((4, width), F32),
        pltpu.VMEM((4, width), F32),
        pltpu.VMEM((3, 4, width), F32),
        pltpu.VMEM((4, width), F32),
        pltpu.VMEM((4, width), F32),
        pltpu.VMEM((4, 1, width), F32),
        pltpu.VMEM((4, 1, width), F32),
        pltpu.VMEM((8, users), F32),
        pltpu.VMEM((3, 8, users), F32),
        pltpu.VMEM((users, 128), F32),
        pltpu.VMEM((users, EMB), F32),
        pltpu.VMEM((LAYERS, 4, EMB, per), F32),
        pltpu.VMEM((LAYERS, 3, EMB, per), F32),
        pltpu.VMEM((7, EMB, n_query), BF16),
        pltpu.VMEM((1, n_query), jnp.int32),
        pltpu.SemaphoreType.DMA((STAGES,)),
        pltpu.SemaphoreType.DMA((3,)),
        pltpu.SemaphoreType.DMA((N_SENT,)),
        pltpu.SemaphoreType.DMA((N_GOT,)),
    ]
    return pl.pallas_call(
        kernel,
        out_shape=(pltpu.VMEM((EMB, per), BF16),
                   pltpu.VMEM((EMB, width), BF16),
                   pltpu.VMEM((EMB, n_query), BF16)),
        in_specs=[hbm, hbm, hbm, hbm],
        out_specs=(vmem, vmem, vmem),
        scratch_shapes=scratch,
        compiler_params=pltpu.CompilerParams(
            collective_id=0, has_side_effects=True, vmem_limit_bytes=61_600_000),
        name='propagate',
    )(mask_blk, item_shard, user_shard, queries.reshape(1, n_query))


def output_kernel(pick_ref, item_ref, user_ref, scores_ref, fi_ref, fu_ref, scores, sem):
    copies = [pltpu.make_async_copy(item_ref, fi_ref, sem.at[0]),
              pltpu.make_async_copy(user_ref, fu_ref, sem.at[1])]
    for copy in copies:
        copy.start()
    picked = pick_ref[...].astype(F32).T.astype(BF16)
    cols = scores.shape[1] // 4
    for i in range(4):
        at = pl.ds(i * cols, cols)
        scores[:, at] = dot(picked, item_ref[:, at], NN)
        copy = pltpu.make_async_copy(scores.at[:, at], scores_ref.at[:, at], sem.at[2 + i])
        copy.start()
        copies.append(copy)
    for copy in copies:
        copy.wait()


def outputs(fu_t, fi_t, picked_t):
    n_query = picked_t.shape[1]
    width, per = fi_t.shape[1], fu_t.shape[1]
    hbm = pl.BlockSpec(memory_space=pl.ANY)
    vmem = pl.BlockSpec(memory_space=pltpu.VMEM)
    args = [pltpu.with_memory_space_constraint(x, pltpu.VMEM) for x in (picked_t, fi_t, fu_t)]
    return pl.pallas_call(
        output_kernel,
        out_shape=(jax.ShapeDtypeStruct((n_query, width), F32),
                   jax.ShapeDtypeStruct((EMB, width), BF16),
                   jax.ShapeDtypeStruct((EMB, per), BF16)),
        in_specs=[vmem, vmem, vmem],
        out_specs=(hbm, hbm, hbm),
        scratch_shapes=[pltpu.VMEM((n_query, width), F32), pltpu.SemaphoreType.DMA((6,))],
        name='outputs',
    )(*args)


def solution(mesh):
    def device_step(mask_blk, user_shard, item_shard, queries):
        fu_t, fi_t, picked_t = propagate(mask_blk, user_shard.T, item_shard.T, queries)
        scores, fi_t, fu_t = outputs(fu_t, fi_t, picked_t)
        return fu_t.T, fi_t.T, scores

    return jax.shard_map(
        device_step, mesh=mesh,
        in_specs=(P('row', 'col'), P(('row', 'col'), None), P(('col', 'row'), None), P()),
        out_specs=(P(('row', 'col'), None), P(('col', 'row'), None), P(None, ('col', 'row'))),
        check_vma=False)
```

```python
import jax
import jax.numpy as jnp
from jax import lax
from jax.experimental import pallas as pl
from jax.experimental.pallas import tpu as pltpu
from jax.sharding import PartitionSpec as P

LAYERS = 3
EMB = 64
HALF = EMB // 2
QUARTER = EMB // 4
NT = (((1,), (1,)), ((), ()))
NN = (((1,), (0,)), ((), ()))
TN = (((0,), (0,)), ((), ()))
F32 = jnp.float32
BF16 = jnp.bfloat16
STAGES = 8
N_SENT = 13
N_GOT = 43


def dot(lhs, rhs, dims):
    return lax.dot_general(lhs, rhs, dims, preferred_element_type=F32)


def kernel(mask_ref, item_ref, user_ref, query_ref, fu_ref, fi_ref, pick_ref,
           adj, stage, panel, upan, psend, drecv, sacc, hop1, rown, isum, usum,
           colacc, rowacc, deg_send, deg_recv, deg_own, deg_in, deg_fin, deg_oth, far_send, far_in,
           udeg, udeg_in, invu, uacc, upart, uin, pk, qbuf, stage_sem, in_sem, send_sem, recv_sem):
    c = lax.axis_index('col')
    r = lax.axis_index('row')
    users = rowacc.shape[0]
    width = adj.shape[2]
    rows = stage.shape[1]
    per_slot = users // rows
    core, cx, cy = r % 2, (r // 2) % 2, r // 4

    def plane(d, k):
        return ((cy + d // 2) % 2) * 4 + ((cx + d % 2) % 2) * 2 + (core + k) % 2

    def zpeer(k):
        return ((c // 2 + k // 2) % 2) * 2 + (c % 2 + k % 2) % 2

    slots = {d * 2 + k: (c, plane(d, k)) for d in range(4) for k in range(2)}
    partner, xn, yn, dg = slots[1], slots[2], slots[4], slots[6]
    zn = [None] + [(zpeer(k), r) for k in (1, 2, 3)]

    got_index, out_index = {}, {}

    def parity(key):
        return key if isinstance(key, str) else (key[0], key[1] % 2) + key[2:]

    def send(src, dst, device, got, out):
        copy = pltpu.make_async_remote_copy(
            src_ref=src, dst_ref=dst,
            send_sem=send_sem.at[out_index.setdefault(out, len(out_index))],
            recv_sem=recv_sem.at[got_index.setdefault(parity(got), len(got_index))],
            device_id=device, device_id_type=pl.DeviceIdType.MESH)
        copy.start()

    def group(whole, got, out):
        return pltpu.make_async_remote_copy(
            src_ref=whole, dst_ref=whole, send_sem=send_sem.at[out], recv_sem=recv_sem.at[got],
            device_id=partner, device_id_type=pl.DeviceIdType.MESH)

    def arrived(got, whole):
        group(whole, got_index[parity(got)], 0).wait_recv()

    def sent(out, whole):
        group(whole, 0, out_index[out]).wait_send()

    def mask_slot(step):
        return (step // per_slot % 4) * 2 + 1 - step // (4 * per_slot)

    def mask_copy(step):
        slot = mask_slot(step)
        part = step % per_slot
        col = plane(slot // 2, slot % 2) * width
        return pltpu.make_async_copy(
            mask_ref.at[pl.ds(pl.multiple_of(part * rows, rows), rows),
                        pl.ds(pl.multiple_of(col, width), width)],
            stage.at[step % STAGES], stage_sem.at[step % STAGES])

    steps = 8 * per_slot
    for s in range(STAGES):
        mask_copy(jnp.int32(s)).start()

    inputs = [pltpu.make_async_copy(item_ref, panel.at[0, 0], in_sem.at[0]),
              pltpu.make_async_copy(user_ref, upan.at[0, c], in_sem.at[1]),
              pltpu.make_async_copy(query_ref, qbuf, in_sem.at[2])]
    for copy in inputs:
        copy.start()

    barrier = pltpu.get_barrier_semaphore()
    peers = tuple(slots[k] for k in range(1, 8)) + (zn[1], zn[2], zn[3])
    for device in peers:
        pl.semaphore_signal(barrier, inc=1, device_id=device, device_id_type=pl.DeviceIdType.MESH)

    rowacc[...] = jnp.zeros_like(rowacc)
    colacc[...] = jnp.zeros_like(colacc)

    def piece(h, i):
        return pl.ds(h * HALF + i * QUARTER, QUARTER)

    def gather_start(n, i):
        own = panel.at[n, 0]
        for h in (0, 1):
            got = ('forward', n, i) if h == 0 else ('near', n)
            at, to = piece(h, i), piece(1 - h, i)
            send(own.at[at], panel.at[n, 2, at], xn, got, 'gather')
            send(own.at[to], panel.at[n, 4, to], yn, got, 'gather')
        if i:
            send(own, panel.at[n, 1], partner, ('p0', n), 'gather')

    def gather_forward(n, i):
        arrived(('forward', n, i), panel.at[n, 2, pl.ds(0, HALF)])
        at, to = piece(0, i), piece(1, i)
        send(panel.at[n, 2, at], panel.at[n, 6, at], yn, ('last', n), 'gather')
        send(panel.at[n, 4, to], panel.at[n, 6, to], xn, ('last', n), 'gather')

    def gather_near(n):
        arrived(('near', n), panel.at[n, 2])
        send(panel.at[n, 2], panel.at[n, 3], partner, ('p12', n), 'gather')
        send(panel.at[n, 4], panel.at[n, 5], partner, ('p12', n), 'gather')

    def gather_last(n):
        arrived(('last', n), panel.at[n, 6])
        send(panel.at[n, 6], panel.at[n, 7], partner, ('p3', n), 'gather')

    def zgather_start(n):
        for k in (3, 2, 1):
            send(upan.at[n, c], upan.at[n, c], zn[k], 'zgather', 'zgather')

    def zgather_wait(n):
        arrived('zgather', upan.at[n, pl.ds(0, 3)])
        return jnp.concatenate([upan[n, k] for k in range(4)], axis=1)

    def zsum_start(n, acc):
        acc_t = acc.T
        for k in range(4):
            upart[n, k] = acc_t[:, k * 128:(k + 1) * 128]
        for k in (3, 2, 1):
            send(upart.at[n, zpeer(k)], uin.at[n, k - 1], zn[k], 'zsum', 'zsum')

    def zsum_wait(n):
        arrived('zsum', uin.at[n])
        total = (upart[n, c] + uin[n, 0]) + (uin[n, 1] + uin[n, 2])
        nxt = total.astype(BF16)
        usum[...] = usum[...] + nxt.astype(F32)
        return nxt

    def mask_step(step, carry):
        mask_copy(step).wait()
        slot = mask_slot(step)
        part = step % per_slot
        buf = step % STAGES

        def convert(i, col):
            at = pl.multiple_of(i * 16, 16)
            x = stage[buf, pl.ds(at, 16), :].astype(F32)
            row = pl.multiple_of(part * rows + i * 16, 16)
            adj[slot, pl.ds(row, 16), :] = x.astype(BF16)
            lanes = x[:, :128]
            for t in range(1, width // 128):
                lanes = lanes + x[:, t * 128:(t + 1) * 128]
            rowacc[pl.ds(row, 16), :] += lanes
            return col + (x[:8] + x[8:])

        colacc[slot] += lax.fori_loop(0, rows // 16, convert, jnp.zeros((8, width), F32), unroll=2)

        @pl.when(step + STAGES < steps)
        def _():
            mask_copy(step + STAGES).start()

        return carry

    with jax.named_scope('mask_a'):
        lax.fori_loop(0, steps // 4, mask_step, 0)
    with jax.named_scope('barrier'):
        pl.semaphore_wait(barrier, len(peers))
    with jax.named_scope('inputs'):
        for copy in inputs:
            copy.wait()
        gather_start(0, 0)
        gather_start(0, 1)
        zgather_start(0)
        isum[...] = panel[0, 0].astype(F32)
        usum[...] = upan[0, c].astype(F32)
    with jax.named_scope('mask_b'):
        lax.fori_loop(steps // 4, steps * 5 // 8, mask_step, 0)
        for d in range(4):
            deg_send[d:d + 1, :] = jnp.sum(colacc[2 * d + 1], axis=0, keepdims=True)
        send(deg_send, deg_recv, partner, 'dp', 'dp')
    with jax.named_scope('mask_c'):
        lax.fori_loop(steps * 5 // 8, steps, mask_step, 0)

    with jax.named_scope('deg_sum'):
        udeg[...] = dot(jnp.ones((8, 128), BF16), rowacc[...].astype(BF16), NT)
        for k in (3, 2, 1):
            send(udeg, udeg_in.at[k - 1], zn[k], 'zd', 'zd')
        mine = jnp.concatenate(
            [jnp.sum(colacc[2 * d], axis=0, keepdims=True) for d in range(4)], axis=0)
    with jax.named_scope('deg_partner'):
        arrived('dp', deg_recv)
        deg_own[...] = mine + deg_recv[...]
        for k, device in enumerate((xn, yn, dg)):
            send(deg_own, deg_in.at[k], device, 'ds', 'ds')
        for d in range(4):
            far_send[d] = deg_own[d:d + 1, :]
            send(far_send.at[d], far_in.at[d], slots[2 * (3 - d) + 1], 'far', 'far')
    with jax.named_scope('deg_users'):
        arrived('zd', udeg_in)
        du = (udeg[...] + udeg_in[0]) + (udeg_in[1] + udeg_in[2])
        inv = lax.rsqrt(jnp.maximum(du, 1.0))
        invu[...] = jnp.broadcast_to(inv[0:1, :], (128, users)).T
    with jax.named_scope('deg_items'):
        arrived('ds', deg_in)
    with jax.named_scope('deg_inv'):
        for d in range(4):
            total = ((deg_own[d:d + 1, :] + deg_in[0, (d ^ 1):(d ^ 1) + 1, :])
                     + (deg_in[1, (d ^ 2):(d ^ 2) + 1, :] + deg_in[2, (d ^ 3):(d ^ 3) + 1, :]))
            deg_fin[d:d + 1, :] = lax.rsqrt(jnp.maximum(total, 1.0))
        send(deg_fin, deg_oth, partner, 'df', 'df')
        arrived('far', far_in)
        for i in (0, 1):
            gather_forward(0, i)
        gather_near(0)

    def normalize(slot, at=0, size=width):
        d = slot // 2
        cols = pl.ds(at, size)
        if slot == 7:
            total = (far_in[3, :, cols] + far_in[2, :, cols]) + (far_in[1, :, cols] + far_in[0, :, cols])
            inv_item = lax.rsqrt(jnp.maximum(total, 1.0))
        else:
            inv_item = (deg_oth if slot % 2 else deg_fin)[d:d + 1, cols]

        step = 16 * max(1, width // 2 // size)

        def scale(i, carry):
            for j in range(step // 16):
                row = pl.ds(pl.multiple_of(i * step + j * 16, 16), 16)
                inv_user = jnp.concatenate([invu[row, :]] * (size // 128), axis=1)
                adj[slot, row, cols] = adj[slot, row, cols] * (inv_user * inv_item).astype(BF16)
            return carry

        lax.fori_loop(0, users // step, scale, 0, unroll=2)

    sizes = (width // 8, width // 4, width - 3 * width // 8)
    starts = (0, width // 8, 3 * width // 8)
    splits = [pl.ds(at, size) for at, size in zip(starts, sizes)]
    lo, hi = pl.ds(0, HALF), pl.ds(HALF, HALF)

    def items_diagonal(n, i=None):
        cols = pl.ds(0, width) if i is None else splits[i]
        send(sacc.at[n, 3, lo, cols], hop1.at[n, 0, :, cols], xn, ('hop1', n), 'sum')
        send(sacc.at[n, 3, hi, cols], hop1.at[n, 1, :, cols], yn, ('hop1', n), 'sum')

    def items_x(n):
        send(sacc.at[n, 1, lo], rown.at[n, 0], xn, ('direct', n), 'sum')

    def items_y(n):
        send(sacc.at[n, 2, hi], rown.at[n, 3], yn, ('direct', n), 'sum')

    def away(n, u, d):
        psend[n, d] = dot(u, adj[2 * d + 1], NN)
        send(psend.at[n, d], drecv.at[n, d], partner, ('partner', n, d), 'items')

    def near(n, u, d):
        part = dot(u, adj[2 * d], NN)
        if d:
            arrived(('partner', n, d), drecv.at[n, d])
            part = part + drecv[n, d]
        sacc[n, d] = part

    def items_first(u):
        def theirs(i):
            cols = splits[i]
            normalize(7, starts[i], sizes[i])
            psend[0, 3, :, cols] = dot(u, adj[7, :, cols], NN)
            send(psend.at[0, 3, :, cols], drecv.at[0, 3, :, cols], partner, ('partner', 0, 3, i), 'items')

        def ours(i):
            cols = splits[i]
            normalize(6, starts[i], sizes[i])
            sacc[0, 3, :, cols] = dot(u, adj[6, :, cols], NN)

        def both(i):
            cols = splits[i]
            with jax.named_scope(f'w6{i}'):
                arrived(('partner', 0, 3, i), drecv.at[0, 3, :, cols])
                sacc[0, 3, :, cols] = sacc[0, 3, :, cols] + drecv[0, 3, :, cols]
            items_diagonal(0, i)

        theirs(0)
        ours(0)
        theirs(1)
        theirs(2)
        both(0)
        ours(1)
        both(1)
        ours(2)
        both(2)
        arrived('df', deg_oth)

        normalize(3)
        away(0, u, 1)
        normalize(5)
        away(0, u, 2)
        normalize(2)
        near(0, u, 1)
        items_x(0)
        normalize(1)
        away(0, u, 0)
        normalize(4)
        near(0, u, 2)
        items_y(0)
        normalize(0)
        near(0, u, 0)

    def items_later(n, u, hooks):
        away(n, u, 3)
        away(n, u, 1)
        hooks[0]()
        near(n, u, 3)
        hooks[1]()
        away(n, u, 2)
        away(n, u, 0)
        near(n, u, 1)
        hooks[2]()
        near(n, u, 2)
        near(n, u, 0)

    def items_mid(n, i):
        if i == 0:
            arrived(('hop1', n), hop1.at[n])
        at = pl.ds(i * QUARTER, QUARTER)
        sacc[n, 2, piece(0, i)] = sacc[n, 2, piece(0, i)] + hop1[n, 0, at]
        send(sacc.at[n, 2, piece(0, i)], rown.at[n, 2, at], yn, ('hop2', n, i), 'sum')
        sacc[n, 1, piece(1, i)] = sacc[n, 1, piece(1, i)] + hop1[n, 1, at]
        send(sacc.at[n, 1, piece(1, i)], rown.at[n, 1, at], xn, ('hop2', n, i), 'sum')

    def items_finish(n, i):
        if i == 0:
            arrived(('partner', n, 0), drecv.at[n, 0])
            arrived(('direct', n), rown.at[n, pl.ds(0, 2)])
        arrived(('hop2', n, i), rown.at[n, 0])
        at = pl.ds(i * QUARTER, QUARTER)
        for h in (0, 1):
            rows_h = piece(h, i)
            total = ((sacc[n, 0, rows_h] + drecv[n, 0, rows_h]) + rown[n, h, at]) + rown[n, 2 + h, at]
            nxt = total.astype(BF16)
            isum[rows_h] = isum[rows_h] + nxt.astype(F32)
            if n + 1 < LAYERS:
                panel[n + 1, 0, rows_h] = nxt

    def user_partial(n, near_done=False, hook=None):
        def some(first, stride, count):
            def one(j, carry):
                at = first + stride * j
                uacc[...] += dot(adj[at], panel[n, at], NT)
                return carry

            lax.fori_loop(0, count, one, 0)

        arrived(('p0', n), panel.at[n, 1])
        uacc[...] = dot(adj[0], panel[n, 0], NT)
        some(1, 1, 1)
        if not near_done:
            gather_near(n)
        some(2, 2, 2)
        arrived(('p12', n), panel.at[n, pl.ds(2, 2)])
        some(3, 2, 2)
        if hook is not None:
            hook()
        gather_last(n)
        some(6, 1, 1)
        arrived(('p3', n), panel.at[n, 7])
        some(7, 1, 1)
        return uacc[...]

    scope = jax.named_scope

    def mid(n):
        items_mid(n, 0)
        items_mid(n, 1)

    def finish(n, i):
        with scope(f'finish{n}{i}'):
            items_finish(n, i)
            gather_start(n + 1, i)

    def forward(n, i):
        with scope(f'forward{n}{i}'):
            gather_forward(n, i)

    def launch1():
        forward(1, 1)
        items_diagonal(1)

    def nothing():
        pass

    with scope('u0'):
        u0 = zgather_wait(0)
    with scope('items0'):
        items_first(u0)
    with scope('user0'):
        zsum_start(0, user_partial(0, near_done=True, hook=lambda: mid(0)))
    finish(0, 0)
    with scope('zsum0'):
        upan[1, c] = zsum_wait(0)
        zgather_start(1)
    finish(0, 1)
    with scope('zgather1'):
        u1 = zgather_wait(1)
    with scope('items1'):
        forward(1, 0)
        items_later(1, u1, (nothing, launch1, nothing))
        items_x(1)
        items_y(1)
    with scope('user1'):
        zsum_start(1, user_partial(1))
    with scope('mid1'):
        mid(1)
    with scope('zsum1'):
        upan[2, c] = zsum_wait(1)
        zgather_start(2)
    with scope('zgather2'):
        u2 = zgather_wait(2)
    with scope('items2'):
        items_later(2, u2, (lambda: finish(1, 0), lambda: finish(1, 1), lambda: forward(2, 0)))
        forward(2, 1)
        items_diagonal(2)
        items_x(2)
        items_y(2)
    with scope('user2'):
        zsum_start(2, user_partial(2))
    with scope('mid2'):
        items_mid(2, 0)

        @pl.when(core == 0)
        def _():
            items_mid(2, 1)

    with scope('zsum2'):
        zsum_wait(2)
        final_user = (usum[...] / (LAYERS + 1)).astype(BF16)
        fu_ref[...] = final_user
        upan[3, c] = final_user
        zgather_start(3)
    with scope('zgather3'):
        ufin = zgather_wait(3)
    with scope('pick'):
        local = qbuf[...] - r * users
        chosen = (lax.broadcasted_iota(jnp.int32, (users, local.shape[1]), 0)
                  == jnp.broadcast_to(local, (users, local.shape[1]))).astype(F32).astype(BF16)
        pk[0] = dot(ufin, chosen, NN).astype(BF16)

        @pl.when(core == 0)
        def _():
            send(pk.at[0], pk.at[1], partner, 'pick', 'pick')

        @pl.when(core == 1)
        def _():
            arrived('pick', pk.at[1])
            pk[2] = pk[0] + pk[1]
            for k, device in enumerate((xn, yn, dg)):
                send(pk.at[2], pk.at[3 + k], device, 'picks', 'picks')
            items_mid(2, 1)

    with scope('finish20'):
        items_finish(2, 0)
    with scope('picked'):
        @pl.when(core == 1)
        def _():
            arrived('picks', pk.at[pl.ds(3, 3)])
            pk[6] = (pk[2] + pk[3]) + (pk[4] + pk[5])
            send(pk.at[6], pk.at[6], partner, 'picked', 'picked')
            sent('picks', pk.at[pl.ds(3, 3)])
            sent('picked', pk.at[6])

        @pl.when(core == 0)
        def _():
            arrived('picked', pk.at[6])
            sent('pick', pk.at[0])

        pick_ref[...] = pk[6].astype(F32).T.astype(BF16)
    with scope('finish21'):
        items_finish(2, 1)
        fi_ref[...] = (isum[...] / (LAYERS + 1)).astype(BF16)
    with scope('drain'):
        sent('gather', panel.at[:, pl.ds(0, 7)])
        sent('items', psend)
        sent('sum', sacc.at[:, pl.ds(1, 3)])
        sent('zsum', uin)
        sent('zgather', upan.at[:, pl.ds(0, 3)])
        for out, whole in (('dp', deg_send), ('zd', udeg_in), ('ds', deg_in), ('far', far_in),
                           ('df', deg_fin)):
            sent(out, whole)


def propagate(mask_blk, user_shard, item_shard, queries):
    users, items = mask_blk.shape
    width = items // 8
    per = user_shard.shape[1]
    n_query = queries.shape[0]
    vmem = pl.BlockSpec(memory_space=pltpu.VMEM)
    hbm = pl.BlockSpec(memory_space=pl.ANY)
    scratch = [
        pltpu.VMEM((8, users, width), BF16),
        pltpu.VMEM((STAGES, users // 4, width), jnp.int32),
        pltpu.VMEM((LAYERS, 8, EMB, width), BF16),
        pltpu.VMEM((LAYERS + 1, 4, EMB, per), BF16),
        pltpu.VMEM((LAYERS, 4, EMB, width), F32),
        pltpu.VMEM((LAYERS, 4, EMB, width), F32),
        pltpu.VMEM((LAYERS, 4, EMB, width), F32),
        pltpu.VMEM((LAYERS, 2, HALF, width), F32),
        pltpu.VMEM((LAYERS, 4, HALF, width), F32),
        pltpu.VMEM((EMB, width), F32),
        pltpu.VMEM((EMB, per), F32),
        pltpu.VMEM((8, 8, width), F32),
        pltpu.VMEM((users, 128), F32),
        pltpu.VMEM((4, width), F32),
        pltpu.VMEM((4, width), F32),
        pltpu.VMEM((4, width), F32),
        pltpu.VMEM((3, 4, width), F32),
        pltpu.VMEM((4, width), F32),
        pltpu.VMEM((4, width), F32),
        pltpu.VMEM((4, 1, width), F32),
        pltpu.VMEM((4, 1, width), F32),
        pltpu.VMEM((8, users), F32),
        pltpu.VMEM((3, 8, users), F32),
        pltpu.VMEM((users, 128), F32),
        pltpu.VMEM((users, EMB), F32),
        pltpu.VMEM((LAYERS, 4, EMB, per), F32),
        pltpu.VMEM((LAYERS, 3, EMB, per), F32),
        pltpu.VMEM((7, EMB, n_query), BF16),
        pltpu.VMEM((1, n_query), jnp.int32),
        pltpu.SemaphoreType.DMA((STAGES,)),
        pltpu.SemaphoreType.DMA((3,)),
        pltpu.SemaphoreType.DMA((N_SENT,)),
        pltpu.SemaphoreType.DMA((N_GOT,)),
    ]
    return pl.pallas_call(
        kernel,
        out_shape=(pltpu.VMEM((EMB, per), BF16),
                   pltpu.VMEM((EMB, width), BF16),
                   pltpu.VMEM((n_query, EMB), BF16)),
        in_specs=[hbm, hbm, hbm, hbm],
        out_specs=(vmem, vmem, vmem),
        scratch_shapes=scratch,
        compiler_params=pltpu.CompilerParams(
            collective_id=0, has_side_effects=True, vmem_limit_bytes=61_600_000),
        name='propagate',
    )(mask_blk, item_shard, user_shard, queries.reshape(1, n_query))


def output_kernel(pick_ref, item_ref, user_ref, scores_ref, fi_ref, fu_ref, scores, sem):
    copies = [pltpu.make_async_copy(item_ref, fi_ref, sem.at[0]),
              pltpu.make_async_copy(user_ref, fu_ref, sem.at[1])]
    for copy in copies:
        copy.start()
    picked = pick_ref[...]
    cols = scores.shape[1] // 4
    for i in range(4):
        at = pl.ds(i * cols, cols)
        scores[:, at] = dot(picked, item_ref[:, at], NN)
        copy = pltpu.make_async_copy(scores.at[:, at], scores_ref.at[:, at], sem.at[2 + i])
        copy.start()
        copies.append(copy)
    for copy in copies:
        copy.wait()


def outputs(fu_t, fi_t, picked):
    n_query = picked.shape[0]
    width, per = fi_t.shape[1], fu_t.shape[1]
    hbm = pl.BlockSpec(memory_space=pl.ANY)
    vmem = pl.BlockSpec(memory_space=pltpu.VMEM)
    args = [pltpu.with_memory_space_constraint(x, pltpu.VMEM) for x in (picked, fi_t, fu_t)]
    return pl.pallas_call(
        output_kernel,
        out_shape=(jax.ShapeDtypeStruct((n_query, width), F32),
                   jax.ShapeDtypeStruct((EMB, width), BF16),
                   jax.ShapeDtypeStruct((EMB, per), BF16)),
        in_specs=[vmem, vmem, vmem],
        out_specs=(hbm, hbm, hbm),
        scratch_shapes=[pltpu.VMEM((n_query, width), F32), pltpu.SemaphoreType.DMA((6,))],
        name='outputs',
    )(*args)


def solution(mesh):
    def device_step(mask_blk, user_shard, item_shard, queries):
        fu_t, fi_t, picked = propagate(mask_blk, user_shard.T, item_shard.T, queries)
        scores, fi_t, fu_t = outputs(fu_t, fi_t, picked)
        return fu_t.T, fi_t.T, scores

    return jax.shard_map(
        device_step, mesh=mesh,
        in_specs=(P('row', 'col'), P(('row', 'col'), None), P(('col', 'row'), None), P()),
        out_specs=(P(('row', 'col'), None), P(('col', 'row'), None), P(None, ('col', 'row'))),
        check_vma=False)
```

```python
import jax
import jax.numpy as jnp
from jax import lax
from jax.experimental import pallas as pl
from jax.experimental.pallas import tpu as pltpu
from jax.sharding import PartitionSpec as P

LAYERS = 3
EMB = 64
HALF = EMB // 2
QUARTER = EMB // 4
NT = (((1,), (1,)), ((), ()))
NN = (((1,), (0,)), ((), ()))
TN = (((0,), (0,)), ((), ()))
F32 = jnp.float32
BF16 = jnp.bfloat16
STAGES = 8
N_SENT = 13
N_GOT = 43


def dot(lhs, rhs, dims):
    return lax.dot_general(lhs, rhs, dims, preferred_element_type=F32)


def kernel(mask_ref, item_ref, user_ref, query_ref, fu_ref, fi_ref, pick_ref,
           adj, stage, panel, upan, psend, drecv, sacc, hop1, hop1b, rown, isum, usum,
           colacc, rowacc, deg_send, deg_recv, deg_own, deg_in, deg_fin, deg_oth, far_send, far_in,
           udeg, udeg_in, invu, uacc, upart, uin, pk, qbuf, stage_sem, in_sem, send_sem, recv_sem):
    c = lax.axis_index('col')
    r = lax.axis_index('row')
    users = rowacc.shape[0]
    width = adj.shape[2]
    rows = stage.shape[1]
    per_slot = users // rows
    core, cx, cy = r % 2, (r // 2) % 2, r // 4

    def flip(bit, by):
        return (bit + by) % 2

    def plane(d, k):
        return flip(cy, d // 2) * 4 + flip(cx, d % 2) * 2 + flip(core, k)

    def zpeer(k):
        return flip(c // 2, k // 2) * 2 + flip(c % 2, k % 2)

    slots = {d * 2 + k: (c, plane(d, k)) for d in range(4) for k in range(2)}
    partner, xn, yn, dg = slots[1], slots[2], slots[4], slots[6]
    zn = {k: (zpeer(k), r) for k in (1, 2, 3)}

    got_index, out_index = {}, {}

    def parity(key):
        return key if isinstance(key, str) else (key[0], key[1] % 2) + key[2:]

    def send(src, dst, device, got, out):
        copy = pltpu.make_async_remote_copy(
            src_ref=src, dst_ref=dst,
            send_sem=send_sem.at[out_index.setdefault(out, len(out_index))],
            recv_sem=recv_sem.at[got_index.setdefault(parity(got), len(got_index))],
            device_id=device, device_id_type=pl.DeviceIdType.MESH)
        copy.start()

    def group(whole, got, out):
        return pltpu.make_async_remote_copy(
            src_ref=whole, dst_ref=whole, send_sem=send_sem.at[out], recv_sem=recv_sem.at[got],
            device_id=partner, device_id_type=pl.DeviceIdType.MESH)

    def arrived(got, whole):
        group(whole, got_index[parity(got)], 0).wait_recv()

    def sent(out, whole):
        group(whole, 0, out_index[out]).wait_send()

    def mask_slot(step):
        return (step // per_slot % 4) * 2 + 1 - step // (4 * per_slot)

    def mask_copy(step):
        slot = mask_slot(step)
        part = step % per_slot
        col = plane(slot // 2, slot % 2) * width
        return pltpu.make_async_copy(
            mask_ref.at[pl.ds(pl.multiple_of(part * rows, rows), rows),
                        pl.ds(pl.multiple_of(col, width), width)],
            stage.at[step % STAGES], stage_sem.at[step % STAGES])

    steps = 8 * per_slot
    for s in range(STAGES):
        mask_copy(jnp.int32(s)).start()

    inputs = [pltpu.make_async_copy(item_ref, panel.at[0, 0], in_sem.at[0]),
              pltpu.make_async_copy(user_ref, upan.at[0, c], in_sem.at[1]),
              pltpu.make_async_copy(query_ref, qbuf, in_sem.at[2])]
    for copy in inputs:
        copy.start()

    barrier = pltpu.get_barrier_semaphore()
    peers = [device for k, device in slots.items() if k] + [zn[k] for k in (1, 2, 3)]
    for device in peers:
        pl.semaphore_signal(barrier, inc=1, device_id=device, device_id_type=pl.DeviceIdType.MESH)

    rowacc[...] = jnp.zeros_like(rowacc)
    colacc[...] = jnp.zeros_like(colacc)

    def piece(h, i):
        return pl.ds(h * HALF + i * QUARTER, QUARTER)

    def gather_start(n, i):
        own = panel.at[n, 0]
        for h in (0, 1):
            got = ('forward', n, i) if h == 0 else ('near', n)
            at, to = piece(h, i), piece(1 - h, i)
            send(own.at[at], panel.at[n, 2, at], xn, got, 'gather')
            send(own.at[to], panel.at[n, 4, to], yn, got, 'gather')
        if i:
            send(own, panel.at[n, 1], partner, ('p0', n), 'gather')

    def gather_forward(n, i):
        arrived(('forward', n, i), panel.at[n, 2, pl.ds(0, HALF)])
        at, to = piece(0, i), piece(1, i)
        send(panel.at[n, 2, at], panel.at[n, 6, at], yn, ('last', n), 'gather')
        send(panel.at[n, 4, to], panel.at[n, 6, to], xn, ('last', n), 'gather')

    def gather_near(n):
        arrived(('near', n), panel.at[n, 2])
        send(panel.at[n, 2], panel.at[n, 3], partner, ('p12', n), 'gather')
        send(panel.at[n, 4], panel.at[n, 5], partner, ('p12', n), 'gather')

    def gather_last(n):
        arrived(('last', n), panel.at[n, 6])
        send(panel.at[n, 6], panel.at[n, 7], partner, ('p3', n), 'gather')

    def zgather_start(n):
        for k in (3, 2, 1):
            send(upan.at[n, c], upan.at[n, c], zn[k], 'zgather', 'zgather')

    def zgather_wait(n):
        arrived('zgather', upan.at[n, pl.ds(0, 3)])
        return jnp.concatenate([upan[n, k] for k in range(4)], axis=1)

    def zsum_start(n, acc):
        acc_t = acc.T
        for k in range(4):
            upart[n, k] = acc_t[:, k * 128:(k + 1) * 128]
        for k in (3, 2, 1):
            send(upart.at[n, zpeer(k)], uin.at[n, k - 1], zn[k], 'zsum', 'zsum')

    def zsum_wait(n):
        arrived('zsum', uin.at[n])
        total = (upart[n, c] + uin[n, 0]) + (uin[n, 1] + uin[n, 2])
        nxt = total.astype(BF16)
        usum[...] = usum[...] + nxt.astype(F32)
        return nxt

    def mask_step(step, carry):
        mask_copy(step).wait()
        slot = mask_slot(step)
        part = step % per_slot
        buf = step % STAGES

        def convert(i, col):
            at = pl.multiple_of(i * 16, 16)
            x = stage[buf, pl.ds(at, 16), :].astype(F32)
            row = pl.multiple_of(part * rows + i * 16, 16)
            adj[slot, pl.ds(row, 16), :] = x.astype(BF16)
            lanes = x[:, :128]
            for t in range(1, width // 128):
                lanes = lanes + x[:, t * 128:(t + 1) * 128]
            rowacc[pl.ds(row, 16), :] += lanes
            return col + (x[:8] + x[8:])

        colacc[slot] += lax.fori_loop(0, rows // 16, convert, jnp.zeros((8, width), F32), unroll=2)

        @pl.when(step + STAGES < steps)
        def _():
            mask_copy(step + STAGES).start()

        return carry

    def column_sum(slot):
        return jnp.sum(colacc[slot], axis=0, keepdims=True)

    def mask_part(first, last):
        lax.fori_loop(steps * first // 8, steps * last // 8, mask_step, 0)

    with jax.named_scope('mask_a'):
        mask_part(0, 1)
    with jax.named_scope('barrier'):
        pl.semaphore_wait(barrier, len(peers))
    with jax.named_scope('inputs'):
        for copy in inputs:
            copy.wait()
        gather_start(0, 0)
        gather_start(0, 1)
        zgather_start(0)
        isum[...] = panel[0, 0].astype(F32)
        usum[...] = upan[0, c].astype(F32)
    with jax.named_scope('mask_b'):
        mask_part(1, 5)
        for d in range(4):
            deg_send[pl.ds(d, 1), :] = column_sum(2 * d + 1)
        send(deg_send, deg_recv, partner, 'dp', 'dp')
        mask_part(5, 6)
    with jax.named_scope('forward00'):
        gather_forward(0, 0)
    with jax.named_scope('mask_c'):
        mask_part(6, 7)
    with jax.named_scope('forward01'):
        gather_forward(0, 1)
    with jax.named_scope('mask_d'):
        mask_part(7, 8)

    with jax.named_scope('deg_sum'):
        udeg[...] = dot(jnp.ones((8, 128), BF16), rowacc[...].astype(BF16), NT)
        for k in (3, 2, 1):
            send(udeg, udeg_in.at[k - 1], zn[k], 'zd', 'zd')
        mine = jnp.concatenate(
            [column_sum(2 * d) for d in range(4)], axis=0)
    with jax.named_scope('deg_partner'):
        arrived('dp', deg_recv)
        deg_own[...] = mine + deg_recv[...]
        for k, device in enumerate((xn, yn, dg)):
            send(deg_own, deg_in.at[k], device, 'ds', 'ds')
        for d in range(4):
            far_send[d] = deg_own[d:d + 1, :]
            send(far_send.at[d], far_in.at[d], slots[2 * (3 - d) + 1], 'far', 'far')
    with jax.named_scope('deg_users'):
        arrived('zd', udeg_in)
        du = udeg[...] + jnp.sum(udeg_in[...], axis=0)
        inv = lax.rsqrt(jnp.maximum(du, 1.0))
        invu[...] = jnp.broadcast_to(inv[0:1, :], (128, users)).T
    with jax.named_scope('deg_items'):
        arrived('ds', deg_in)
    with jax.named_scope('deg_inv'):
        for d in range(4):
            total = deg_own[pl.ds(d, 1), :]
            for k in range(3):
                total = total + deg_in[k, pl.ds(d ^ (k + 1), 1), :]
            deg_fin[pl.ds(d, 1), :] = lax.rsqrt(jnp.maximum(total, 1.0))
        send(deg_fin, deg_oth, partner, 'df', 'df')
        arrived('far', far_in)
        gather_near(0)

    def normalize(slot, at=0, size=width):
        d = slot // 2
        cols = pl.ds(at, size)
        if slot == 7:
            total = jnp.sum(far_in[:, :, cols], axis=0)
            inv_item = lax.rsqrt(jnp.maximum(total, 1.0))
        else:
            inv_item = (deg_oth if slot % 2 else deg_fin)[d:d + 1, cols]

        step = 16 * max(1, width // 2 // size)

        def scale(i, carry):
            for j in range(step // 16):
                row = pl.ds(pl.multiple_of(i * step + j * 16, 16), 16)
                inv_user = jnp.concatenate([invu[row, :]] * (size // 128), axis=1)
                adj[slot, row, cols] = adj[slot, row, cols] * (inv_user * inv_item).astype(BF16)
            return carry

        lax.fori_loop(0, users // step, scale, 0, unroll=2)

    sizes = (width // 8, width // 4, width - 3 * width // 8)
    starts = (0, width // 8, 3 * width // 8)
    splits = [pl.ds(at, size) for at, size in zip(starts, sizes)]
    lo, hi = pl.ds(0, HALF), pl.ds(HALF, HALF)

    def items_diagonal(n, i=None):
        cols = pl.ds(0, width) if i is None else splits[i]
        send(sacc.at[n, 3, lo, cols], hop1.at[n, 0, :, cols], xn, ('hop1', n), 'sum')
        send(sacc.at[n, 3, hi, cols], hop1.at[n, 1, :, cols], yn, ('hop1', n), 'sum')

    def items_x(n):
        send(sacc.at[n, 1, lo], rown.at[n, 0], xn, ('direct', n), 'sum')

    def items_y(n):
        send(sacc.at[n, 2, hi], rown.at[n, 3], yn, ('direct', n), 'sum')

    def away(n, u, d):
        psend[n, d] = dot(u, adj[2 * d + 1], NN)
        send(psend.at[n, d], drecv.at[n, d], partner, ('partner', n, d), 'items')

    def near(n, u, d):
        part = dot(u, adj[2 * d], NN)
        if d:
            arrived(('partner', n, d), drecv.at[n, d])
            part = part + drecv[n, d]
        sacc[n, d] = part

    def items_first(u):
        n, d = 0, 3

        def theirs(i):
            cols = splits[i]
            normalize(2 * d + 1, starts[i], sizes[i])
            psend[n, d, :, cols] = dot(u, adj[2 * d + 1, :, cols], NN)
            if i:
                send(psend.at[n, d, :, cols], drecv.at[n, d, :, cols], partner, ('partner', n, d, i), 'items')
            else:
                for k, half in enumerate((lo, hi)):
                    send(psend.at[n, d, half, cols], hop1b.at[k], slots[3 + 2 * k], 'hop1b', 'items')

        def ours(i):
            cols = splits[i]
            normalize(2 * d, starts[i], sizes[i])
            sacc[n, d, :, cols] = dot(u, adj[2 * d, :, cols], NN)

        def both(i):
            cols = splits[i]
            arrived(('partner', n, d, i), drecv.at[n, d, :, cols])
            sacc[n, d, :, cols] = sacc[n, d, :, cols] + drecv[n, d, :, cols]
            items_diagonal(n, i)

        theirs(0)
        ours(0)
        items_diagonal(n, 0)
        theirs(1)
        theirs(2)
        for i in (1, 2):
            ours(i)
            both(i)
        arrived('df', deg_oth)

        for k in (1, 2):
            normalize(2 * k + 1)
            away(n, u, k)
        normalize(2)
        near(n, u, 1)
        items_x(n)
        normalize(4)
        near(n, u, 2)
        items_y(n)
        normalize(1)
        away(n, u, 0)
        normalize(0)
        near(n, u, 0)

    def items_later(n, u, hooks):
        away(n, u, 3)
        away(n, u, 1)
        hooks[0]()
        near(n, u, 3)
        hooks[1]()
        away(n, u, 2)
        away(n, u, 0)
        near(n, u, 1)
        hooks[2]()
        near(n, u, 2)
        near(n, u, 0)

    def items_mid(n, i):
        if i == 0:
            arrived(('hop1', n), hop1.at[n])
            if n == 0:
                arrived('hop1b', hop1b)
                for k in range(2):
                    hop1[n, k, :, splits[0]] = hop1[n, k, :, splits[0]] + hop1b[k]
        at = pl.ds(i * QUARTER, QUARTER)
        for h, device in enumerate((yn, xn)):
            block, part = 2 - h, piece(h, i)
            sacc[n, block, part] = sacc[n, block, part] + hop1[n, h, at]
            send(sacc.at[n, block, part], rown.at[n, block, at], device, ('hop2', n, i), 'sum')

    def items_finish(n, i):
        if i == 0:
            arrived(('partner', n, 0), drecv.at[n, 0])
            arrived(('direct', n), rown.at[n, pl.ds(0, 2)])
        arrived(('hop2', n, i), rown.at[n, 0])
        at = pl.ds(i * QUARTER, QUARTER)
        for h in (0, 1):
            rows_h = piece(h, i)
            total = ((sacc[n, 0, rows_h] + drecv[n, 0, rows_h]) + rown[n, h, at]) + rown[n, 2 + h, at]
            nxt = total.astype(BF16)
            isum[rows_h] = isum[rows_h] + nxt.astype(F32)
            if n + 1 < LAYERS:
                panel[n + 1, 0, rows_h] = nxt

    def user_partial(n, near_done=False, hook=None):
        def some(first, stride, count):
            def one(j, carry):
                at = first + stride * j
                uacc[...] += dot(adj[at], panel[n, at], NT)
                return carry

            lax.fori_loop(0, count, one, 0)

        arrived(('p0', n), panel.at[n, 1])
        uacc[...] = dot(adj[0], panel[n, 0], NT)
        some(1, 1, 1)
        if hook is not None:
            hook()
        if not near_done:
            gather_near(n)
        some(2, 2, 2)
        arrived(('p12', n), panel.at[n, pl.ds(2, 2)])
        some(3, 2, 2)
        gather_last(n)
        some(6, 1, 1)
        arrived(('p3', n), panel.at[n, 7])
        some(7, 1, 1)
        return uacc[...]

    scope = jax.named_scope

    def mid(n):
        items_mid(n, 0)
        items_mid(n, 1)

    def finish(n, i):
        with scope(f'finish{n}{i}'):
            items_finish(n, i)
            gather_start(n + 1, i)

    def forward(n, i):
        with scope(f'forward{n}{i}'):
            gather_forward(n, i)

    def nothing():
        pass

    with scope('u0'):
        u0 = zgather_wait(0)
    with scope('items0'):
        items_first(u0)
    with scope('user0'):
        zsum_start(0, user_partial(0, True, lambda: mid(0)))
    finish(0, 0)
    with scope('zsum0'):
        upan[1, c] = zsum_wait(0)
        zgather_start(1)
    finish(0, 1)
    with scope('zgather1'):
        u1 = zgather_wait(1)
    with scope('items1'):
        forward(1, 0)
        items_later(1, u1, (lambda: forward(1, 1), lambda: items_diagonal(1), nothing))
        items_x(1)
        items_y(1)
    with scope('user1'):
        zsum_start(1, user_partial(1))
    with scope('mid1'):
        mid(1)
    with scope('zsum1'):
        upan[2, c] = zsum_wait(1)
        zgather_start(2)
    finish(1, 0)
    with scope('zgather2'):
        u2 = zgather_wait(2)
    with scope('items2'):
        items_later(2, u2, (nothing, lambda: finish(1, 1), lambda: forward(2, 0)))
        forward(2, 1)
        items_diagonal(2)
        items_x(2)
        items_y(2)
    with scope('user2'):
        zsum_start(2, user_partial(2))
    with scope('mid2'):
        items_mid(2, 0)

        @pl.when(core == 0)
        def _():
            items_mid(2, 1)

    with scope('zsum2'):
        zsum_wait(2)
        final_user = (usum[...] / (LAYERS + 1)).astype(BF16)
        fu_ref[...] = final_user
        upan[3, c] = final_user
        zgather_start(3)
    with scope('zgather3'):
        ufin = zgather_wait(3)
    with scope('pick'):
        local = qbuf[...] - r * users
        chosen = (lax.broadcasted_iota(jnp.int32, (users, local.shape[1]), 0)
                  == jnp.broadcast_to(local, (users, local.shape[1]))).astype(F32).astype(BF16)
        pk[0] = dot(ufin, chosen, NN).astype(BF16)

        @pl.when(core == 0)
        def _():
            send(pk.at[0], pk.at[1], partner, 'pick', 'pick')

        @pl.when(core == 1)
        def _():
            arrived('pick', pk.at[1])
            pk[2] = pk[0] + pk[1]
            for k, device in enumerate((xn, yn, dg)):
                send(pk.at[2], pk.at[3 + k], device, 'picks', 'picks')
            items_mid(2, 1)

    with scope('finish20'):
        items_finish(2, 0)
    with scope('picked'):
        @pl.when(core == 1)
        def _():
            arrived('picks', pk.at[pl.ds(3, 3)])
            total = pk[2]
            for k in range(3):
                total = total + pk[3 + k]
            pk[6] = total
            send(pk.at[6], pk.at[6], partner, 'picked', 'picked')
            sent('picks', pk.at[pl.ds(3, 3)])
            sent('picked', pk.at[6])

        @pl.when(core == 0)
        def _():
            arrived('picked', pk.at[6])
            sent('pick', pk.at[0])

        pick_ref[...] = pk[6].astype(F32).T.astype(BF16)
    with scope('finish21'):
        items_finish(2, 1)
        fi_ref[...] = (isum[...] / (LAYERS + 1)).astype(BF16)
    with scope('drain'):
        sent('gather', panel.at[:, pl.ds(0, 7)])
        sent('items', psend)
        sent('sum', sacc.at[:, pl.ds(1, 3)])
        sent('zsum', uin)
        sent('zgather', upan.at[:, pl.ds(0, 3)])
        for out, whole in (('dp', deg_send), ('zd', udeg_in), ('ds', deg_in), ('far', far_in),
                           ('df', deg_fin)):
            sent(out, whole)


def propagate(mask_blk, user_shard, item_shard, queries):
    users, items = mask_blk.shape
    width = items // 8
    per = user_shard.shape[1]
    n_query = queries.shape[0]
    vmem = pl.BlockSpec(memory_space=pltpu.VMEM)
    hbm = pl.BlockSpec(memory_space=pl.ANY)
    scratch = [
        pltpu.VMEM((8, users, width), BF16),
        pltpu.VMEM((STAGES, users // 4, width), jnp.int32),
        pltpu.VMEM((LAYERS, 8, EMB, width), BF16),
        pltpu.VMEM((LAYERS + 1, 4, EMB, per), BF16),
        pltpu.VMEM((LAYERS, 4, EMB, width), F32),
        pltpu.VMEM((LAYERS, 4, EMB, width), F32),
        pltpu.VMEM((LAYERS, 4, EMB, width), F32),
        pltpu.VMEM((LAYERS, 2, HALF, width), F32),
        pltpu.VMEM((2, HALF, width // 8), F32),
        pltpu.VMEM((LAYERS, 4, HALF, width), F32),
        pltpu.VMEM((EMB, width), F32),
        pltpu.VMEM((EMB, per), F32),
        pltpu.VMEM((8, 8, width), F32),
        pltpu.VMEM((users, 128), F32),
        pltpu.VMEM((4, width), F32),
        pltpu.VMEM((4, width), F32),
        pltpu.VMEM((4, width), F32),
        pltpu.VMEM((3, 4, width), F32),
        pltpu.VMEM((4, width), F32),
        pltpu.VMEM((4, width), F32),
        pltpu.VMEM((4, 1, width), F32),
        pltpu.VMEM((4, 1, width), F32),
        pltpu.VMEM((8, users), F32),
        pltpu.VMEM((3, 8, users), F32),
        pltpu.VMEM((users, 128), F32),
        pltpu.VMEM((users, EMB), F32),
        pltpu.VMEM((LAYERS, 4, EMB, per), F32),
        pltpu.VMEM((LAYERS, 3, EMB, per), F32),
        pltpu.VMEM((7, EMB, n_query), BF16),
        pltpu.VMEM((1, n_query), jnp.int32),
        pltpu.SemaphoreType.DMA((STAGES,)),
        pltpu.SemaphoreType.DMA((3,)),
        pltpu.SemaphoreType.DMA((N_SENT,)),
        pltpu.SemaphoreType.DMA((N_GOT,)),
    ]
    return pl.pallas_call(
        kernel,
        out_shape=(pltpu.VMEM((EMB, per), BF16),
                   pltpu.VMEM((EMB, width), BF16),
                   pltpu.VMEM((n_query, EMB), BF16)),
        in_specs=[hbm, hbm, hbm, hbm],
        out_specs=(vmem, vmem, vmem),
        scratch_shapes=scratch,
        compiler_params=pltpu.CompilerParams(
            collective_id=0, has_side_effects=True, vmem_limit_bytes=61_600_000),
        name='propagate',
    )(mask_blk, item_shard, user_shard, queries.reshape(1, n_query))


def output_kernel(pick_ref, item_ref, user_ref, scores_ref, fi_ref, fu_ref, scores, sem):
    copies = [pltpu.make_async_copy(item_ref, fi_ref, sem.at[0]),
              pltpu.make_async_copy(user_ref, fu_ref, sem.at[1])]
    for copy in copies:
        copy.start()
    picked = pick_ref[...]
    cols = scores.shape[1] // 4
    for i in range(4):
        at = pl.ds(i * cols, cols)
        scores[:, at] = dot(picked, item_ref[:, at], NN)
        copy = pltpu.make_async_copy(scores.at[:, at], scores_ref.at[:, at], sem.at[2 + i])
        copy.start()
        copies.append(copy)
    for copy in copies:
        copy.wait()


def outputs(fu_t, fi_t, picked):
    n_query = picked.shape[0]
    width, per = fi_t.shape[1], fu_t.shape[1]
    hbm = pl.BlockSpec(memory_space=pl.ANY)
    vmem = pl.BlockSpec(memory_space=pltpu.VMEM)
    args = [pltpu.with_memory_space_constraint(x, pltpu.VMEM) for x in (picked, fi_t, fu_t)]
    return pl.pallas_call(
        output_kernel,
        out_shape=(jax.ShapeDtypeStruct((n_query, width), F32),
                   jax.ShapeDtypeStruct((EMB, width), BF16),
                   jax.ShapeDtypeStruct((EMB, per), BF16)),
        in_specs=[vmem, vmem, vmem],
        out_specs=(hbm, hbm, hbm),
        scratch_shapes=[pltpu.VMEM((n_query, width), F32), pltpu.SemaphoreType.DMA((6,))],
        name='outputs',
    )(*args)


def solution(mesh):
    def device_step(mask_blk, user_shard, item_shard, queries):
        fu_t, fi_t, picked = propagate(mask_blk, user_shard.T, item_shard.T, queries)
        scores, fi_t, fu_t = outputs(fu_t, fi_t, picked)
        return fu_t.T, fi_t.T, scores

    return jax.shard_map(
        device_step, mesh=mesh,
        in_specs=(P('row', 'col'), P(('row', 'col'), None), P(('col', 'row'), None), P()),
        out_specs=(P(('row', 'col'), None), P(('col', 'row'), None), P(None, ('col', 'row'))),
        check_vma=False)
```

```python
import jax
import jax.numpy as jnp
from jax import lax
from jax.experimental import pallas as pl
from jax.experimental.pallas import tpu as pltpu
from jax.sharding import PartitionSpec as P

LAYERS = 3
EMB = 64
HALF = EMB // 2
QUARTER = EMB // 4
NT = (((1,), (1,)), ((), ()))
NN = (((1,), (0,)), ((), ()))
TN = (((0,), (0,)), ((), ()))
F32 = jnp.float32
BF16 = jnp.bfloat16
STAGES = 8
N_SENT = 13
N_GOT = 43


def dot(lhs, rhs, dims):
    return lax.dot_general(lhs, rhs, dims, preferred_element_type=F32)


def kernel(mask_ref, item_ref, user_ref, query_ref, fu_ref, fi_ref, pick_ref,
           adj, stage, panel, upan, psend, drecv, sacc, hop1, hop1b, rown, isum, usum,
           colacc, rowacc, deg_send, deg_recv, deg_own, deg_in, deg_fin, deg_oth, far_send, far_in,
           udeg, udeg_in, invu, uacc, upart, uin, pk, qbuf, stage_sem, in_sem, send_sem, recv_sem):
    c = lax.axis_index('col')
    r = lax.axis_index('row')
    users = rowacc.shape[0]
    width = adj.shape[2]
    rows = stage.shape[1]
    per_slot = users // rows
    core, cx, cy = r % 2, (r // 2) % 2, r // 4

    def flip(bit, by):
        return (bit + by) % 2

    def plane(d, k):
        return flip(cy, d // 2) * 4 + flip(cx, d % 2) * 2 + flip(core, k)

    def zpeer(k):
        return flip(c // 2, k // 2) * 2 + flip(c % 2, k % 2)

    slots = {d * 2 + k: (c, plane(d, k)) for d in range(4) for k in range(2)}
    partner, xn, yn, dg = slots[1], slots[2], slots[4], slots[6]
    far_z = 3 - (c + 1) // 2 % 2
    zorder = (far_z, 5 - far_z, 1)
    zn = {k: (zpeer(k), r) for k in (1, 2, 3)}

    got_index, out_index = {}, {}

    def parity(key):
        return key if isinstance(key, str) else (key[0], key[1] % 2) + key[2:]

    def send(src, dst, device, got, out):
        copy = pltpu.make_async_remote_copy(
            src_ref=src, dst_ref=dst,
            send_sem=send_sem.at[out_index.setdefault(out, len(out_index))],
            recv_sem=recv_sem.at[got_index.setdefault(parity(got), len(got_index))],
            device_id=device, device_id_type=pl.DeviceIdType.MESH)
        copy.start()

    def group(whole, got, out):
        return pltpu.make_async_remote_copy(
            src_ref=whole, dst_ref=whole, send_sem=send_sem.at[out], recv_sem=recv_sem.at[got],
            device_id=partner, device_id_type=pl.DeviceIdType.MESH)

    def arrived(got, whole):
        group(whole, got_index[parity(got)], 0).wait_recv()

    def sent(out, whole):
        group(whole, 0, out_index[out]).wait_send()

    def mask_slot(step):
        return (step // per_slot % 4) * 2 + 1 - step // (4 * per_slot)

    def mask_copy(step):
        slot = mask_slot(step)
        part = step % per_slot
        col = plane(slot // 2, slot % 2) * width
        return pltpu.make_async_copy(
            mask_ref.at[pl.ds(pl.multiple_of(part * rows, rows), rows),
                        pl.ds(pl.multiple_of(col, width), width)],
            stage.at[step % STAGES], stage_sem.at[step % STAGES])

    steps = 8 * per_slot
    for s in range(STAGES):
        mask_copy(jnp.int32(s)).start()

    inputs = [pltpu.make_async_copy(item_ref, panel.at[0, 0], in_sem.at[0]),
              pltpu.make_async_copy(user_ref, upan.at[0, c], in_sem.at[1]),
              pltpu.make_async_copy(query_ref, qbuf, in_sem.at[2])]
    for copy in inputs:
        copy.start()

    barrier = pltpu.get_barrier_semaphore()
    peers = [device for k, device in slots.items() if k] + [zn[k] for k in (1, 2, 3)]
    for device in peers:
        pl.semaphore_signal(barrier, inc=1, device_id=device, device_id_type=pl.DeviceIdType.MESH)

    rowacc[...] = jnp.zeros_like(rowacc)
    colacc[...] = jnp.zeros_like(colacc)

    def piece(h, i):
        return pl.ds(h * HALF + i * QUARTER, QUARTER)

    def gather_start(n, i):
        own = panel.at[n, 0]
        for h in (0, 1):
            got = ('forward', n, i) if h == 0 else ('near', n)
            at, to = piece(h, i), piece(1 - h, i)
            send(own.at[at], panel.at[n, 2, at], xn, got, 'gather')
            send(own.at[to], panel.at[n, 4, to], yn, got, 'gather')
        if i:
            send(own, panel.at[n, 1], partner, ('p0', n), 'gather')

    def gather_forward(n, i):
        arrived(('forward', n, i), panel.at[n, 2, pl.ds(0, HALF)])
        at, to = piece(0, i), piece(1, i)
        send(panel.at[n, 2, at], panel.at[n, 6, at], yn, ('last', n), 'gather')
        send(panel.at[n, 4, to], panel.at[n, 6, to], xn, ('last', n), 'gather')

    def gather_near(n):
        arrived(('near', n), panel.at[n, 2])
        send(panel.at[n, 2], panel.at[n, 3], partner, ('p12', n), 'gather')
        send(panel.at[n, 4], panel.at[n, 5], partner, ('p12', n), 'gather')

    def gather_last(n):
        arrived(('last', n), panel.at[n, 6])
        send(panel.at[n, 6], panel.at[n, 7], partner, ('p3', n), 'gather')

    def zgather_start(n):
        for k in zorder:
            send(upan.at[n, c], upan.at[n, c], (zpeer(k), r), 'zgather', 'zgather')

    def zgather_wait(n):
        arrived('zgather', upan.at[n, pl.ds(0, 3)])
        return jnp.concatenate([upan[n, k] for k in range(4)], axis=1)

    def zsum_start(n, acc):
        acc_t = acc.T
        for k in range(4):
            upart[n, k] = acc_t[:, k * 128:(k + 1) * 128]
        for k in zorder:
            send(upart.at[n, zpeer(k)], uin.at[n, k - 1], (zpeer(k), r), 'zsum', 'zsum')

    def zsum_wait(n):
        arrived('zsum', uin.at[n])
        total = (upart[n, c] + uin[n, 0]) + (uin[n, 1] + uin[n, 2])
        nxt = total.astype(BF16)
        usum[...] = usum[...] + nxt.astype(F32)
        return nxt

    def mask_step(step, carry):
        mask_copy(step).wait()
        slot = mask_slot(step)
        part = step % per_slot
        buf = step % STAGES

        def convert(i, col):
            at = pl.multiple_of(i * 16, 16)
            x = stage[buf, pl.ds(at, 16), :].astype(F32)
            row = pl.multiple_of(part * rows + i * 16, 16)
            adj[slot, pl.ds(row, 16), :] = x.astype(BF16)
            lanes = x[:, :128]
            for t in range(1, width // 128):
                lanes = lanes + x[:, t * 128:(t + 1) * 128]
            rowacc[pl.ds(row, 16), :] += lanes
            return col + (x[:8] + x[8:])

        colacc[slot] += lax.fori_loop(0, rows // 16, convert, jnp.zeros((8, width), F32), unroll=2)

        @pl.when(step + STAGES < steps)
        def _():
            mask_copy(step + STAGES).start()

        return carry

    def column_sum(slot):
        return jnp.sum(colacc[slot], axis=0, keepdims=True)

    def mask_part(first, last):
        lax.fori_loop(steps * first // 8, steps * last // 8, mask_step, 0)

    with jax.named_scope('mask_a'):
        mask_part(0, 1)
    with jax.named_scope('barrier'):
        pl.semaphore_wait(barrier, len(peers))
    with jax.named_scope('inputs'):
        for copy in inputs:
            copy.wait()
        gather_start(0, 0)
        gather_start(0, 1)
        zgather_start(0)
        isum[...] = panel[0, 0].astype(F32)
        usum[...] = upan[0, c].astype(F32)
    with jax.named_scope('mask_b'):
        mask_part(1, 5)
        for d in range(4):
            deg_send[pl.ds(d, 1), :] = column_sum(2 * d + 1)
        send(deg_send, deg_recv, partner, 'dp', 'dp')
        mask_part(5, 6)
    with jax.named_scope('forward00'):
        gather_forward(0, 0)
    with jax.named_scope('mask_c'):
        mask_part(6, 7)
    with jax.named_scope('forward01'):
        gather_forward(0, 1)
    with jax.named_scope('mask_d'):
        mask_part(7, 8)

    with jax.named_scope('deg_sum'):
        udeg[...] = dot(jnp.ones((8, 128), BF16), rowacc[...].astype(BF16), NT)
        for k in zorder:
            send(udeg, udeg_in.at[k - 1], (zpeer(k), r), 'zd', 'zd')
        mine = jnp.concatenate(
            [column_sum(2 * d) for d in range(4)], axis=0)
    with jax.named_scope('deg_partner'):
        arrived('dp', deg_recv)
        deg_own[...] = mine + deg_recv[...]
        for k, device in enumerate((xn, yn, dg)):
            send(deg_own, deg_in.at[k], device, 'ds', 'ds')
        for d in range(4):
            far_send[d] = deg_own[d:d + 1, :]
            send(far_send.at[d], far_in.at[d], slots[2 * (3 - d) + 1], 'far', 'far')
    with jax.named_scope('deg_users'):
        arrived('zd', udeg_in)
        du = udeg[...] + jnp.sum(udeg_in[...], axis=0)
        inv = lax.rsqrt(jnp.maximum(du, 1.0))
        invu[...] = jnp.broadcast_to(inv[0:1, :], (128, users)).T
    with jax.named_scope('deg_items'):
        arrived('ds', deg_in)
    with jax.named_scope('deg_inv'):
        for d in range(4):
            total = deg_own[pl.ds(d, 1), :]
            for k in range(3):
                total = total + deg_in[k, pl.ds(d ^ (k + 1), 1), :]
            deg_fin[pl.ds(d, 1), :] = lax.rsqrt(jnp.maximum(total, 1.0))
        send(deg_fin, deg_oth, partner, 'df', 'df')
        arrived('far', far_in)
        gather_near(0)

    def normalize(slot, at=0, size=width):
        d = slot // 2
        cols = pl.ds(at, size)
        if slot == 7:
            total = jnp.sum(far_in[:, :, cols], axis=0)
            inv_item = lax.rsqrt(jnp.maximum(total, 1.0))
        else:
            inv_item = (deg_oth if slot % 2 else deg_fin)[d:d + 1, cols]

        step = 16 * max(1, width // 2 // size)

        def scale(i, carry):
            for j in range(step // 16):
                row = pl.ds(pl.multiple_of(i * step + j * 16, 16), 16)
                inv_user = jnp.concatenate([invu[row, :]] * (size // 128), axis=1)
                adj[slot, row, cols] = adj[slot, row, cols] * (inv_user * inv_item).astype(BF16)
            return carry

        lax.fori_loop(0, users // step, scale, 0, unroll=2)

    sizes = (width // 8, width // 4, width - 3 * width // 8)
    starts = (0, width // 8, 3 * width // 8)
    splits = [pl.ds(at, size) for at, size in zip(starts, sizes)]
    lo, hi = pl.ds(0, HALF), pl.ds(HALF, HALF)

    def items_diagonal(n, i=None):
        cols = pl.ds(0, width) if i is None else splits[i]
        send(sacc.at[n, 3, lo, cols], hop1.at[n, 0, :, cols], xn, ('hop1', n), 'sum')
        send(sacc.at[n, 3, hi, cols], hop1.at[n, 1, :, cols], yn, ('hop1', n), 'sum')

    def items_x(n):
        send(sacc.at[n, 1, lo], rown.at[n, 0], xn, ('direct', n), 'sum')

    def items_y(n):
        send(sacc.at[n, 2, hi], rown.at[n, 3], yn, ('direct', n), 'sum')

    def away(n, u, d):
        psend[n, d] = dot(u, adj[2 * d + 1], NN)
        send(psend.at[n, d], drecv.at[n, d], partner, ('partner', n, d), 'items')

    def near(n, u, d):
        part = dot(u, adj[2 * d], NN)
        if d:
            arrived(('partner', n, d), drecv.at[n, d])
            part = part + drecv[n, d]
        sacc[n, d] = part

    def items_first(u):
        n, d = 0, 3

        def theirs(i):
            cols = splits[i]
            normalize(2 * d + 1, starts[i], sizes[i])
            psend[n, d, :, cols] = dot(u, adj[2 * d + 1, :, cols], NN)
            if i:
                send(psend.at[n, d, :, cols], drecv.at[n, d, :, cols], partner, ('partner', n, d, i), 'items')
            else:
                for k, half in enumerate((lo, hi)):
                    send(psend.at[n, d, half, cols], hop1b.at[k], slots[3 + 2 * k], 'hop1b', 'items')

        def ours(i):
            cols = splits[i]
            normalize(2 * d, starts[i], sizes[i])
            sacc[n, d, :, cols] = dot(u, adj[2 * d, :, cols], NN)

        def both(i):
            cols = splits[i]
            arrived(('partner', n, d, i), drecv.at[n, d, :, cols])
            sacc[n, d, :, cols] = sacc[n, d, :, cols] + drecv[n, d, :, cols]
            items_diagonal(n, i)

        theirs(0)
        ours(0)
        items_diagonal(n, 0)
        theirs(1)
        theirs(2)
        for i in (1, 2):
            ours(i)
            both(i)
        arrived('df', deg_oth)

        for k in (1, 2):
            normalize(2 * k + 1)
            away(n, u, k)
        normalize(2)
        near(n, u, 1)
        items_x(n)
        normalize(4)
        near(n, u, 2)
        items_y(n)
        normalize(1)
        away(n, u, 0)
        normalize(0)
        near(n, u, 0)

    def items_later(n, u, hooks):
        away(n, u, 3)
        away(n, u, 1)
        hooks[0]()
        near(n, u, 3)
        hooks[1]()
        away(n, u, 2)
        away(n, u, 0)
        near(n, u, 1)
        hooks[2]()
        near(n, u, 2)
        near(n, u, 0)

    def items_mid(n, i):
        if i == 0:
            arrived(('hop1', n), hop1.at[n])
            if n == 0:
                arrived('hop1b', hop1b)
                for k in range(2):
                    hop1[n, k, :, splits[0]] = hop1[n, k, :, splits[0]] + hop1b[k]
        at = pl.ds(i * QUARTER, QUARTER)
        for h, device in enumerate((yn, xn)):
            block, part = 2 - h, piece(h, i)
            sacc[n, block, part] = sacc[n, block, part] + hop1[n, h, at]
            send(sacc.at[n, block, part], rown.at[n, block, at], device, ('hop2', n, i), 'sum')

    def items_finish(n, i):
        if i == 0:
            arrived(('partner', n, 0), drecv.at[n, 0])
            arrived(('direct', n), rown.at[n, pl.ds(0, 2)])
        arrived(('hop2', n, i), rown.at[n, 0])
        at = pl.ds(i * QUARTER, QUARTER)
        for h in (0, 1):
            rows_h = piece(h, i)
            total = ((sacc[n, 0, rows_h] + drecv[n, 0, rows_h]) + rown[n, h, at]) + rown[n, 2 + h, at]
            nxt = total.astype(BF16)
            isum[rows_h] = isum[rows_h] + nxt.astype(F32)
            if n + 1 < LAYERS:
                panel[n + 1, 0, rows_h] = nxt

    def user_partial(n, near_done=False, hook=None):
        def some(first, stride, count):
            def one(j, carry):
                at = first + stride * j
                uacc[...] += dot(adj[at], panel[n, at], NT)
                return carry

            lax.fori_loop(0, count, one, 0)

        arrived(('p0', n), panel.at[n, 1])
        uacc[...] = dot(adj[0], panel[n, 0], NT)
        some(1, 1, 1)
        if hook is not None:
            hook()
        if not near_done:
            gather_near(n)
        some(2, 2, 2)
        arrived(('p12', n), panel.at[n, pl.ds(2, 2)])
        some(3, 2, 2)
        gather_last(n)
        some(6, 1, 1)
        arrived(('p3', n), panel.at[n, 7])
        some(7, 1, 1)
        return uacc[...]

    scope = jax.named_scope

    def mid(n):
        items_mid(n, 0)
        items_mid(n, 1)

    def finish(n, i):
        with scope(f'finish{n}{i}'):
            items_finish(n, i)
            gather_start(n + 1, i)

    def forward(n, i):
        with scope(f'forward{n}{i}'):
            gather_forward(n, i)

    def nothing():
        pass

    with scope('u0'):
        u0 = zgather_wait(0)
    with scope('items0'):
        items_first(u0)
    with scope('user0'):
        zsum_start(0, user_partial(0, True, lambda: mid(0)))
    finish(0, 0)
    with scope('zsum0'):
        upan[1, c] = zsum_wait(0)
        zgather_start(1)
    finish(0, 1)
    with scope('zgather1'):
        u1 = zgather_wait(1)
    with scope('items1'):
        forward(1, 0)
        items_later(1, u1, (lambda: forward(1, 1), lambda: items_diagonal(1), nothing))
        items_x(1)
        items_y(1)
    with scope('user1'):
        zsum_start(1, user_partial(1))
    with scope('mid1'):
        mid(1)
    with scope('zsum1'):
        upan[2, c] = zsum_wait(1)
        zgather_start(2)
    finish(1, 0)
    with scope('zgather2'):
        u2 = zgather_wait(2)
    with scope('items2'):
        items_later(2, u2, (nothing, lambda: finish(1, 1), lambda: forward(2, 0)))
        forward(2, 1)
        items_diagonal(2)
        items_x(2)
        items_y(2)
    with scope('user2'):
        zsum_start(2, user_partial(2))
    with scope('mid2'):
        items_mid(2, 0)

        @pl.when(core == 0)
        def _():
            items_mid(2, 1)

    with scope('zsum2'):
        zsum_wait(2)
        final_user = (usum[...] / (LAYERS + 1)).astype(BF16)
        fu_ref[...] = final_user
        upan[3, c] = final_user
        zgather_start(3)
    with scope('zgather3'):
        ufin = zgather_wait(3)
    with scope('pick'):
        local = qbuf[...] - r * users
        chosen = (lax.broadcasted_iota(jnp.int32, (users, local.shape[1]), 0)
                  == jnp.broadcast_to(local, (users, local.shape[1]))).astype(F32).astype(BF16)
        pk[0] = dot(ufin, chosen, NN).astype(BF16)

        @pl.when(core == 0)
        def _():
            send(pk.at[0], pk.at[1], partner, 'pick', 'pick')

        @pl.when(core == 1)
        def _():
            arrived('pick', pk.at[1])
            pk[2] = pk[0] + pk[1]
            for k, device in enumerate((xn, yn, dg)):
                send(pk.at[2], pk.at[3 + k], device, 'picks', 'picks')
            items_mid(2, 1)

    with scope('finish20'):
        items_finish(2, 0)
    with scope('picked'):
        @pl.when(core == 1)
        def _():
            arrived('picks', pk.at[pl.ds(3, 3)])
            total = pk[2]
            for k in range(3):
                total = total + pk[3 + k]
            pk[6] = total
            send(pk.at[6], pk.at[6], partner, 'picked', 'picked')
            sent('picks', pk.at[pl.ds(3, 3)])
            sent('picked', pk.at[6])

        @pl.when(core == 0)
        def _():
            arrived('picked', pk.at[6])
            sent('pick', pk.at[0])

        pick_ref[...] = pk[6].astype(F32).T.astype(BF16)
    with scope('finish21'):
        items_finish(2, 1)
        fi_ref[...] = (isum[...] / (LAYERS + 1)).astype(BF16)
    with scope('drain'):
        sent('gather', panel.at[:, pl.ds(0, 7)])
        sent('items', psend)
        sent('sum', sacc.at[:, pl.ds(1, 3)])
        sent('zsum', uin)
        sent('zgather', upan.at[:, pl.ds(0, 3)])
        for out, whole in (('dp', deg_send), ('zd', udeg_in), ('ds', deg_in), ('far', far_in),
                           ('df', deg_fin)):
            sent(out, whole)


def propagate(mask_blk, user_shard, item_shard, queries):
    users, items = mask_blk.shape
    width = items // 8
    per = user_shard.shape[1]
    n_query = queries.shape[0]
    vmem = pl.BlockSpec(memory_space=pltpu.VMEM)
    hbm = pl.BlockSpec(memory_space=pl.ANY)
    scratch = [
        pltpu.VMEM((8, users, width), BF16),
        pltpu.VMEM((STAGES, users // 4, width), jnp.int32),
        pltpu.VMEM((LAYERS, 8, EMB, width), BF16),
        pltpu.VMEM((LAYERS + 1, 4, EMB, per), BF16),
        pltpu.VMEM((LAYERS, 4, EMB, width), F32),
        pltpu.VMEM((LAYERS, 4, EMB, width), F32),
        pltpu.VMEM((LAYERS, 4, EMB, width), F32),
        pltpu.VMEM((LAYERS, 2, HALF, width), F32),
        pltpu.VMEM((2, HALF, width // 8), F32),
        pltpu.VMEM((LAYERS, 4, HALF, width), F32),
        pltpu.VMEM((EMB, width), F32),
        pltpu.VMEM((EMB, per), F32),
        pltpu.VMEM((8, 8, width), F32),
        pltpu.VMEM((users, 128), F32),
        pltpu.VMEM((4, width), F32),
        pltpu.VMEM((4, width), F32),
        pltpu.VMEM((4, width), F32),
        pltpu.VMEM((3, 4, width), F32),
        pltpu.VMEM((4, width), F32),
        pltpu.VMEM((4, width), F32),
        pltpu.VMEM((4, 1, width), F32),
        pltpu.VMEM((4, 1, width), F32),
        pltpu.VMEM((8, users), F32),
        pltpu.VMEM((3, 8, users), F32),
        pltpu.VMEM((users, 128), F32),
        pltpu.VMEM((users, EMB), F32),
        pltpu.VMEM((LAYERS, 4, EMB, per), F32),
        pltpu.VMEM((LAYERS, 3, EMB, per), F32),
        pltpu.VMEM((7, EMB, n_query), BF16),
        pltpu.VMEM((1, n_query), jnp.int32),
        pltpu.SemaphoreType.DMA((STAGES,)),
        pltpu.SemaphoreType.DMA((3,)),
        pltpu.SemaphoreType.DMA((N_SENT,)),
        pltpu.SemaphoreType.DMA((N_GOT,)),
    ]
    return pl.pallas_call(
        kernel,
        out_shape=(pltpu.VMEM((EMB, per), BF16),
                   pltpu.VMEM((EMB, width), BF16),
                   pltpu.VMEM((n_query, EMB), BF16)),
        in_specs=[hbm, hbm, hbm, hbm],
        out_specs=(vmem, vmem, vmem),
        scratch_shapes=scratch,
        compiler_params=pltpu.CompilerParams(
            collective_id=0, has_side_effects=True, vmem_limit_bytes=61_600_000),
        name='propagate',
    )(mask_blk, item_shard, user_shard, queries.reshape(1, n_query))


def output_kernel(pick_ref, item_ref, user_ref, scores_ref, fi_ref, fu_ref, scores, sem):
    copies = [pltpu.make_async_copy(item_ref, fi_ref, sem.at[0]),
              pltpu.make_async_copy(user_ref, fu_ref, sem.at[1])]
    for copy in copies:
        copy.start()
    picked = pick_ref[...]
    cols = scores.shape[1] // 4
    for i in range(4):
        at = pl.ds(i * cols, cols)
        scores[:, at] = dot(picked, item_ref[:, at], NN)
        copy = pltpu.make_async_copy(scores.at[:, at], scores_ref.at[:, at], sem.at[2 + i])
        copy.start()
        copies.append(copy)
    for copy in copies:
        copy.wait()


def outputs(fu_t, fi_t, picked):
    n_query = picked.shape[0]
    width, per = fi_t.shape[1], fu_t.shape[1]
    hbm = pl.BlockSpec(memory_space=pl.ANY)
    vmem = pl.BlockSpec(memory_space=pltpu.VMEM)
    args = [pltpu.with_memory_space_constraint(x, pltpu.VMEM) for x in (picked, fi_t, fu_t)]
    return pl.pallas_call(
        output_kernel,
        out_shape=(jax.ShapeDtypeStruct((n_query, width), F32),
                   jax.ShapeDtypeStruct((EMB, width), BF16),
                   jax.ShapeDtypeStruct((EMB, per), BF16)),
        in_specs=[vmem, vmem, vmem],
        out_specs=(hbm, hbm, hbm),
        scratch_shapes=[pltpu.VMEM((n_query, width), F32), pltpu.SemaphoreType.DMA((6,))],
        name='outputs',
    )(*args)


def solution(mesh):
    def device_step(mask_blk, user_shard, item_shard, queries):
        fu_t, fi_t, picked = propagate(mask_blk, user_shard.T, item_shard.T, queries)
        scores, fi_t, fu_t = outputs(fu_t, fi_t, picked)
        return fu_t.T, fi_t.T, scores

    return jax.shard_map(
        device_step, mesh=mesh,
        in_specs=(P('row', 'col'), P(('row', 'col'), None), P(('col', 'row'), None), P()),
        out_specs=(P(('row', 'col'), None), P(('col', 'row'), None), P(None, ('col', 'row'))),
        check_vma=False)
```

```python
import jax
import jax.numpy as jnp
from jax import lax
from jax.experimental import pallas as pl
from jax.experimental.pallas import tpu as pltpu
from jax.sharding import PartitionSpec as P

LAYERS = 3
EMB = 64
HALF = EMB // 2
QUARTER = EMB // 4
NT = (((1,), (1,)), ((), ()))
NN = (((1,), (0,)), ((), ()))
TN = (((0,), (0,)), ((), ()))
F32 = jnp.float32
BF16 = jnp.bfloat16
STAGES = 8
N_SENT = 13
N_GOT = 43


def dot(lhs, rhs, dims):
    return lax.dot_general(lhs, rhs, dims, preferred_element_type=F32)


def kernel(mask_ref, item_ref, user_ref, query_ref, fu_ref, fi_ref, pick_ref,
           adj, stage, panel, upan, psend, drecv, sacc, hop1, hop1b, rown, isum, usum,
           colacc, rowacc, deg_send, deg_recv, deg_own, deg_in, deg_fin, deg_oth, far_send, far_in,
           udeg, udeg_in, invu, uacc, upart, uin, pk, qbuf, stage_sem, in_sem, send_sem, recv_sem):
    c = lax.axis_index('col')
    r = lax.axis_index('row')
    users = rowacc.shape[0]
    width = adj.shape[2]
    rows = stage.shape[1]
    per_slot = users // rows
    core, cx, cy = r % 2, (r // 2) % 2, r // 4

    def flip(bit, by):
        return (bit + by) % 2

    def plane(d, k):
        return flip(cy, d // 2) * 4 + flip(cx, d % 2) * 2 + flip(core, k)

    def zpeer(k):
        return flip(c // 2, k // 2) * 2 + flip(c % 2, k % 2)

    slots = {d * 2 + k: (c, plane(d, k)) for d in range(4) for k in range(2)}
    partner, xn, yn, dg = slots[1], slots[2], slots[4], slots[6]
    far_z = 3 - (c + 1) // 2 % 2
    zorder = (far_z, 5 - far_z, 1)
    zn = {k: (zpeer(k), r) for k in (1, 2, 3)}

    got_index, out_index = {}, {}

    def parity(key):
        return key if isinstance(key, str) else (key[0], key[1] % 2) + key[2:]

    def send(src, dst, device, got, out):
        copy = pltpu.make_async_remote_copy(
            src_ref=src, dst_ref=dst,
            send_sem=send_sem.at[out_index.setdefault(out, len(out_index))],
            recv_sem=recv_sem.at[got_index.setdefault(parity(got), len(got_index))],
            device_id=device, device_id_type=pl.DeviceIdType.MESH)
        copy.start()

    def group(whole, got, out):
        return pltpu.make_async_remote_copy(
            src_ref=whole, dst_ref=whole, send_sem=send_sem.at[out], recv_sem=recv_sem.at[got],
            device_id=partner, device_id_type=pl.DeviceIdType.MESH)

    def arrived(got, whole):
        group(whole, got_index[parity(got)], 0).wait_recv()

    def sent(out, whole):
        group(whole, 0, out_index[out]).wait_send()

    def mask_slot(step):
        return (step // per_slot % 4) * 2 + 1 - step // (4 * per_slot)

    def mask_copy(step):
        slot = mask_slot(step)
        part = step % per_slot
        col = plane(slot // 2, slot % 2) * width
        return pltpu.make_async_copy(
            mask_ref.at[pl.ds(pl.multiple_of(part * rows, rows), rows),
                        pl.ds(pl.multiple_of(col, width), width)],
            stage.at[step % STAGES], stage_sem.at[step % STAGES])

    steps = 8 * per_slot
    inputs = [pltpu.make_async_copy(item_ref, panel.at[0, 0], in_sem.at[0]),
              pltpu.make_async_copy(user_ref, upan.at[0, c], in_sem.at[1]),
              pltpu.make_async_copy(query_ref, qbuf, in_sem.at[2])]
    for copy in inputs:
        copy.start()
    for s in range(STAGES):
        mask_copy(jnp.int32(s)).start()


    barrier = pltpu.get_barrier_semaphore()
    peers = [device for k, device in slots.items() if k] + [zn[k] for k in (1, 2, 3)]
    for device in peers:
        pl.semaphore_signal(barrier, inc=1, device_id=device, device_id_type=pl.DeviceIdType.MESH)

    rowacc[...] = jnp.zeros_like(rowacc)
    colacc[...] = jnp.zeros_like(colacc)

    def piece(h, i):
        return pl.ds(h * HALF + i * QUARTER, QUARTER)

    def gather_start(n, i):
        own = panel.at[n, 0]
        for h in (0, 1):
            got = ('forward', n, i) if h == 0 else ('near', n)
            at, to = piece(h, i), piece(1 - h, i)
            send(own.at[at], panel.at[n, 2, at], xn, got, 'gather')
            send(own.at[to], panel.at[n, 4, to], yn, got, 'gather')
        if i:
            send(own, panel.at[n, 1], partner, ('p0', n), 'gather')

    def gather_forward(n, i):
        arrived(('forward', n, i), panel.at[n, 2, pl.ds(0, HALF)])
        at, to = piece(0, i), piece(1, i)
        send(panel.at[n, 2, at], panel.at[n, 6, at], yn, ('last', n), 'gather')
        send(panel.at[n, 4, to], panel.at[n, 6, to], xn, ('last', n), 'gather')

    def gather_near(n):
        arrived(('near', n), panel.at[n, 2])
        send(panel.at[n, 2], panel.at[n, 3], partner, ('p12', n), 'gather')
        send(panel.at[n, 4], panel.at[n, 5], partner, ('p12', n), 'gather')

    def gather_last(n):
        arrived(('last', n), panel.at[n, 6])
        send(panel.at[n, 6], panel.at[n, 7], partner, ('p3', n), 'gather')

    def zgather_start(n):
        for k in zorder:
            send(upan.at[n, c], upan.at[n, c], (zpeer(k), r), 'zgather', 'zgather')

    def zgather_wait(n):
        arrived('zgather', upan.at[n, pl.ds(0, 3)])
        return jnp.concatenate([upan[n, k] for k in range(4)], axis=1)

    def zsum_start(n, acc):
        acc_t = acc.T
        for k in range(4):
            upart[n, k] = acc_t[:, k * 128:(k + 1) * 128]
        for k in zorder:
            send(upart.at[n, zpeer(k)], uin.at[n, k - 1], (zpeer(k), r), 'zsum', 'zsum')

    def zsum_wait(n):
        arrived('zsum', uin.at[n])
        total = (upart[n, c] + uin[n, 0]) + (uin[n, 1] + uin[n, 2])
        nxt = total.astype(BF16)
        usum[...] = usum[...] + nxt.astype(F32)
        return nxt

    def mask_step(step, carry):
        mask_copy(step).wait()
        slot = mask_slot(step)
        part = step % per_slot
        buf = step % STAGES

        def convert(i, col):
            at = pl.multiple_of(i * 16, 16)
            x = stage[buf, pl.ds(at, 16), :].astype(F32)
            row = pl.multiple_of(part * rows + i * 16, 16)
            adj[slot, pl.ds(row, 16), :] = x.astype(BF16)
            lanes = x[:, :128]
            for t in range(1, width // 128):
                lanes = lanes + x[:, t * 128:(t + 1) * 128]
            rowacc[pl.ds(row, 16), :] += lanes
            return col + (x[:8] + x[8:])

        colacc[slot] += lax.fori_loop(0, rows // 16, convert, jnp.zeros((8, width), F32), unroll=2)

        @pl.when(step + STAGES < steps)
        def _():
            mask_copy(step + STAGES).start()

        return carry

    def column_sum(slot):
        return jnp.sum(colacc[slot], axis=0, keepdims=True)

    def mask_part(first, last):
        lax.fori_loop(steps * first // 8, steps * last // 8, mask_step, 0)

    with jax.named_scope('mask_a'):
        mask_part(0, 1)
    with jax.named_scope('barrier'):
        pl.semaphore_wait(barrier, len(peers))
    with jax.named_scope('inputs'):
        for copy in inputs:
            copy.wait()
        gather_start(0, 0)
        gather_start(0, 1)
        zgather_start(0)
        isum[...] = panel[0, 0].astype(F32)
        usum[...] = upan[0, c].astype(F32)
    with jax.named_scope('mask_b'):
        mask_part(1, 5)
        for d in range(4):
            deg_send[pl.ds(d, 1), :] = column_sum(2 * d + 1)
        send(deg_send, deg_recv, partner, 'dp', 'dp')
        mask_part(5, 6)
    with jax.named_scope('forward00'):
        gather_forward(0, 0)
    with jax.named_scope('mask_c'):
        mask_part(6, 7)
    with jax.named_scope('forward01'):
        gather_forward(0, 1)
    with jax.named_scope('mask_d'):
        mask_part(7, 8)

    with jax.named_scope('deg_sum'):
        udeg[...] = dot(jnp.ones((8, 128), BF16), rowacc[...].astype(BF16), NT)
        for k in zorder:
            send(udeg, udeg_in.at[k - 1], (zpeer(k), r), 'zd', 'zd')
        mine = jnp.concatenate(
            [column_sum(2 * d) for d in range(4)], axis=0)
    with jax.named_scope('deg_partner'):
        arrived('dp', deg_recv)
        deg_own[...] = mine + deg_recv[...]
        for k, device in enumerate((xn, yn, dg)):
            send(deg_own, deg_in.at[k], device, 'ds', 'ds')
        for d in range(4):
            far_send[d] = deg_own[d:d + 1, :]
            send(far_send.at[d], far_in.at[d], slots[2 * (3 - d) + 1], 'far', 'far')
    with jax.named_scope('deg_users'):
        arrived('zd', udeg_in)
        du = udeg[...] + jnp.sum(udeg_in[...], axis=0)
        inv = lax.rsqrt(jnp.maximum(du, 1.0))
        invu[...] = jnp.broadcast_to(inv[0:1, :], (128, users)).T
    with jax.named_scope('deg_items'):
        arrived('ds', deg_in)
    with jax.named_scope('deg_inv'):
        for d in range(4):
            total = deg_own[pl.ds(d, 1), :]
            for k in range(3):
                total = total + deg_in[k, pl.ds(d ^ (k + 1), 1), :]
            deg_fin[pl.ds(d, 1), :] = lax.rsqrt(jnp.maximum(total, 1.0))
        send(deg_fin, deg_oth, partner, 'df', 'df')
        arrived('far', far_in)
        gather_near(0)

    def normalize(slot, at=0, size=width):
        d = slot // 2
        cols = pl.ds(at, size)
        if slot == 7:
            total = jnp.sum(far_in[:, :, cols], axis=0)
            inv_item = lax.rsqrt(jnp.maximum(total, 1.0))
        else:
            inv_item = (deg_oth if slot % 2 else deg_fin)[d:d + 1, cols]

        step = 16 * max(1, width // 2 // size)

        def scale(i, carry):
            for j in range(step // 16):
                row = pl.ds(pl.multiple_of(i * step + j * 16, 16), 16)
                inv_user = jnp.concatenate([invu[row, :]] * (size // 128), axis=1)
                adj[slot, row, cols] = adj[slot, row, cols] * (inv_user * inv_item).astype(BF16)
            return carry

        lax.fori_loop(0, users // step, scale, 0, unroll=2)

    sizes = (width // 8, width // 4, width - 3 * width // 8)
    starts = (0, width // 8, 3 * width // 8)
    splits = [pl.ds(at, size) for at, size in zip(starts, sizes)]
    lo, hi = pl.ds(0, HALF), pl.ds(HALF, HALF)

    def items_diagonal(n, i=None):
        cols = pl.ds(0, width) if i is None else splits[i]
        send(sacc.at[n, 3, lo, cols], hop1.at[n, 0, :, cols], xn, ('hop1', n), 'sum')
        send(sacc.at[n, 3, hi, cols], hop1.at[n, 1, :, cols], yn, ('hop1', n), 'sum')

    def items_x(n):
        send(sacc.at[n, 1, lo], rown.at[n, 0], xn, ('direct', n), 'sum')

    def items_y(n):
        send(sacc.at[n, 2, hi], rown.at[n, 3], yn, ('direct', n), 'sum')

    def away(n, u, d):
        psend[n, d] = dot(u, adj[2 * d + 1], NN)
        send(psend.at[n, d], drecv.at[n, d], partner, ('partner', n, d), 'items')

    def near(n, u, d):
        part = dot(u, adj[2 * d], NN)
        if d:
            arrived(('partner', n, d), drecv.at[n, d])
            part = part + drecv[n, d]
        sacc[n, d] = part

    def items_first(u):
        n, d = 0, 3

        def theirs(i):
            cols = splits[i]
            normalize(2 * d + 1, starts[i], sizes[i])
            psend[n, d, :, cols] = dot(u, adj[2 * d + 1, :, cols], NN)
            if i:
                send(psend.at[n, d, :, cols], drecv.at[n, d, :, cols], partner, ('partner', n, d, i), 'items')
            else:
                for k, half in enumerate((lo, hi)):
                    send(psend.at[n, d, half, cols], hop1b.at[k], slots[3 + 2 * k], 'hop1b', 'items')

        def ours(i):
            cols = splits[i]
            normalize(2 * d, starts[i], sizes[i])
            sacc[n, d, :, cols] = dot(u, adj[2 * d, :, cols], NN)

        def both(i):
            cols = splits[i]
            arrived(('partner', n, d, i), drecv.at[n, d, :, cols])
            sacc[n, d, :, cols] = sacc[n, d, :, cols] + drecv[n, d, :, cols]
            items_diagonal(n, i)

        theirs(0)
        ours(0)
        items_diagonal(n, 0)
        theirs(1)
        theirs(2)
        for i in (1, 2):
            ours(i)
            both(i)
        arrived('df', deg_oth)

        for k in (1, 2):
            normalize(2 * k + 1)
            away(n, u, k)
        normalize(2)
        near(n, u, 1)
        items_x(n)
        normalize(4)
        near(n, u, 2)
        items_y(n)
        normalize(1)
        away(n, u, 0)
        normalize(0)
        near(n, u, 0)

    def items_later(n, u, hooks):
        away(n, u, 3)
        away(n, u, 1)
        hooks[0]()
        near(n, u, 3)
        hooks[1]()
        away(n, u, 2)
        away(n, u, 0)
        near(n, u, 1)
        hooks[2]()
        near(n, u, 2)
        near(n, u, 0)

    def items_mid(n, i):
        if i == 0:
            arrived(('hop1', n), hop1.at[n])
            if n == 0:
                arrived('hop1b', hop1b)
                for k in range(2):
                    hop1[n, k, :, splits[0]] = hop1[n, k, :, splits[0]] + hop1b[k]
        at = pl.ds(i * QUARTER, QUARTER)
        for h, device in enumerate((yn, xn)):
            block, part = 2 - h, piece(h, i)
            sacc[n, block, part] = sacc[n, block, part] + hop1[n, h, at]
            send(sacc.at[n, block, part], rown.at[n, block, at], device, ('hop2', n, i), 'sum')

    def items_finish(n, i):
        if i == 0:
            arrived(('partner', n, 0), drecv.at[n, 0])
            arrived(('direct', n), rown.at[n, pl.ds(0, 2)])
        arrived(('hop2', n, i), rown.at[n, 0])
        at = pl.ds(i * QUARTER, QUARTER)
        for h in (0, 1):
            rows_h = piece(h, i)
            total = ((sacc[n, 0, rows_h] + drecv[n, 0, rows_h]) + rown[n, h, at]) + rown[n, 2 + h, at]
            nxt = total.astype(BF16)
            isum[rows_h] = isum[rows_h] + nxt.astype(F32)
            if n + 1 < LAYERS:
                panel[n + 1, 0, rows_h] = nxt

    def user_partial(n, near_done=False, hook=None):
        def some(first, stride, count):
            def one(j, carry):
                at = first + stride * j
                uacc[...] += dot(adj[at], panel[n, at], NT)
                return carry

            lax.fori_loop(0, count, one, 0)

        arrived(('p0', n), panel.at[n, 1])
        uacc[...] = dot(adj[0], panel[n, 0], NT)
        some(1, 1, 1)
        if hook is not None:
            hook()
        if not near_done:
            gather_near(n)
        some(2, 2, 2)
        arrived(('p12', n), panel.at[n, pl.ds(2, 2)])
        some(3, 2, 2)
        gather_last(n)
        some(6, 1, 1)
        arrived(('p3', n), panel.at[n, 7])
        some(7, 1, 1)
        return uacc[...]

    scope = jax.named_scope

    def mid(n):
        items_mid(n, 0)
        items_mid(n, 1)

    def finish(n, i):
        with scope(f'finish{n}{i}'):
            items_finish(n, i)
            gather_start(n + 1, i)

    def forward(n, i):
        with scope(f'forward{n}{i}'):
            gather_forward(n, i)

    def nothing():
        pass

    with scope('u0'):
        u0 = zgather_wait(0)
    with scope('items0'):
        items_first(u0)
    with scope('user0'):
        zsum_start(0, user_partial(0, True, lambda: mid(0)))
    finish(0, 0)
    with scope('zsum0'):
        upan[1, c] = zsum_wait(0)
        zgather_start(1)
    finish(0, 1)
    with scope('zgather1'):
        u1 = zgather_wait(1)
    with scope('items1'):
        forward(1, 0)
        items_later(1, u1, (lambda: forward(1, 1), lambda: items_diagonal(1), nothing))
        items_x(1)
        items_y(1)
    with scope('user1'):
        zsum_start(1, user_partial(1))
    with scope('mid1'):
        mid(1)
    with scope('zsum1'):
        upan[2, c] = zsum_wait(1)
        zgather_start(2)
    finish(1, 0)
    with scope('zgather2'):
        u2 = zgather_wait(2)
    with scope('items2'):
        items_later(2, u2, (nothing, lambda: finish(1, 1), lambda: forward(2, 0)))
        forward(2, 1)
        items_diagonal(2)
        items_x(2)
        items_y(2)
    with scope('user2'):
        zsum_start(2, user_partial(2))
    with scope('mid2'):
        items_mid(2, 0)

        @pl.when(core == 0)
        def _():
            items_mid(2, 1)

    with scope('zsum2'):
        zsum_wait(2)
        final_user = (usum[...] / (LAYERS + 1)).astype(BF16)
        fu_ref[...] = final_user
        upan[3, c] = final_user
        zgather_start(3)
    with scope('zgather3'):
        ufin = zgather_wait(3)
    with scope('pick'):
        local = qbuf[...] - r * users
        chosen = (lax.broadcasted_iota(jnp.int32, (users, local.shape[1]), 0)
                  == jnp.broadcast_to(local, (users, local.shape[1]))).astype(F32).astype(BF16)
        pk[0] = dot(ufin, chosen, NN).astype(BF16)

        @pl.when(core == 0)
        def _():
            send(pk.at[0], pk.at[1], partner, 'pick', 'pick')

        @pl.when(core == 1)
        def _():
            arrived('pick', pk.at[1])
            pk[2] = pk[0] + pk[1]
            for k, device in enumerate((xn, yn, dg)):
                send(pk.at[2], pk.at[3 + k], device, 'picks', 'picks')
            items_mid(2, 1)

    with scope('finish20'):
        items_finish(2, 0)
    with scope('picked'):
        @pl.when(core == 1)
        def _():
            arrived('picks', pk.at[pl.ds(3, 3)])
            total = pk[2]
            for k in range(3):
                total = total + pk[3 + k]
            pk[6] = total
            send(pk.at[6], pk.at[6], partner, 'picked', 'picked')
            sent('picks', pk.at[pl.ds(3, 3)])
            sent('picked', pk.at[6])

        @pl.when(core == 0)
        def _():
            arrived('picked', pk.at[6])
            sent('pick', pk.at[0])

        pick_ref[...] = pk[6].astype(F32).T.astype(BF16)
    with scope('finish21'):
        items_finish(2, 1)
        fi_ref[...] = (isum[...] / (LAYERS + 1)).astype(BF16)
    with scope('drain'):
        sent('gather', panel.at[:, pl.ds(0, 7)])
        sent('items', psend)
        sent('sum', sacc.at[:, pl.ds(1, 3)])
        sent('zsum', uin)
        sent('zgather', upan.at[:, pl.ds(0, 3)])
        for out, whole in (('dp', deg_send), ('zd', udeg_in), ('ds', deg_in), ('far', far_in),
                           ('df', deg_fin)):
            sent(out, whole)


def propagate(mask_blk, user_shard, item_shard, queries):
    users, items = mask_blk.shape
    width = items // 8
    per = user_shard.shape[1]
    n_query = queries.shape[0]
    vmem = pl.BlockSpec(memory_space=pltpu.VMEM)
    hbm = pl.BlockSpec(memory_space=pl.ANY)
    scratch = [
        pltpu.VMEM((8, users, width), BF16),
        pltpu.VMEM((STAGES, users // 4, width), jnp.int32),
        pltpu.VMEM((LAYERS, 8, EMB, width), BF16),
        pltpu.VMEM((LAYERS + 1, 4, EMB, per), BF16),
        pltpu.VMEM((LAYERS, 4, EMB, width), F32),
        pltpu.VMEM((LAYERS, 4, EMB, width), F32),
        pltpu.VMEM((LAYERS, 4, EMB, width), F32),
        pltpu.VMEM((LAYERS, 2, HALF, width), F32),
        pltpu.VMEM((2, HALF, width // 8), F32),
        pltpu.VMEM((LAYERS, 4, HALF, width), F32),
        pltpu.VMEM((EMB, width), F32),
        pltpu.VMEM((EMB, per), F32),
        pltpu.VMEM((8, 8, width), F32),
        pltpu.VMEM((users, 128), F32),
        pltpu.VMEM((4, width), F32),
        pltpu.VMEM((4, width), F32),
        pltpu.VMEM((4, width), F32),
        pltpu.VMEM((3, 4, width), F32),
        pltpu.VMEM((4, width), F32),
        pltpu.VMEM((4, width), F32),
        pltpu.VMEM((4, 1, width), F32),
        pltpu.VMEM((4, 1, width), F32),
        pltpu.VMEM((8, users), F32),
        pltpu.VMEM((3, 8, users), F32),
        pltpu.VMEM((users, 128), F32),
        pltpu.VMEM((users, EMB), F32),
        pltpu.VMEM((LAYERS, 4, EMB, per), F32),
        pltpu.VMEM((LAYERS, 3, EMB, per), F32),
        pltpu.VMEM((7, EMB, n_query), BF16),
        pltpu.VMEM((1, n_query), jnp.int32),
        pltpu.SemaphoreType.DMA((STAGES,)),
        pltpu.SemaphoreType.DMA((3,)),
        pltpu.SemaphoreType.DMA((N_SENT,)),
        pltpu.SemaphoreType.DMA((N_GOT,)),
    ]
    return pl.pallas_call(
        kernel,
        out_shape=(pltpu.VMEM((EMB, per), BF16),
                   pltpu.VMEM((EMB, width), BF16),
                   pltpu.VMEM((n_query, EMB), BF16)),
        in_specs=[hbm, hbm, hbm, hbm],
        out_specs=(vmem, vmem, vmem),
        scratch_shapes=scratch,
        compiler_params=pltpu.CompilerParams(
            collective_id=0, has_side_effects=True, vmem_limit_bytes=61_600_000),
        name='propagate',
    )(mask_blk, item_shard, user_shard, queries.reshape(1, n_query))


def output_kernel(pick_ref, item_ref, user_ref, scores_ref, fi_ref, fu_ref, scores, sem):
    copies = [pltpu.make_async_copy(item_ref, fi_ref, sem.at[0]),
              pltpu.make_async_copy(user_ref, fu_ref, sem.at[1])]
    for copy in copies:
        copy.start()
    picked = pick_ref[...]
    cols = scores.shape[1] // 4
    for i in range(4):
        at = pl.ds(i * cols, cols)
        scores[:, at] = dot(picked, item_ref[:, at], NN)
        copy = pltpu.make_async_copy(scores.at[:, at], scores_ref.at[:, at], sem.at[2 + i])
        copy.start()
        copies.append(copy)
    for copy in copies:
        copy.wait()


def outputs(fu_t, fi_t, picked):
    n_query = picked.shape[0]
    width, per = fi_t.shape[1], fu_t.shape[1]
    hbm = pl.BlockSpec(memory_space=pl.ANY)
    vmem = pl.BlockSpec(memory_space=pltpu.VMEM)
    args = [pltpu.with_memory_space_constraint(x, pltpu.VMEM) for x in (picked, fi_t, fu_t)]
    return pl.pallas_call(
        output_kernel,
        out_shape=(jax.ShapeDtypeStruct((n_query, width), F32),
                   jax.ShapeDtypeStruct((EMB, width), BF16),
                   jax.ShapeDtypeStruct((EMB, per), BF16)),
        in_specs=[vmem, vmem, vmem],
        out_specs=(hbm, hbm, hbm),
        scratch_shapes=[pltpu.VMEM((n_query, width), F32), pltpu.SemaphoreType.DMA((6,))],
        name='outputs',
    )(*args)


def solution(mesh):
    def device_step(mask_blk, user_shard, item_shard, queries):
        fu_t, fi_t, picked = propagate(mask_blk, user_shard.T, item_shard.T, queries)
        scores, fi_t, fu_t = outputs(fu_t, fi_t, picked)
        return fu_t.T, fi_t.T, scores

    return jax.shard_map(
        device_step, mesh=mesh,
        in_specs=(P('row', 'col'), P(('row', 'col'), None), P(('col', 'row'), None), P()),
        out_specs=(P(('row', 'col'), None), P(('col', 'row'), None), P(None, ('col', 'row'))),
        check_vma=False)
```

```python
import jax
import jax.numpy as jnp
from jax import lax
from jax.experimental import pallas as pl
from jax.experimental.pallas import tpu as pltpu
from jax.sharding import PartitionSpec as P

LAYERS = 3
EMB = 64
HALF = EMB // 2
QUARTER = EMB // 4
NT = (((1,), (1,)), ((), ()))
NN = (((1,), (0,)), ((), ()))
TN = (((0,), (0,)), ((), ()))
F32 = jnp.float32
BF16 = jnp.bfloat16
STAGES = 8
N_SENT = 13
N_GOT = 43


def dot(lhs, rhs, dims):
    return lax.dot_general(lhs, rhs, dims, preferred_element_type=F32)


def kernel(mask_ref, item_ref, user_ref, query_ref, fu_ref, fi_ref, pick_ref,
           adj, stage, panel, upan, psend, drecv, sacc, hop1, hop1b, rown, isum, usum,
           colacc, rowacc, deg_send, deg_recv, deg_own, deg_in, deg_fin, deg_oth, far_send, far_in,
           udeg, udeg_in, invu, uacc, upart, uin, pk, qbuf, stage_sem, in_sem, send_sem, recv_sem):
    c = lax.axis_index('col')
    r = lax.axis_index('row')
    users = rowacc.shape[0]
    width = adj.shape[2]
    rows = stage.shape[1]
    per_slot = users // rows
    core, cx, cy = r % 2, (r // 2) % 2, r // 4

    def flip(bit, by):
        return (bit + by) % 2

    def plane(d, k):
        return flip(cy, d // 2) * 4 + flip(cx, d % 2) * 2 + flip(core, k)

    def zpeer(k):
        return flip(c // 2, k // 2) * 2 + flip(c % 2, k % 2)

    slots = {d * 2 + k: (c, plane(d, k)) for d in range(4) for k in range(2)}
    partner, xn, yn, dg = slots[1], slots[2], slots[4], slots[6]
    far_z = 3 - (c + 1) // 2 % 2
    zorder = (far_z, 5 - far_z, 1)
    zn = {k: (zpeer(k), r) for k in (1, 2, 3)}

    got_index, out_index = {}, {}

    def parity(key):
        return key if isinstance(key, str) else (key[0], key[1] % 2) + key[2:]

    def send(src, dst, device, got, out):
        copy = pltpu.make_async_remote_copy(
            src_ref=src, dst_ref=dst,
            send_sem=send_sem.at[out_index.setdefault(out, len(out_index))],
            recv_sem=recv_sem.at[got_index.setdefault(parity(got), len(got_index))],
            device_id=device, device_id_type=pl.DeviceIdType.MESH)
        copy.start()

    def group(whole, got, out):
        return pltpu.make_async_remote_copy(
            src_ref=whole, dst_ref=whole, send_sem=send_sem.at[out], recv_sem=recv_sem.at[got],
            device_id=partner, device_id_type=pl.DeviceIdType.MESH)

    def arrived(got, whole):
        group(whole, got_index[parity(got)], 0).wait_recv()

    def sent(out, whole):
        group(whole, 0, out_index[out]).wait_send()

    def mask_slot(step):
        return (step // per_slot % 4) * 2 + 1 - step // (4 * per_slot)

    def mask_copy(step):
        slot = mask_slot(step)
        part = step % per_slot
        col = plane(slot // 2, slot % 2) * width
        return pltpu.make_async_copy(
            mask_ref.at[pl.ds(pl.multiple_of(part * rows, rows), rows),
                        pl.ds(pl.multiple_of(col, width), width)],
            stage.at[step % STAGES], stage_sem.at[step % STAGES])

    steps = 8 * per_slot
    inputs = [pltpu.make_async_copy(item_ref, panel.at[0, 0], in_sem.at[0]),
              pltpu.make_async_copy(user_ref, upan.at[0, c], in_sem.at[1]),
              pltpu.make_async_copy(query_ref, qbuf, in_sem.at[2])]
    for copy in inputs:
        copy.start()
    for s in range(STAGES):
        mask_copy(jnp.int32(s)).start()


    barrier = pltpu.get_barrier_semaphore()
    peers = [device for k, device in slots.items() if k] + [zn[k] for k in (1, 2, 3)]
    for device in peers:
        pl.semaphore_signal(barrier, inc=1, device_id=device, device_id_type=pl.DeviceIdType.MESH)

    rowacc[...] = jnp.zeros_like(rowacc)
    colacc[...] = jnp.zeros_like(colacc)

    def piece(h, i):
        return pl.ds(h * HALF + i * QUARTER, QUARTER)

    def gather_start(n, i):
        own = panel.at[n, 0]
        for h in (0, 1):
            got = ('forward', n, i) if h == 0 else ('near', n)
            at, to = piece(h, i), piece(1 - h, i)
            send(own.at[at], panel.at[n, 2, at], xn, got, 'gather')
            send(own.at[to], panel.at[n, 4, to], yn, got, 'gather')
        if i:
            send(own, panel.at[n, 1], partner, ('p0', n), 'gather')

    def gather_forward(n, i):
        arrived(('forward', n, i), panel.at[n, 2, pl.ds(0, HALF)])
        at, to = piece(0, i), piece(1, i)
        send(panel.at[n, 2, at], panel.at[n, 6, at], yn, ('last', n), 'gather')
        send(panel.at[n, 4, to], panel.at[n, 6, to], xn, ('last', n), 'gather')

    def gather_near(n):
        arrived(('near', n), panel.at[n, 2])
        send(panel.at[n, 2], panel.at[n, 3], partner, ('p12', n), 'gather')
        send(panel.at[n, 4], panel.at[n, 5], partner, ('p12', n), 'gather')

    def gather_last(n):
        arrived(('last', n), panel.at[n, 6])
        send(panel.at[n, 6], panel.at[n, 7], partner, ('p3', n), 'gather')

    def zgather_start(n):
        for k in zorder:
            send(upan.at[n, c], upan.at[n, c], (zpeer(k), r), 'zgather', 'zgather')

    def zgather_wait(n):
        arrived('zgather', upan.at[n, pl.ds(0, 3)])
        return jnp.concatenate([upan[n, k] for k in range(4)], axis=1)

    def zsum_start(n, acc):
        acc_t = acc.T
        for k in range(4):
            upart[n, k] = acc_t[:, k * 128:(k + 1) * 128]
        for k in zorder:
            send(upart.at[n, zpeer(k)], uin.at[n, k - 1], (zpeer(k), r), 'zsum', 'zsum')

    def zsum_wait(n):
        arrived('zsum', uin.at[n])
        total = (upart[n, c] + uin[n, 0]) + (uin[n, 1] + uin[n, 2])
        nxt = total.astype(BF16)
        usum[...] = usum[...] + nxt.astype(F32)
        return nxt

    def mask_step(step, carry):
        mask_copy(step).wait()
        slot = mask_slot(step)
        part = step % per_slot
        buf = step % STAGES

        def convert(i, col):
            at = pl.multiple_of(i * 16, 16)
            x = stage[buf, pl.ds(at, 16), :].astype(F32)
            row = pl.multiple_of(part * rows + i * 16, 16)
            adj[slot, pl.ds(row, 16), :] = x.astype(BF16)
            lanes = x[:, :128]
            for t in range(1, width // 128):
                lanes = lanes + x[:, t * 128:(t + 1) * 128]
            rowacc[pl.ds(row, 16), :] += lanes
            return col + (x[:8] + x[8:])

        colacc[slot] += lax.fori_loop(0, rows // 16, convert, jnp.zeros((8, width), F32), unroll=2)

        @pl.when(step + STAGES < steps)
        def _():
            mask_copy(step + STAGES).start()

        return carry

    def column_sum(slot):
        return jnp.sum(colacc[slot], axis=0, keepdims=True)

    def mask_part(first, last):
        lax.fori_loop(steps * first // 8, steps * last // 8, mask_step, 0)

    with jax.named_scope('mask_a'):
        mask_part(0, 1)
    with jax.named_scope('barrier'):
        pl.semaphore_wait(barrier, len(peers))
    with jax.named_scope('inputs'):
        for copy in inputs:
            copy.wait()
        gather_start(0, 0)
        gather_start(0, 1)
        zgather_start(0)
        isum[...] = panel[0, 0].astype(F32)
        usum[...] = upan[0, c].astype(F32)
    with jax.named_scope('mask_b'):
        mask_part(1, 5)
        for d in range(4):
            deg_send[pl.ds(d, 1), :] = column_sum(2 * d + 1)
        send(deg_send, deg_recv, partner, 'dp', 'dp')
    with jax.named_scope('forward00'):
        gather_forward(0, 0)
    with jax.named_scope('mask_c'):
        mask_part(5, 7)
    with jax.named_scope('forward01'):
        gather_forward(0, 1)
    with jax.named_scope('mask_d'):
        mask_part(7, 8)

    with jax.named_scope('deg_sum'):
        udeg[...] = dot(jnp.ones((8, 128), BF16), rowacc[...].astype(BF16), NT)
        for k in zorder:
            send(udeg, udeg_in.at[k - 1], (zpeer(k), r), 'zd', 'zd')
        mine = jnp.concatenate(
            [column_sum(2 * d) for d in range(4)], axis=0)
    with jax.named_scope('deg_partner'):
        arrived('dp', deg_recv)
        deg_own[...] = mine + deg_recv[...]
        for k, device in enumerate((xn, yn, dg)):
            send(deg_own, deg_in.at[k], device, 'ds', 'ds')
        for d in range(4):
            far_send[d] = deg_own[d:d + 1, :]
            send(far_send.at[d], far_in.at[d], slots[2 * (3 - d) + 1], 'far', 'far')
    with jax.named_scope('deg_users'):
        arrived('zd', udeg_in)
        du = udeg[...] + jnp.sum(udeg_in[...], axis=0)
        inv = lax.rsqrt(jnp.maximum(du, 1.0))
        invu[...] = jnp.broadcast_to(inv[0:1, :], (128, users)).T
    with jax.named_scope('deg_items'):
        arrived('ds', deg_in)
    with jax.named_scope('deg_inv'):
        for d in range(4):
            total = deg_own[pl.ds(d, 1), :]
            for k in range(3):
                total = total + deg_in[k, pl.ds(d ^ (k + 1), 1), :]
            deg_fin[pl.ds(d, 1), :] = lax.rsqrt(jnp.maximum(total, 1.0))
        send(deg_fin, deg_oth, partner, 'df', 'df')
        arrived('far', far_in)
        gather_near(0)

    def normalize(slot, at=0, size=width):
        d = slot // 2
        cols = pl.ds(at, size)
        if slot == 7:
            total = jnp.sum(far_in[:, :, cols], axis=0)
            inv_item = lax.rsqrt(jnp.maximum(total, 1.0))
        else:
            inv_item = (deg_oth if slot % 2 else deg_fin)[d:d + 1, cols]

        step = 16 * max(1, width // 2 // size)

        def scale(i, carry):
            for j in range(step // 16):
                row = pl.ds(pl.multiple_of(i * step + j * 16, 16), 16)
                inv_user = jnp.concatenate([invu[row, :]] * (size // 128), axis=1)
                adj[slot, row, cols] = adj[slot, row, cols] * (inv_user * inv_item).astype(BF16)
            return carry

        lax.fori_loop(0, users // step, scale, 0, unroll=2)

    sizes = (width // 8, width // 4, width - 3 * width // 8)
    starts = (0, width // 8, 3 * width // 8)
    splits = [pl.ds(at, size) for at, size in zip(starts, sizes)]
    lo, hi = pl.ds(0, HALF), pl.ds(HALF, HALF)

    def items_diagonal(n, i=None):
        cols = pl.ds(0, width) if i is None else splits[i]
        send(sacc.at[n, 3, lo, cols], hop1.at[n, 0, :, cols], xn, ('hop1', n), 'sum')
        send(sacc.at[n, 3, hi, cols], hop1.at[n, 1, :, cols], yn, ('hop1', n), 'sum')

    def items_x(n):
        send(sacc.at[n, 1, lo], rown.at[n, 0], xn, ('direct', n), 'sum')

    def items_y(n):
        send(sacc.at[n, 2, hi], rown.at[n, 3], yn, ('direct', n), 'sum')

    def away(n, u, d):
        psend[n, d] = dot(u, adj[2 * d + 1], NN)
        send(psend.at[n, d], drecv.at[n, d], partner, ('partner', n, d), 'items')

    def near(n, u, d):
        part = dot(u, adj[2 * d], NN)
        if d:
            arrived(('partner', n, d), drecv.at[n, d])
            part = part + drecv[n, d]
        sacc[n, d] = part

    def items_first(u):
        n, d = 0, 3

        def theirs(i):
            cols = splits[i]
            normalize(2 * d + 1, starts[i], sizes[i])
            psend[n, d, :, cols] = dot(u, adj[2 * d + 1, :, cols], NN)
            if i:
                send(psend.at[n, d, :, cols], drecv.at[n, d, :, cols], partner, ('partner', n, d, i), 'items')
            else:
                for k, half in enumerate((lo, hi)):
                    send(psend.at[n, d, half, cols], hop1b.at[k], slots[3 + 2 * k], 'hop1b', 'items')

        def ours(i):
            cols = splits[i]
            normalize(2 * d, starts[i], sizes[i])
            sacc[n, d, :, cols] = dot(u, adj[2 * d, :, cols], NN)

        def both(i):
            cols = splits[i]
            arrived(('partner', n, d, i), drecv.at[n, d, :, cols])
            sacc[n, d, :, cols] = sacc[n, d, :, cols] + drecv[n, d, :, cols]
            items_diagonal(n, i)

        theirs(0)
        ours(0)
        items_diagonal(n, 0)
        theirs(1)
        theirs(2)
        for i in (1, 2):
            ours(i)
            both(i)
        arrived('df', deg_oth)

        for k in (1, 2):
            normalize(2 * k + 1)
            away(n, u, k)
        normalize(2)
        near(n, u, 1)
        items_x(n)
        normalize(4)
        near(n, u, 2)
        items_y(n)
        normalize(1)
        away(n, u, 0)
        normalize(0)
        near(n, u, 0)

    def items_later(n, u, hooks):
        away(n, u, 3)
        away(n, u, 1)
        hooks[0]()
        near(n, u, 3)
        hooks[1]()
        away(n, u, 2)
        away(n, u, 0)
        near(n, u, 1)
        hooks[2]()
        near(n, u, 2)
        near(n, u, 0)

    def items_mid(n, i):
        if i == 0:
            arrived(('hop1', n), hop1.at[n])
            if n == 0:
                arrived('hop1b', hop1b)
                for k in range(2):
                    hop1[n, k, :, splits[0]] = hop1[n, k, :, splits[0]] + hop1b[k]
        at = pl.ds(i * QUARTER, QUARTER)
        for h, device in enumerate((yn, xn)):
            block, part = 2 - h, piece(h, i)
            sacc[n, block, part] = sacc[n, block, part] + hop1[n, h, at]
            send(sacc.at[n, block, part], rown.at[n, block, at], device, ('hop2', n, i), 'sum')

    def items_finish(n, i):
        if i == 0:
            arrived(('partner', n, 0), drecv.at[n, 0])
            arrived(('direct', n), rown.at[n, pl.ds(0, 2)])
        arrived(('hop2', n, i), rown.at[n, 0])
        at = pl.ds(i * QUARTER, QUARTER)
        for h in (0, 1):
            rows_h = piece(h, i)
            total = ((sacc[n, 0, rows_h] + drecv[n, 0, rows_h]) + rown[n, h, at]) + rown[n, 2 + h, at]
            nxt = total.astype(BF16)
            isum[rows_h] = isum[rows_h] + nxt.astype(F32)
            if n + 1 < LAYERS:
                panel[n + 1, 0, rows_h] = nxt

    def user_partial(n, near_done=False, hook=None):
        def some(first, stride, count):
            def one(j, carry):
                at = first + stride * j
                uacc[...] += dot(adj[at], panel[n, at], NT)
                return carry

            lax.fori_loop(0, count, one, 0)

        arrived(('p0', n), panel.at[n, 1])
        uacc[...] = dot(adj[0], panel[n, 0], NT)
        some(1, 1, 1)
        if hook is not None:
            hook()
        if not near_done:
            gather_near(n)
        some(2, 2, 2)
        arrived(('p12', n), panel.at[n, pl.ds(2, 2)])
        some(3, 2, 2)
        gather_last(n)
        some(6, 1, 1)
        arrived(('p3', n), panel.at[n, 7])
        some(7, 1, 1)
        return uacc[...]

    scope = jax.named_scope

    def mid(n):
        items_mid(n, 0)
        items_mid(n, 1)

    def finish(n, i):
        with scope(f'finish{n}{i}'):
            items_finish(n, i)
            gather_start(n + 1, i)

    def forward(n, i):
        with scope(f'forward{n}{i}'):
            gather_forward(n, i)

    def nothing():
        pass

    with scope('u0'):
        u0 = zgather_wait(0)
    with scope('items0'):
        items_first(u0)
    with scope('user0'):
        zsum_start(0, user_partial(0, True, lambda: mid(0)))
    finish(0, 0)
    with scope('zsum0'):
        upan[1, c] = zsum_wait(0)
        zgather_start(1)
    finish(0, 1)
    with scope('zgather1'):
        u1 = zgather_wait(1)
    with scope('items1'):
        forward(1, 0)
        items_later(1, u1, (lambda: forward(1, 1), lambda: items_diagonal(1), nothing))
        items_x(1)
        items_y(1)
    with scope('user1'):
        zsum_start(1, user_partial(1))
    with scope('mid1'):
        mid(1)
    with scope('zsum1'):
        upan[2, c] = zsum_wait(1)
        zgather_start(2)
    finish(1, 0)
    with scope('zgather2'):
        u2 = zgather_wait(2)
    with scope('items2'):
        items_later(2, u2, (nothing, lambda: finish(1, 1), lambda: forward(2, 0)))
        forward(2, 1)
        items_diagonal(2)
        items_x(2)
        items_y(2)
    with scope('user2'):
        zsum_start(2, user_partial(2))
    with scope('mid2'):
        items_mid(2, 0)

        @pl.when(core == 0)
        def _():
            items_mid(2, 1)

    with scope('zsum2'):
        zsum_wait(2)
        final_user = (usum[...] / (LAYERS + 1)).astype(BF16)
        fu_ref[...] = final_user
        upan[3, c] = final_user
        zgather_start(3)
    with scope('zgather3'):
        ufin = zgather_wait(3)
    with scope('pick'):
        local = qbuf[...] - r * users
        chosen = (lax.broadcasted_iota(jnp.int32, (users, local.shape[1]), 0)
                  == jnp.broadcast_to(local, (users, local.shape[1]))).astype(F32).astype(BF16)
        pk[0] = dot(ufin, chosen, NN).astype(BF16)

        @pl.when(core == 0)
        def _():
            send(pk.at[0], pk.at[1], partner, 'pick', 'pick')

        @pl.when(core == 1)
        def _():
            arrived('pick', pk.at[1])
            pk[2] = pk[0] + pk[1]
            for k, device in enumerate((xn, yn, dg)):
                send(pk.at[2], pk.at[3 + k], device, 'picks', 'picks')
            items_mid(2, 1)

    with scope('finish20'):
        items_finish(2, 0)
    with scope('picked'):
        @pl.when(core == 1)
        def _():
            arrived('picks', pk.at[pl.ds(3, 3)])
            total = pk[2]
            for k in range(3):
                total = total + pk[3 + k]
            pk[6] = total
            send(pk.at[6], pk.at[6], partner, 'picked', 'picked')
            sent('picks', pk.at[pl.ds(3, 3)])
            sent('picked', pk.at[6])

        @pl.when(core == 0)
        def _():
            arrived('picked', pk.at[6])
            sent('pick', pk.at[0])

        pick_ref[...] = pk[6].astype(F32).T.astype(BF16)
    with scope('finish21'):
        items_finish(2, 1)
        fi_ref[...] = (isum[...] / (LAYERS + 1)).astype(BF16)
    with scope('drain'):
        sent('gather', panel.at[:, pl.ds(0, 7)])
        sent('items', psend)
        sent('sum', sacc.at[:, pl.ds(1, 3)])
        sent('zsum', uin)
        sent('zgather', upan.at[:, pl.ds(0, 3)])
        for out, whole in (('dp', deg_send), ('zd', udeg_in), ('ds', deg_in), ('far', far_in),
                           ('df', deg_fin)):
            sent(out, whole)


def propagate(mask_blk, user_shard, item_shard, queries):
    users, items = mask_blk.shape
    width = items // 8
    per = user_shard.shape[1]
    n_query = queries.shape[0]
    vmem = pl.BlockSpec(memory_space=pltpu.VMEM)
    hbm = pl.BlockSpec(memory_space=pl.ANY)
    scratch = [
        pltpu.VMEM((8, users, width), BF16),
        pltpu.VMEM((STAGES, users // 4, width), jnp.int32),
        pltpu.VMEM((LAYERS, 8, EMB, width), BF16),
        pltpu.VMEM((LAYERS + 1, 4, EMB, per), BF16),
        pltpu.VMEM((LAYERS, 4, EMB, width), F32),
        pltpu.VMEM((LAYERS, 4, EMB, width), F32),
        pltpu.VMEM((LAYERS, 4, EMB, width), F32),
        pltpu.VMEM((LAYERS, 2, HALF, width), F32),
        pltpu.VMEM((2, HALF, width // 8), F32),
        pltpu.VMEM((LAYERS, 4, HALF, width), F32),
        pltpu.VMEM((EMB, width), F32),
        pltpu.VMEM((EMB, per), F32),
        pltpu.VMEM((8, 8, width), F32),
        pltpu.VMEM((users, 128), F32),
        pltpu.VMEM((4, width), F32),
        pltpu.VMEM((4, width), F32),
        pltpu.VMEM((4, width), F32),
        pltpu.VMEM((3, 4, width), F32),
        pltpu.VMEM((4, width), F32),
        pltpu.VMEM((4, width), F32),
        pltpu.VMEM((4, 1, width), F32),
        pltpu.VMEM((4, 1, width), F32),
        pltpu.VMEM((8, users), F32),
        pltpu.VMEM((3, 8, users), F32),
        pltpu.VMEM((users, 128), F32),
        pltpu.VMEM((users, EMB), F32),
        pltpu.VMEM((LAYERS, 4, EMB, per), F32),
        pltpu.VMEM((LAYERS, 3, EMB, per), F32),
        pltpu.VMEM((7, EMB, n_query), BF16),
        pltpu.VMEM((1, n_query), jnp.int32),
        pltpu.SemaphoreType.DMA((STAGES,)),
        pltpu.SemaphoreType.DMA((3,)),
        pltpu.SemaphoreType.DMA((N_SENT,)),
        pltpu.SemaphoreType.DMA((N_GOT,)),
    ]
    return pl.pallas_call(
        kernel,
        out_shape=(pltpu.VMEM((EMB, per), BF16),
                   pltpu.VMEM((EMB, width), BF16),
                   pltpu.VMEM((n_query, EMB), BF16)),
        in_specs=[hbm, hbm, hbm, hbm],
        out_specs=(vmem, vmem, vmem),
        scratch_shapes=scratch,
        compiler_params=pltpu.CompilerParams(
            collective_id=0, has_side_effects=True, vmem_limit_bytes=61_600_000),
        name='propagate',
    )(mask_blk, item_shard, user_shard, queries.reshape(1, n_query))


def output_kernel(pick_ref, item_ref, user_ref, scores_ref, fi_ref, fu_ref, scores, sem):
    copies = [pltpu.make_async_copy(item_ref, fi_ref, sem.at[0]),
              pltpu.make_async_copy(user_ref, fu_ref, sem.at[1])]
    for copy in copies:
        copy.start()
    picked = pick_ref[...]
    cols = scores.shape[1] // 4
    for i in range(4):
        at = pl.ds(i * cols, cols)
        scores[:, at] = dot(picked, item_ref[:, at], NN)
        copy = pltpu.make_async_copy(scores.at[:, at], scores_ref.at[:, at], sem.at[2 + i])
        copy.start()
        copies.append(copy)
    for copy in copies:
        copy.wait()


def outputs(fu_t, fi_t, picked):
    n_query = picked.shape[0]
    width, per = fi_t.shape[1], fu_t.shape[1]
    hbm = pl.BlockSpec(memory_space=pl.ANY)
    vmem = pl.BlockSpec(memory_space=pltpu.VMEM)
    args = [pltpu.with_memory_space_constraint(x, pltpu.VMEM) for x in (picked, fi_t, fu_t)]
    return pl.pallas_call(
        output_kernel,
        out_shape=(jax.ShapeDtypeStruct((n_query, width), F32),
                   jax.ShapeDtypeStruct((EMB, width), BF16),
                   jax.ShapeDtypeStruct((EMB, per), BF16)),
        in_specs=[vmem, vmem, vmem],
        out_specs=(hbm, hbm, hbm),
        scratch_shapes=[pltpu.VMEM((n_query, width), F32), pltpu.SemaphoreType.DMA((6,))],
        name='outputs',
    )(*args)


def solution(mesh):
    def device_step(mask_blk, user_shard, item_shard, queries):
        fu_t, fi_t, picked = propagate(mask_blk, user_shard.T, item_shard.T, queries)
        scores, fi_t, fu_t = outputs(fu_t, fi_t, picked)
        return fu_t.T, fi_t.T, scores

    return jax.shard_map(
        device_step, mesh=mesh,
        in_specs=(P('row', 'col'), P(('row', 'col'), None), P(('col', 'row'), None), P()),
        out_specs=(P(('row', 'col'), None), P(('col', 'row'), None), P(None, ('col', 'row'))),
        check_vma=False)
```
